32 devices in a mesh: ctx: 8 (over z, x), exp: 4 (over y, core).
Axes of the slice: x: 2, y: 2, z: 4, core: 2. Of those that a mesh axis runs over, the one named last changes fastest.
Arguments:
- tokens: bfloat16 [2, 4, 1024, 1024], P(None, 'exp', 'ctx'), may hold values from -6 to 6
- cotangent: bfloat16 [2, 4, 1024, 1024], P(None, 'exp', 'ctx'), may hold values from -6 to 6
- bucket_ids: int32 [2048], replicated, may hold values from 0 to 31
- routes: int32 [2, 4, 1024, 2], P(None, 'exp', 'ctx'), may hold values from 0 to 3, all different within a row; in each aligned block of 128 rows (0 to 127, 128 to 255, ..., all dimensions but the last counted through in order) at most 80 rows name the same one
- qkv_master: float32 [3, 1024, 1024], P(None, ('ctx', 'exp')), may hold values from -0.1875 to 0.1875
- out_master: float32 [1024, 1024], P(('ctx', 'exp')), may hold values from -1.5 to 1.5
- router_master: float32 [1024, 4], P(('ctx', 'exp')), may hold values from -0.375 to 0.375
- gain_attn_master: float32 [1024], P(('ctx', 'exp')), may hold values from 0.5 to 1.5
- gain_mix_master: float32 [1024], P(('ctx', 'exp')), may hold values from 0.5 to 1.5
- table_master: float32 [512], P(('ctx', 'exp')), may hold values from -4 to 4
- gate_master: float32 [4, 1024, 2816], P('exp', 'ctx'), may hold values from -0.1875 to 0.1875
- up_master: float32 [4, 1024, 2816], P('exp', 'ctx'), may hold values from -0.1875 to 0.1875
- down_master: float32 [4, 2816, 1024], P('exp', 'ctx'), may hold values from -0.109375 to 0.109375
- qkv_first: float32 [3, 1024, 1024], P(None, ('ctx', 'exp')), may hold values from -543.058 to 543.058
- out_first: float32 [1024, 1024], P(('ctx', 'exp')), may hold values from -13.57645 to 13.57645
- router_first: float32 [1024, 4], P(('ctx', 'exp')), may hold values from -814.58701 to 814.58701
- gain_attn_first: float32 [1024], P(('ctx', 'exp')), may hold values from -2715.29 to 2715.29
- gain_mix_first: float32 [1024], P(('ctx', 'exp')), may hold values from -271.529 to 271.529
- table_first: float32 [512], P(('ctx', 'exp')), may hold values from -814.58701 to 814.58701
- gate_first: float32 [4, 1024, 2816], P('exp', 'ctx'), may hold values from -27.1529 to 27.1529
- up_first: float32 [4, 1024, 2816], P('exp', 'ctx'), may hold values from -27.1529 to 27.1529
- down_first: float32 [4, 2816, 1024], P('exp', 'ctx'), may hold values from -54.3058 to 54.3058
- qkv_second: float32 [3, 1024, 1024], P(None, ('ctx', 'exp')), may hold values from 9830.4 to 98304
- out_second: float32 [1024, 1024], P(('ctx', 'exp')), may hold values from 6.144 to 61.44
- router_second: float32 [1024, 4], P(('ctx', 'exp')), may hold values from 22118.4 to 221184
- gain_attn_second: float32 [1024], P(('ctx', 'exp')), may hold values from 245760 to 2457600
- gain_mix_second: float32 [1024], P(('ctx', 'exp')), may hold values from 2457.6 to 24576
- table_second: float32 [512], P(('ctx', 'exp')), may hold values from 22118.4 to 221184
- gate_second: float32 [4, 1024, 2816], P('exp', 'ctx'), may hold values from 24.576 to 245.76
- up_second: float32 [4, 1024, 2816], P('exp', 'ctx'), may hold values from 24.576 to 245.76
- down_second: float32 [4, 2816, 1024], P('exp', 'ctx'), may hold values from 98.304 to 983.04
Outputs:
- output: bfloat16 [2, 4, 1024, 1024], P(None, 'exp', 'ctx')
- grad_tokens: float32 [2, 4, 1024, 1024], P(None, 'exp', 'ctx')
- qkv_grad: float32 [3, 1024, 1024], P(None, ('ctx', 'exp'))
- out_grad: float32 [1024, 1024], P(('ctx', 'exp'))
- router_grad: float32 [1024, 4], P(('ctx', 'exp'))
- gain_attn_grad: float32 [1024], P(('ctx', 'exp'))
- gain_mix_grad: float32 [1024], P(('ctx', 'exp'))
- table_grad: float32 [512], P(('ctx', 'exp'))
- gate_grad: float32 [4, 1024, 2816], P('exp', 'ctx')
- up_grad: float32 [4, 1024, 2816], P('exp', 'ctx')
- down_grad: float32 [4, 2816, 1024], P('exp', 'ctx')
- qkv_first_new: float32 [3, 1024, 1024], P(None, ('ctx', 'exp'))
- out_first_new: float32 [1024, 1024], P(('ctx', 'exp'))
- router_first_new: float32 [1024, 4], P(('ctx', 'exp'))
- gain_attn_first_new: float32 [1024], P(('ctx', 'exp'))
- gain_mix_first_new: float32 [1024], P(('ctx', 'exp'))
- table_first_new: float32 [512], P(('ctx', 'exp'))
- gate_first_new: float32 [4, 1024, 2816], P('exp', 'ctx')
- up_first_new: float32 [4, 1024, 2816], P('exp', 'ctx')
- down_first_new: float32 [4, 2816, 1024], P('exp', 'ctx')
- qkv_second_new: float32 [3, 1024, 1024], P(None, ('ctx', 'exp'))
- out_second_new: float32 [1024, 1024], P(('ctx', 'exp'))
- router_second_new: float32 [1024, 4], P(('ctx', 'exp'))
- gain_attn_second_new: float32 [1024], P(('ctx', 'exp'))
- gain_mix_second_new: float32 [1024], P(('ctx', 'exp'))
- table_second_new: float32 [512], P(('ctx', 'exp'))
- gate_second_new: float32 [4, 1024, 2816], P('exp', 'ctx')
- up_second_new: float32 [4, 1024, 2816], P('exp', 'ctx')
- down_second_new: float32 [4, 2816, 1024], P('exp', 'ctx')
- qkv_update: float32 [3, 1024, 1024], P(None, ('ctx', 'exp'))
- out_update: float32 [1024, 1024], P(('ctx', 'exp'))
- router_update: float32 [1024, 4], P(('ctx', 'exp'))
- gain_attn_update: float32 [1024], P(('ctx', 'exp'))
- gain_mix_update: float32 [1024], P(('ctx', 'exp'))
- table_update: float32 [512], P(('ctx', 'exp'))
- gate_update: float32 [4, 1024, 2816], P('exp', 'ctx')
- up_update: float32 [4, 1024, 2816], P('exp', 'ctx')
- down_update: float32 [4, 2816, 1024], P('exp', 'ctx')
The draws below stay inside these ranges and needn't reach their ends.
Inputs may be any that keep to these rules, and one draw needn't show every extreme that they name: `routes`: in each aligned block of 128 tokens (one index of ctx, one sequence) no expert is named by more than 80 choices, and in some block one expert is named exactly 80 times; the two experts of a token differ.
All inputs are finite; a program needn't handle non-finite values.
Results may differ from the reference program's by a relative error of at most 0.024.
The reference program's roundings to bfloat16 on the way count: a program that leaves them out, or rounds other values in their place, can miss the bound.
Values may be sent and summed in bfloat16 or wider, within the bound.
A program may use at most 256 MiB of HBM per device.

```python
import math
import jax
import jax.numpy as jnp
import numpy as np
from jax import lax

D = 1024
HEADS = 16
HEAD_DIM = 64
FF = 2816
BUCKETS = 32
TOP = 2
BLOCK = 256
MICRO = 2
STEP = 3
TOK_DEV = 128
LENGTH = 1024
SEQS = 4
EXPERTS = 4
CAP = 80


def grad_scale(factor):
    return factor * math.sqrt(MICRO * SEQS * LENGTH)


def first_draw(key, salt_value, array_shape, factor):
    noise = jax.random.truncated_normal(jax.random.fold_in(key, salt_value), -3.0, 3.0, array_shape, jnp.float32)
    return grad_scale(factor) * noise


def second_draw(key, salt_value, array_shape, factor):
    spread = jax.random.uniform(jax.random.fold_in(key, salt_value), array_shape, jnp.float32, math.log(0.3), math.log(3.0))
    return grad_scale(factor) ** 2 * jnp.exp(spread)


def draw_qkv_first(key, part):
    return first_draw(key, 11, (3, D, D), 2.0)


def draw_out_first(key, part):
    return first_draw(key, 12, (D, D), 0.05)


def draw_router_first(key, part):
    return first_draw(key, 13, (D, EXPERTS), 3.0)


def draw_gain_attn_first(key, part):
    return first_draw(key, 14, (D,), 10.0)


def draw_gain_mix_first(key, part):
    return first_draw(key, 15, (D,), 1.0)


def draw_table_first(key, part):
    return first_draw(key, 16, (HEADS * BUCKETS,), 3.0)


def draw_gate_first(key, part):
    return first_draw(key, 17, (EXPERTS, D, FF), 0.1)


def draw_up_first(key, part):
    return first_draw(key, 18, (EXPERTS, D, FF), 0.1)


def draw_down_first(key, part):
    return first_draw(key, 19, (EXPERTS, FF, D), 0.2)


def draw_qkv_second(key, part):
    return second_draw(key, 21, (3, D, D), 2.0)


def draw_out_second(key, part):
    return second_draw(key, 22, (D, D), 0.05)


def draw_router_second(key, part):
    return second_draw(key, 23, (D, EXPERTS), 3.0)


def draw_gain_attn_second(key, part):
    return second_draw(key, 24, (D,), 10.0)


def draw_gain_mix_second(key, part):
    return second_draw(key, 25, (D,), 1.0)


def draw_table_second(key, part):
    return second_draw(key, 26, (HEADS * BUCKETS,), 3.0)


def draw_gate_second(key, part):
    return second_draw(key, 27, (EXPERTS, D, FF), 0.1)


def draw_up_second(key, part):
    return second_draw(key, 28, (EXPERTS, D, FF), 0.1)


def draw_down_second(key, part):
    return second_draw(key, 29, (EXPERTS, FF, D), 0.2)


def set_ends(array, stream_key, least, high):
    index_at = [jax.random.randint(jax.random.fold_in(stream_key, axis), (), 0, length) for axis, length in enumerate(array.shape)]
    widest = array.shape.index(max(array.shape))
    next_to = index_at[:widest] + [(index_at[widest] + 1) % array.shape[widest]] + index_at[widest + 1:]
    return array.at[tuple(index_at)].set(least).at[tuple(next_to)].set(high)


def shard_levels(rng, dims, shards, smallest, high):
    factor_of, own = 1.0, jax.random.fold_in(rng, 6)
    for axis_at, shards_of in shards:
        heights = jnp.exp(jax.random.uniform(jax.random.fold_in(own, axis_at), (shards_of,), jnp.float32, smallest / len(shards), high / len(shards)))
        factor_of = factor_of * jnp.repeat(heights, dims[axis_at] // shards_of).reshape([-1 if axis == axis_at else 1 for axis in range(len(dims))])
    return factor_of


def deal_out(stream_key, own, number, rows, amount, top, reach, skew):
    order = jax.random.permutation(stream_key, amount)
    packed, ordinary = portions_of(amount, rows * top, reach, skew, True), portions_of(amount, rows * top, reach, skew, False)
    places = jnp.arange(amount)

    def named(tallies, offset_by):
        used = int((tallies > 0).sum())
        fixed = max(1, used // 4)
        passed = fixed + (places - fixed + offset_by * (used - fixed)) % max(1, amount - fixed)
        return jnp.zeros((amount,), jnp.int32).at[order[jnp.where(places < fixed, places, passed)]].set(jnp.asarray(tallies, jnp.int32))

    tallies = jnp.where(number % 4 == 0, named(packed, number // 4), named(ordinary, number - number // 4 - 1))
    mixed = jax.random.permutation(jax.random.fold_in(own, 3), amount)
    donor, taker = mixed[0:amount // 2 * 2:2], mixed[1:amount // 2 * 2:2]
    room = jnp.minimum(tallies[donor] - 1, reach - tallies[taker]) // 2
    room = jnp.where((donor == order[0]) | (taker == order[0]) | (tallies[taker] == 0), 0, jnp.maximum(room, 0))
    passed = jax.random.randint(jax.random.fold_in(own, 4), (amount // 2,), 0, 1 << 20) % (room + 1)
    tallies = tallies.at[donor].add(-passed).at[taker].add(passed)
    items = jnp.searchsorted(jnp.cumsum(tallies), jnp.arange(rows * top), side="right").astype(jnp.int32)
    grid = items.reshape(top, rows).T
    grid = grid[jax.random.permutation(jax.random.fold_in(own, 1), rows)]
    offset_by = jax.random.randint(jax.random.fold_in(own, 2), (rows, 1), 0, top)
    return jnp.take_along_axis(grid, (jnp.arange(top)[None, :] + offset_by) % top, axis=1)


def portions_of(amount, total, most, skew, full):
    weights = [(1 << 20) // math.isqrt(standing ** skew) + 1 for standing in range(1, amount + 1)]
    largest = most if full else min(most, max(-(-total // amount), total * weights[0] // sum(weights)))
    least = 1 if total - largest >= amount - 1 else 0
    counts, surplus = [largest] + [least] * (amount - 1), total - largest - least * (amount - 1)
    while surplus > 0:
        candidates = [i for i in range(1, amount) if counts[i] < largest] or [i for i in range(1, amount) if counts[i] < most]
        whole, remaining = sum([weights[i] for i in candidates]), surplus
        for i in candidates:
            more = min(most - counts[i], max(1, remaining * weights[i] // whole), surplus)
            counts[i] = counts[i] + more
            surplus = surplus - more
    return np.array(counts)


def scatter_about(key, dims, width, reach, cuts=(), held_as=jnp.bfloat16):
    values = jax.random.normal(key, dims, jnp.float32) * width
    if len(cuts) > 0:
        values = shard_levels(key, dims, cuts, -0.22, 0.18) * values
    return jnp.clip(values, min=-reach, max=reach).astype(held_as)


def setup_inputs(seed: int = 0) -> dict:
    key_list = jax.random.split(jax.random.key(seed), 32)
    tokens = scatter_about(key_list[0], (MICRO, SEQS, LENGTH, D), 1.0, 6.0, ((1, 4), (2, 8)))
    cotangent = scatter_about(key_list[1], (MICRO, SEQS, LENGTH, D), 1.0, 6.0, ((1, 4), (2, 8)))
    bucket_ids = set_ends(jax.random.randint(key_list[2], (2 * LENGTH,), 0, BUCKETS), jax.random.fold_in(key_list[2], 1), 0, BUCKETS - 1).astype(jnp.int32)
    routes_keys = jax.random.split(jax.random.fold_in(key_list[3], 1), MICRO * SEQS * LENGTH // TOK_DEV)
    routes_turns = jax.random.permutation(jax.random.fold_in(key_list[3], 3), MICRO * SEQS * LENGTH // TOK_DEV)
    routes = jax.vmap(lambda own, number: deal_out(jax.random.fold_in(key_list[3], 2), own, number, TOK_DEV, EXPERTS, TOP, CAP, 2))(routes_keys, routes_turns).reshape((MICRO, SEQS, LENGTH, TOP))
    qkv_master = scatter_about(key_list[4], (3, D, D), D ** -0.5, 0.1875, ((1, 32),), jnp.float32)
    out_master = scatter_about(key_list[5], (D, D), (max(1, 16 * D // LENGTH)) ** -0.5, 1.5, ((0, 32),), jnp.float32)
    router_master = scatter_about(key_list[6], (D, EXPERTS), (D // 4) ** -0.5, 0.375, ((0, 32),), jnp.float32)
    gain_attn_master = jnp.clip(1.0 + 0.1 * jax.random.normal(key_list[7], (D,), jnp.float32), 0.5, 1.5)
    gain_mix_master = jnp.clip(1.0 + 0.1 * jax.random.normal(key_list[8], (D,), jnp.float32), 0.5, 1.5)
    table_master = scatter_about(key_list[9], (HEADS * BUCKETS,), 1.0, 4.0, ((0, 32),), jnp.float32)
    gate_master = scatter_about(key_list[10], (EXPERTS, D, FF), D ** -0.5, 0.1875, ((0, 4), (1, 8)), jnp.float32)
    up_master = scatter_about(key_list[11], (EXPERTS, D, FF), D ** -0.5, 0.1875, ((0, 4), (1, 8)), jnp.float32)
    down_master = scatter_about(key_list[12], (EXPERTS, FF, D), FF ** -0.5, 0.109375, ((0, 4), (1, 8)), jnp.float32)
    qkv_first = draw_qkv_first(jax.random.fold_in(key_list[31], 71), 0)
    out_first = draw_out_first(jax.random.fold_in(key_list[31], 71), 0)
    router_first = draw_router_first(jax.random.fold_in(key_list[31], 71), 0)
    gain_attn_first = draw_gain_attn_first(jax.random.fold_in(key_list[31], 71), 0)
    gain_mix_first = draw_gain_mix_first(jax.random.fold_in(key_list[31], 71), 0)
    table_first = draw_table_first(jax.random.fold_in(key_list[31], 71), 0)
    gate_first = draw_gate_first(jax.random.fold_in(key_list[31], 71), 0)
    up_first = draw_up_first(jax.random.fold_in(key_list[31], 71), 0)
    down_first = draw_down_first(jax.random.fold_in(key_list[31], 71), 0)
    qkv_second = draw_qkv_second(jax.random.fold_in(key_list[31], 71), 0)
    out_second = draw_out_second(jax.random.fold_in(key_list[31], 71), 0)
    router_second = draw_router_second(jax.random.fold_in(key_list[31], 71), 0)
    gain_attn_second = draw_gain_attn_second(jax.random.fold_in(key_list[31], 71), 0)
    gain_mix_second = draw_gain_mix_second(jax.random.fold_in(key_list[31], 71), 0)
    table_second = draw_table_second(jax.random.fold_in(key_list[31], 71), 0)
    gate_second = draw_gate_second(jax.random.fold_in(key_list[31], 71), 0)
    up_second = draw_up_second(jax.random.fold_in(key_list[31], 71), 0)
    down_second = draw_down_second(jax.random.fold_in(key_list[31], 71), 0)
    return {"tokens": tokens, "cotangent": cotangent, "bucket_ids": bucket_ids, "routes": routes, "qkv_master": qkv_master, "out_master": out_master, "router_master": router_master, "gain_attn_master": gain_attn_master, "gain_mix_master": gain_mix_master, "table_master": table_master, "gate_master": gate_master, "up_master": up_master, "down_master": down_master, "qkv_first": qkv_first, "out_first": out_first, "router_first": router_first, "gain_attn_first": gain_attn_first, "gain_mix_first": gain_mix_first, "table_first": table_first, "gate_first": gate_first, "up_first": up_first, "down_first": down_first, "qkv_second": qkv_second, "out_second": out_second, "router_second": router_second, "gain_attn_second": gain_attn_second, "gain_mix_second": gain_mix_second, "table_second": table_second, "gate_second": gate_second, "up_second": up_second, "down_second": down_second}


eps_norm = 1e-06
eps_adam = 1e-08
score_scale = 0.125
decay_rate = 0.5
learn_rate = 1.0
weight_decay = 0.1
highest = lax.Precision.HIGHEST

@jax.custom_vjp
def low(v):
    return lax.optimization_barrier(v.astype(jnp.bfloat16)).astype(jnp.float32)

@jax.custom_vjp
def low_back(v):
    return v

def low_keep(v):
    return (low(v), None)

def low_pass(kept, grad):
    return (grad,)

def back_keep(v):
    return (v, None)

def back_low(kept, grad):
    return (low(grad),)
low.defvjp(low_keep, low_pass)
low_back.defvjp(back_keep, back_low)

def rms_scale(norm_input, gain_wide):
    factor = lax.rsqrt(lax.optimization_barrier(jnp.mean(norm_input * norm_input, axis=-1, keepdims=True)) + eps_norm)
    return norm_input * factor * gain_wide

def attend_rows(queries, first_row, keys_all, values_all, offset_bias):
    block_rows = queries.shape[0]
    length = keys_all.shape[0]
    query_pos = first_row + jnp.arange(block_rows, dtype=jnp.int32)
    key_pos = jnp.arange(length, dtype=jnp.int32)
    offsets = key_pos[None, :] - query_pos[:, None] + (length - 1)
    pos_bias = offset_bias[:, offsets]
    raw_scores = jnp.einsum('qhd,khd->hqk', queries, keys_all, precision=highest) * score_scale + pos_bias
    raw_scores = low_back(raw_scores)
    allowed = key_pos[None, :] // BLOCK <= query_pos[:, None] // BLOCK
    exp_scores = jnp.where(allowed[None], jnp.exp(raw_scores), 0.0)
    row_total = lax.optimization_barrier(jnp.sum(exp_scores, axis=-1))
    summed = jnp.einsum('hqk,khd->qhd', low(exp_scores), values_all, precision=highest)
    summed = low_back(summed)
    return summed / jnp.transpose(row_total)[:, :, None]

def attention(queries, keys_all, values_all, offset_bias):
    length = queries.shape[0]
    block_rows = math.gcd(length, 512)
    block_count = length // block_rows
    blocks = queries.reshape(block_count, block_rows, HEADS, HEAD_DIM)
    starts = jnp.arange(block_count, dtype=jnp.int32) * block_rows

    def one_block(block_item):
        return attend_rows(block_item[0], block_item[1], keys_all, values_all, offset_bias)
    result = lax.map(jax.checkpoint(one_block), (blocks, starts))
    return result.reshape(length, HEADS * HEAD_DIM)

def slot_index(route_rows):
    blocks = route_rows.reshape(-1, TOK_DEV * TOP)
    route_hits = (blocks[:, :, None] == jnp.arange(EXPERTS, dtype=jnp.int32)).astype(jnp.int32)
    before = (jnp.cumsum(route_hits, axis=1) - route_hits).astype(jnp.int32)
    position = lax.optimization_barrier(jnp.sum(before * route_hits, axis=-1)).astype(jnp.int32)
    return (blocks * CAP + position).astype(jnp.int32)

def expert_layer(expert_rows, w_gate, w_up, w_down):
    gate_pre = low_back(jnp.einsum('erd,edf->erf', expert_rows, w_gate, precision=highest))
    up_pre = low_back(jnp.einsum('erd,edf->erf', expert_rows, w_up, precision=highest))
    hidden = low(jax.nn.gelu(gate_pre, approximate=True) * up_pre)
    result = jnp.einsum('erf,efd->erd', hidden, w_down, precision=highest)
    return low_back(low(result))

def mixture(normed, route_rows, router, w_gate, w_up, w_down):
    length = normed.shape[0]
    logits = jnp.dot(low(normed), router, precision=highest)
    router_probs = jax.nn.softmax(logits, axis=-1)
    chosen = jnp.take_along_axis(router_probs, route_rows, axis=1)
    weights = chosen / lax.optimization_barrier(jnp.sum(chosen, axis=-1, keepdims=True))
    slots = slot_index(route_rows)
    block_count = slots.shape[0]
    targets = jnp.arange(EXPERTS * CAP, dtype=jnp.int32)
    dispatch = (slots[:, None, :] == targets[None, :, None]).astype(jnp.float32)
    entries = low_back(low(jnp.repeat(normed, TOP, axis=0)))
    entries = entries.reshape(block_count, TOK_DEV * TOP, D)
    placed = jnp.einsum('nst,ntd->nsd', dispatch, entries, precision=highest)
    expert_rows = placed.reshape(block_count, EXPERTS, CAP, D).transpose(1, 0, 2, 3).reshape(EXPERTS, block_count * CAP, D)
    result = expert_layer(expert_rows, w_gate, w_up, w_down)
    result = result.reshape(EXPERTS, block_count, CAP, D).transpose(1, 0, 2, 3).reshape(block_count, EXPERTS * CAP, D)
    returned = jnp.einsum('nst,nsd->ntd', dispatch, result, precision=highest).reshape(length, TOP, D)
    return lax.optimization_barrier(jnp.sum(weights[:, :, None] * returned, axis=1))

def layer(params, seq_rows, route_rows, bucket_ids):
    w_qkv, w_out, router, gain_attn, gain_mix, table, w_gate, w_up, w_down = params
    length = seq_rows.shape[0]
    normed = low(rms_scale(seq_rows, gain_attn))
    projected = [low_back(low(jnp.dot(normed, w_qkv[member], precision=highest))) for member in range(3)]
    shaped = [member.reshape(length, HEADS, HEAD_DIM) for member in projected]
    offset_bias = table.reshape(HEADS, BUCKETS)[:, bucket_ids]
    attended = low_back(low(attention(shaped[0], shaped[1], shaped[2], offset_bias)))
    branch = low_back(jnp.dot(attended, w_out, precision=highest))
    hidden_state = seq_rows + branch
    normed_mix = rms_scale(hidden_state, gain_mix)
    return hidden_state + mixture(normed_mix, route_rows, router, w_gate, w_up, w_down)

def adamw_step(master, gradient, first_old, second_old):
    first_new = decay_rate * first_old + (1.0 - decay_rate) * gradient
    second_new = decay_rate * second_old + (1.0 - decay_rate) * gradient * gradient
    correct = 1.0 - decay_rate ** STEP
    update = -learn_rate * (first_new / correct / (jnp.sqrt(second_new / correct) + eps_adam) + weight_decay * master)
    return (gradient, first_new, second_new, update)

def reference(tokens, cotangent, bucket_ids, routes, qkv_master, out_master, router_master, gain_attn_master, gain_mix_master, table_master, gate_master, up_master, down_master, qkv_first, out_first, router_first, gain_attn_first, gain_mix_first, table_first, gate_first, up_first, down_first, qkv_second, out_second, router_second, gain_attn_second, gain_mix_second, table_second, gate_second, up_second, down_second):
    masters = (qkv_master, out_master, router_master, gain_attn_master, gain_mix_master, table_master, gate_master, up_master, down_master)
    firsts = (qkv_first, out_first, router_first, gain_attn_first, gain_mix_first, table_first, gate_first, up_first, down_first)
    seconds = (qkv_second, out_second, router_second, gain_attn_second, gain_mix_second, table_second, gate_second, up_second, down_second)
    params = tuple((member.astype(jnp.bfloat16).astype(jnp.float32) for member in masters))
    length = tokens.shape[2]
    seq_tokens = tokens.reshape(-1, length, D)
    seq_cots = cotangent.reshape(-1, length, D)
    seq_routes = routes.reshape(-1, length, TOP)

    def one_sequence(totals, seq_item):
        seq_input, seq_cot, seq_route = seq_item

        def forward(weights, rows_in):
            return layer(weights, rows_in, seq_route, bucket_ids)
        result, pullback = jax.vjp(forward, params, seq_input.astype(jnp.float32))
        grad_params, grad_rows = pullback(seq_cot.astype(jnp.float32))
        totals = tuple((total_sum + member for total_sum, member in zip(totals, grad_params)))
        return (totals, (result.astype(jnp.bfloat16), grad_rows))
    zero_sums = tuple((jnp.zeros_like(member) for member in params))
    grad_sums, (outputs, grad_seq) = lax.scan(one_sequence, zero_sums, (seq_tokens, seq_cots, seq_routes))
    results = [adamw_step(master, gradient, first_old, second_old) for master, gradient, first_old, second_old in zip(masters, grad_sums, firsts, seconds)]
    qkv_grad, qkv_first_new, qkv_second_new, qkv_update = results[0]
    out_grad, out_first_new, out_second_new, out_update = results[1]
    router_grad, router_first_new, router_second_new, router_update = results[2]
    gain_attn_grad, gain_attn_first_new, gain_attn_second_new, gain_attn_update = results[3]
    gain_mix_grad, gain_mix_first_new, gain_mix_second_new, gain_mix_update = results[4]
    table_grad, table_first_new, table_second_new, table_update = results[5]
    gate_grad, gate_first_new, gate_second_new, gate_update = results[6]
    up_grad, up_first_new, up_second_new, up_update = results[7]
    down_grad, down_first_new, down_second_new, down_update = results[8]
    return (outputs.reshape(tokens.shape), grad_seq.reshape(tokens.shape), qkv_grad, out_grad, router_grad, gain_attn_grad, gain_mix_grad, table_grad, gate_grad, up_grad, down_grad, qkv_first_new, out_first_new, router_first_new, gain_attn_first_new, gain_mix_first_new, table_first_new, gate_first_new, up_first_new, down_first_new, qkv_second_new, out_second_new, router_second_new, gain_attn_second_new, gain_mix_second_new, table_second_new, gate_second_new, up_second_new, down_second_new, qkv_update, out_update, router_update, gain_attn_update, gain_mix_update, table_update, gate_update, up_update, down_update)
```

```python
from functools import partial

import jax
import jax.numpy as jnp
from jax import lax
from jax.experimental import pallas as pl
from jax.experimental.pallas import tpu as pltpu
from jax.sharding import PartitionSpec as P

D = 1024
HEADS = 16
HEAD_DIM = 64
TOP = 2
BLOCK = 256
STEP = 3
EXP_AXIS = 4

eps_norm = 1e-06
eps_adam = 1e-08
score_scale = 0.125
decay_rate = 0.5
learn_rate = 1.0
weight_decay = 0.1
highest = lax.Precision.HIGHEST
last_dims = (((1,), (1,)), ((), ()))
first_dims = (((0,), (0,)), ((), ()))
bf16 = jnp.bfloat16
f32 = jnp.float32
both = ("ctx", "exp")


def swap_bit(value, bit):
    count = lax.axis_size("ctx") * EXP_AXIS
    return lax.ppermute(value, both, [(d, d ^ (1 << bit)) for d in range(count)])


def flat_index():
    return lax.axis_index("ctx") * EXP_AXIS + lax.axis_index("exp")


def my_bit(bit):
    return (flat_index() >> bit) & 1


def turn(value):
    count = lax.axis_size("ctx") * EXP_AXIS

    def other(d):
        low, high = d & 1, (d >> 2) & 1
        return (d & ~5) | (low << 2) | high

    return lax.ppermute(value, both, [(d, other(d)) for d in range(count)])


def cube_gather(value, bits):
    out = value[None]
    for bit in bits:
        theirs = swap_bit(out, bit)
        low = my_bit(bit) == 0
        out = jnp.concatenate([jnp.where(low, out, theirs), jnp.where(low, theirs, out)], axis=0)
    return out


def cube_scatter(value, bits):
    for bit in bits:
        pairs = value.reshape((value.shape[0] // 2, 2) + value.shape[1:])
        mine = lax.dynamic_index_in_dim(pairs, my_bit(bit), 1, keepdims=False)
        theirs = lax.dynamic_index_in_dim(pairs, 1 - my_bit(bit), 1, keepdims=False)
        got = swap_bit(theirs, bit)
        value = (mine.astype(f32) + got.astype(f32)).astype(value.dtype)
    return value[0]


def pair_groups():
    count = lax.axis_size("ctx")
    return [[c for c in range(low, count, 2)] for low in range(2)]


def gather_expert(shard):
    moved = turn(shard)
    mine = lax.all_gather(moved, "ctx", axis=0, axis_index_groups=pair_groups())
    theirs = swap_bit(mine, 0)
    low = my_bit(0) == 0
    whole = jnp.stack([jnp.where(low, mine, theirs), jnp.where(low, theirs, mine)], axis=1)
    return whole.reshape(-1, shard.shape[1])


def scatter_expert(grad):
    half = lax.axis_size("ctx") // 2
    rows = grad.shape[0] // (2 * half)
    value = grad.reshape(half, 2, rows, grad.shape[1])
    mine = lax.dynamic_index_in_dim(value, my_bit(0), 1, keepdims=False)
    theirs = lax.dynamic_index_in_dim(value, 1 - my_bit(0), 1, keepdims=False)
    got = swap_bit(theirs.astype(bf16), 0)
    total = (mine.astype(f32) + got.astype(f32)).astype(bf16)
    part = lax.psum_scatter(total, "ctx", scatter_dimension=0, axis_index_groups=pair_groups())
    return turn(part)


def lane_mask(width, head, dtype):
    lane = lax.broadcasted_iota(jnp.int32, (1, width), 1)
    return ((lane // HEAD_DIM) == head).astype(dtype)


def fill_bias(ob_ref, head, bias, blocks):
    for d in range(blocks):
        first = (blocks - d - 1) * BLOCK
        window = ob_ref[0, pl.ds(head, 1), pl.ds(first, 2 * BLOCK)]
        wide = jnp.broadcast_to(window, (BLOCK, 2 * BLOCK))
        bias[d] = pltpu.roll(wide, 0, 1, stride=1, stride_axis=0)[:, BLOCK:]


def attend_kernel(blocks, heads, qkv_ref, ob_ref, att_ref, summed_ref, total_ref, bias, km, acc, tot):
    width = qkv_ref.shape[2]
    for head in range(heads):
        mask = lane_mask(width, head, bf16)
        wide_mask = lane_mask(width, head, f32)
        fill_bias(ob_ref, head, bias, blocks)
        km[...] = qkv_ref[1] * mask

        @pl.loop(0, blocks)
        def _(qb):
            rows = pl.ds(pl.multiple_of(qb * BLOCK, BLOCK), BLOCK)
            queries = qkv_ref[0, rows, :] * jnp.asarray(score_scale, bf16)
            acc[...] = jnp.zeros_like(acc)
            tot[...] = jnp.zeros_like(tot)

            @pl.loop(0, qb + 1)
            def _(kb):
                cols = pl.ds(pl.multiple_of(kb * BLOCK, BLOCK), BLOCK)
                score = lax.dot_general(queries, km[cols, :], last_dims, preferred_element_type=f32)
                expo = jnp.exp(score + bias[qb - kb])
                tot[...] += expo[:, :128] + expo[:, 128:]
                acc[...] += jnp.dot(
                    expo.astype(bf16), qkv_ref[2, cols, :], preferred_element_type=f32
                )

            total = jnp.sum(tot[...], axis=1, keepdims=True)
            summed = acc[...]
            if head == 0:
                summed_ref[rows, :] = summed * wide_mask
                total_ref[rows, :] = jnp.broadcast_to(total, summed.shape) * wide_mask
            else:
                summed_ref[rows, :] += summed * wide_mask
                total_ref[rows, :] += jnp.broadcast_to(total, summed.shape) * wide_mask

    @pl.loop(0, blocks)
    def _(qb):
        rows = pl.ds(pl.multiple_of(qb * BLOCK, BLOCK), BLOCK)
        att_ref[rows, :] = (summed_ref[rows, :] / total_ref[rows, :]).astype(bf16)


def attend(qkv, ob):
    _, length, width = qkv.shape
    lanes = min(width, 128)
    heads = lanes // HEAD_DIM
    steps = width // lanes
    blocks = length // BLOCK
    rows = pl.BlockSpec((length, lanes), lambda i: (0, i))
    return pl.pallas_call(
        partial(attend_kernel, blocks, heads),
        grid=(steps,),
        in_specs=[
            pl.BlockSpec((3, length, lanes), lambda i: (0, 0, i)),
            pl.BlockSpec((1, heads, 2 * length), lambda i: (i, 0, 0)),
        ],
        out_specs=[rows, rows, rows],
        out_shape=[
            jax.ShapeDtypeStruct((length, width), bf16),
            jax.ShapeDtypeStruct((length, width), f32),
            jax.ShapeDtypeStruct((length, width), f32),
        ],
        scratch_shapes=[
            pltpu.VMEM((blocks, BLOCK, BLOCK), f32),
            pltpu.VMEM((length, lanes), bf16),
            pltpu.VMEM((BLOCK, lanes), f32),
            pltpu.VMEM((BLOCK, 128), f32),
        ],
        compiler_params=pltpu.CompilerParams(vmem_limit_bytes=48 << 20),
        cost_estimate=pl.CostEstimate(
            flops=4 * length * length * width, bytes_accessed=20 * length * width, transcendentals=0
        ),
        name="attend",
    )(qkv, ob.reshape(steps, heads, 2 * length))


def attend_back_kernel(
    blocks, heads, qkv_ref, ob_ref, da_ref, summed_ref, total_ref, dqkv_ref, diag_ref,
    bias, diff, qm, km, dm, dt, acc_q, acc_k, acc_v,
):
    width = qkv_ref.shape[2]
    acc_q[...] = jnp.zeros_like(acc_q)
    acc_k[...] = jnp.zeros_like(acc_k)
    acc_v[...] = jnp.zeros_like(acc_v)
    for head in range(heads):
        mask = lane_mask(width, head, bf16)
        wide_mask = lane_mask(width, head, f32)
        fill_bias(ob_ref, head, bias, blocks)
        diff[...] = jnp.zeros_like(diff)
        qm[...] = qkv_ref[0] * (mask * jnp.asarray(score_scale, bf16))
        km[...] = qkv_ref[1] * mask

        @pl.loop(0, blocks)
        def _(qb):
            rows = pl.ds(pl.multiple_of(qb * BLOCK, BLOCK), BLOCK)
            grad = da_ref[rows, :].astype(f32)
            total = total_ref[rows, :]
            dm[rows, :] = (grad / total * wide_mask).astype(bf16)
            inner = jnp.sum(grad * summed_ref[rows, :] / (total * total) * wide_mask, axis=1, keepdims=True)
            dt[rows, :] = jnp.broadcast_to(-inner, (BLOCK, 128))

        @pl.loop(0, blocks)
        def _(qb):
            rows = pl.ds(pl.multiple_of(qb * BLOCK, BLOCK), BLOCK)
            queries = qm[rows, :]
            grads = dm[rows, :]
            shift = dt[rows, :][:, :1]

            @pl.loop(0, qb + 1)
            def _(kb):
                cols = pl.ds(pl.multiple_of(kb * BLOCK, BLOCK), BLOCK)
                keys = km[cols, :]
                score = lax.dot_general(queries, keys, last_dims, preferred_element_type=f32)
                expo = jnp.exp(score + bias[qb - kb])
                probs = lax.dot_general(
                    grads, qkv_ref[2, cols, :], last_dims, preferred_element_type=f32
                )
                dscore = (expo * (probs + shift)).astype(bf16)
                diff[qb - kb] += dscore.astype(f32)
                acc_q[rows, :] += jnp.dot(dscore, keys, preferred_element_type=f32)
                acc_k[cols, :] += lax.dot_general(
                    dscore, queries, first_dims, preferred_element_type=f32
                )
                acc_v[cols, :] += lax.dot_general(
                    expo.astype(bf16), grads, first_dims, preferred_element_type=f32
                )

        lower = lax.broadcasted_iota(jnp.int32, (8, 2 * BLOCK), 0)
        for d in range(blocks):

            def add_rows(i, fold):
                part = diff[d, pl.ds(pl.multiple_of(i * 8, 8), 8), :]
                wide = jnp.concatenate([jnp.zeros((8, BLOCK), f32), part], axis=1)
                return fold + pltpu.roll(wide, 2 * BLOCK - 8 * i, 1)

            fold = lax.fori_loop(0, BLOCK // 8, add_rows, jnp.zeros((8, 2 * BLOCK), f32))
            for bit in (1, 2, 4):
                fold = jnp.where((lower & bit) != 0, pltpu.roll(fold, 2 * BLOCK - bit, 1), fold)
            diag_ref[0, pl.ds(head * blocks + d, 1), :] = jnp.sum(fold, axis=0, keepdims=True)
    dqkv_ref[0] = (acc_q[...] * score_scale).astype(bf16)
    dqkv_ref[1] = acc_k[...].astype(bf16)
    dqkv_ref[2] = acc_v[...].astype(bf16)


def attend_back(qkv, ob, grad, summed, total):
    _, length, width = qkv.shape
    lanes = min(width, 128)
    heads = lanes // HEAD_DIM
    steps = width // lanes
    blocks = length // BLOCK
    rows = pl.BlockSpec((length, lanes), lambda i: (0, i))
    wide = pl.BlockSpec((3, length, lanes), lambda i: (0, 0, i))
    dqkv, diag = pl.pallas_call(
        partial(attend_back_kernel, blocks, heads),
        grid=(steps,),
        in_specs=[wide, pl.BlockSpec((1, heads, 2 * length), lambda i: (i, 0, 0)), rows, rows, rows],
        out_specs=[wide, pl.BlockSpec((1, heads * blocks, 2 * BLOCK), lambda i: (i, 0, 0))],
        out_shape=[
            jax.ShapeDtypeStruct((3, length, width), bf16),
            jax.ShapeDtypeStruct((steps, heads * blocks, 2 * BLOCK), f32),
        ],
        scratch_shapes=[
            pltpu.VMEM((blocks, BLOCK, BLOCK), f32),
            pltpu.VMEM((blocks, BLOCK, BLOCK), f32),
            pltpu.VMEM((length, lanes), bf16),
            pltpu.VMEM((length, lanes), bf16),
            pltpu.VMEM((length, lanes), bf16),
            pltpu.VMEM((length, 128), f32),
            pltpu.VMEM((length, lanes), f32),
            pltpu.VMEM((length, lanes), f32),
            pltpu.VMEM((length, lanes), f32),
        ],
        compiler_params=pltpu.CompilerParams(vmem_limit_bytes=56 << 20),
        cost_estimate=pl.CostEstimate(
            flops=10 * length * length * width, bytes_accessed=30 * length * width, transcendentals=0
        ),
        name="attend_back",
    )(qkv, ob.reshape(steps, heads, 2 * length), grad, summed, total)
    return dqkv, diag.reshape(steps * heads, blocks, 2 * BLOCK)


def norm_back(norm_input, factor, gain_wide, grad_normed):
    scaled = grad_normed * gain_wide
    gain_grad = jnp.sum(grad_normed * norm_input * factor, axis=(0, 1))
    mean_term = jnp.mean(scaled * norm_input, axis=-1, keepdims=True)
    return (factor * scaled - norm_input * factor * factor * factor * mean_term, gain_grad)


def adamw_step(master, gradient, first_old, second_old):
    first_new = decay_rate * first_old + (1.0 - decay_rate) * gradient
    second_new = decay_rate * second_old + (1.0 - decay_rate) * gradient * gradient
    correct = 1.0 - decay_rate**STEP
    update = -learn_rate * (
        first_new / correct / (jnp.sqrt(second_new / correct) + eps_adam) + weight_decay * master
    )
    return (gradient, first_new, second_new, update)


def body(tokens, cotangent, bucket_ids, routes, *state):
    masters, firsts, seconds = state[:9], state[9:18], state[18:]
    (
        qkv_master, out_master, router_master, gain_attn_master, gain_mix_master, table_master,
        gate_master, up_master, down_master,
    ) = masters
    micro, tok_rows = tokens.shape[0], tokens.shape[2]
    cycle = lax.axis_size("ctx")
    count = cycle * EXP_AXIS
    all_bits = list(range(count.bit_length() - 1))
    length = tok_rows * cycle
    group = cycle // micro
    width = D // group
    place = lax.axis_index("ctx")
    head_group = place % group
    rows = D // count
    table_rows = table_master.shape[0]
    experts_all = router_master.shape[1]
    capacity = 5 * tok_rows * TOP // (4 * experts_all)

    tok = tokens[:, 0]
    seq = lax.all_to_all(jnp.repeat(tok, group, axis=0), "ctx", 0, 0, tiled=True)
    seq = seq.reshape(length, D)

    cols = qkv_master.astype(bf16).reshape(3, rows, group, width).transpose(2, 0, 1, 3)
    cols = jnp.concatenate([cols] * micro, axis=0)
    cols = lax.all_to_all(cols, "ctx", 0, 0, tiled=True)
    cols = cube_gather(cols, (0, 1))
    w_qkv = cols.transpose(2, 1, 0, 3, 4).reshape(3, D, width)

    small = jnp.concatenate(
        [
            router_master.reshape(-1), gain_attn_master, gain_mix_master, table_master,
        ]
    ).astype(bf16)
    small = cube_gather(small, all_bits)
    edges = (0, rows * experts_all, rows * (experts_all + 1), rows * (experts_all + 2))
    router_bf = small[:, : edges[1]].reshape(D, experts_all)
    gain_attn = small[:, edges[1] : edges[2]].reshape(D).astype(f32)
    gain_mix = small[:, edges[2] : edges[3]].reshape(D).astype(f32)
    table = small[:, edges[3] :].reshape(HEADS, -1)
    bucket_count = table.shape[1]
    router_wide = router_bf.astype(f32)
    bucket_hits = bucket_ids[:, None] == jnp.arange(bucket_count, dtype=jnp.int32)[None, :]
    own_heads = HEADS // group
    own_table = lax.dynamic_slice_in_dim(table, head_group * own_heads, own_heads, 0)
    offset_bias = lax.dot_general(
        own_table, bucket_hits.astype(bf16), last_dims, preferred_element_type=f32
    )
    offset_bias = jnp.pad(offset_bias, ((0, 0), (1, 0)))[:, :-1]

    w_gate = gather_expert(gate_master[0].astype(bf16))
    w_up = gather_expert(up_master[0].astype(bf16))
    w_out = lax.all_gather(out_master.astype(bf16), both, axis=0, tiled=True)
    w_down = gather_expert(down_master[0].astype(bf16))

    seq_wide = seq.astype(f32)
    seq_factor = lax.rsqrt(jnp.mean(seq_wide * seq_wide, axis=-1, keepdims=True) + eps_norm)
    normed = (seq_wide * seq_factor * gain_attn).astype(bf16)
    qkv = jnp.einsum("td,cde->cte", normed, w_qkv, preferred_element_type=f32).astype(bf16)
    attended, summed, total = attend(qkv, offset_bias)

    back = lax.all_to_all(attended.reshape(cycle, tok_rows, width), "ctx", 0, 0, tiled=True)
    attended_bf = back.reshape(micro, group, tok_rows, width).transpose(0, 2, 1, 3)
    attended_bf = attended_bf.reshape(micro, tok_rows, D)
    inputs = tok.astype(f32)
    factor_attn = lax.rsqrt(jnp.mean(inputs * inputs, axis=-1, keepdims=True) + eps_norm)
    branch = jnp.dot(attended_bf, w_out, preferred_element_type=f32)
    hidden_state = inputs + branch
    factor_mix = lax.rsqrt(jnp.mean(hidden_state * hidden_state, axis=-1, keepdims=True) + eps_norm)
    normed_mix = hidden_state * factor_mix * gain_mix
    normed_bf = normed_mix.astype(bf16)
    logits = jnp.einsum("mtd,de->mte", normed_bf, router_bf, preferred_element_type=f32)
    router_probs = jax.nn.softmax(logits, axis=-1)
    route_rows = routes.reshape(micro, tok_rows, TOP)
    expert_ids = jnp.arange(experts_all, dtype=jnp.int32)
    picked = (route_rows[:, :, :, None] == expert_ids).astype(f32)
    chosen = jnp.sum(picked * router_probs[:, :, None, :], axis=-1)
    chosen_sum = jnp.sum(chosen, axis=-1, keepdims=True)
    gate_share = chosen / chosen_sum
    flat_routes = route_rows.reshape(micro, tok_rows * TOP)
    route_hits = (flat_routes[:, :, None] == expert_ids).astype(jnp.int32)
    before = jnp.cumsum(route_hits, axis=1) - route_hits
    slot_index = flat_routes * capacity + jnp.sum(before * route_hits, axis=-1)
    targets = expert_ids[:, None] * capacity + jnp.arange(capacity, dtype=jnp.int32)[None, :]
    dispatch = (slot_index[:, None, None, :] == targets[None, :, :, None]).astype(bf16)
    entries = jnp.repeat(normed_bf, TOP, axis=1)
    sent_rows = jnp.einsum("mect,mtd->emcd", dispatch, entries, preferred_element_type=f32)
    dy_rows = cotangent.reshape(micro, tok_rows, D).astype(f32)
    scaled_dy = (gate_share[:, :, :, None] * dy_rows[:, :, None, :]).astype(bf16)
    scaled_dy = scaled_dy.reshape(micro, tok_rows * TOP, D)
    sent_grads = jnp.einsum("mect,mtd->emcd", dispatch, scaled_dy, preferred_element_type=f32)

    def to_expert(value):
        return turn(lax.all_to_all(value.astype(bf16), "exp", 0, 0, tiled=True))

    def from_expert(value):
        return lax.all_to_all(turn(value), "exp", 0, 0, tiled=True)

    got_rows = to_expert(sent_rows)
    got_grads = to_expert(sent_grads)
    slots = got_rows.shape
    flat_rows = got_rows.reshape(-1, D)
    flat_grads = got_grads.reshape(-1, D)
    gate_pre = jnp.dot(flat_rows, w_gate, preferred_element_type=f32)
    up_pre = jnp.dot(flat_rows, w_up, preferred_element_type=f32)
    gelu_out, gelu_pull = jax.vjp(partial(jax.nn.gelu, approximate=True), gate_pre)
    units = (gelu_out * up_pre).astype(bf16)
    out_rows = jnp.dot(units, w_down, preferred_element_type=f32).astype(bf16)
    back_out = from_expert(out_rows.reshape(slots))
    grad_units = lax.dot_general(flat_grads, w_down, last_dims, preferred_element_type=f32)
    down_grad = lax.dot_general(units, flat_grads, first_dims, preferred_element_type=f32)
    grad_gate = gelu_pull(grad_units * up_pre)[0].astype(bf16)
    grad_up = (grad_units * gelu_out).astype(bf16)
    grad_rows = lax.dot_general(grad_gate, w_gate, last_dims, preferred_element_type=f32)
    grad_rows = grad_rows + lax.dot_general(grad_up, w_up, last_dims, preferred_element_type=f32)
    back_grad = from_expert(grad_rows.astype(bf16).reshape(slots))
    gate_grad = lax.dot_general(flat_rows, grad_gate, first_dims, preferred_element_type=f32)
    up_grad = lax.dot_general(flat_rows, grad_up, first_dims, preferred_element_type=f32)
    expert_sums = [
        scatter_expert(member.astype(bf16))[None].astype(f32)
        for member in (gate_grad, up_grad, down_grad)
    ]

    returned = jnp.einsum("mect,emcd->mtd", dispatch, back_out, preferred_element_type=f32)
    returned = returned.reshape(micro, tok_rows, TOP, D)
    mix_out = jnp.sum(gate_share[:, :, :, None] * returned, axis=2)
    output = (hidden_state + mix_out).astype(bf16)
    grad_entries = jnp.einsum("mect,emcd->mtd", dispatch, back_grad, preferred_element_type=f32)
    grad_entries = grad_entries.reshape(micro, tok_rows, TOP, D)
    grad_gates = jnp.sum(dy_rows[:, :, None, :] * returned, axis=-1)
    grad_chosen = grad_gates / chosen_sum - jnp.sum(grad_gates * chosen, axis=-1, keepdims=True) / (
        chosen_sum * chosen_sum
    )
    grad_probs = jnp.sum(grad_chosen[:, :, :, None] * picked, axis=2)
    grad_logits = router_probs * (
        grad_probs - jnp.sum(router_probs * grad_probs, axis=-1, keepdims=True)
    )
    router_grad = jnp.einsum("mtd,mte->de", normed_bf.astype(f32), grad_logits, precision=highest)
    grad_normed = jnp.sum(grad_entries, axis=2) + jnp.einsum(
        "mte,de->mtd", grad_logits, router_wide, precision=highest
    )
    grad_hidden, gain_mix_grad = norm_back(hidden_state, factor_mix, gain_mix, grad_normed)
    grad_hidden = grad_hidden + dy_rows
    grad_branch = grad_hidden.astype(bf16)
    grad_attended = jnp.einsum("mte,de->mtd", grad_branch, w_out, preferred_element_type=f32)
    grad_attended = grad_attended.astype(bf16).reshape(micro, tok_rows, group, width)
    grad_attended = grad_attended.transpose(0, 2, 1, 3).reshape(cycle, tok_rows, width)
    grad_attended = lax.all_to_all(grad_attended, "ctx", 0, 0, tiled=True).reshape(length, width)
    out_grad = jnp.einsum("mtd,mte->de", attended_bf, grad_branch, preferred_element_type=f32)
    out_sum = cube_scatter(out_grad.astype(bf16).reshape(count, rows, D), all_bits).astype(f32)

    dqkv, diag = attend_back(qkv, offset_bias, grad_attended, summed, total)
    partial_normed = jnp.einsum("cte,cde->td", dqkv, w_qkv, preferred_element_type=f32)
    partial_normed = partial_normed.astype(bf16).reshape(cycle, tok_rows, D)
    pieces = lax.all_to_all(partial_normed, "ctx", 0, 0, tiled=True)
    grad_normed_attn = jnp.sum(pieces.reshape(micro, group, tok_rows, D).astype(f32), axis=1)
    grad_inputs, gain_attn_grad = norm_back(inputs, factor_attn, gain_attn, grad_normed_attn)
    grad_inputs = grad_inputs + grad_hidden

    qkv_grad = jnp.einsum("td,cte->cde", normed, dqkv, preferred_element_type=f32)
    qkv_grad = qkv_grad.astype(bf16).reshape(3, cycle, EXP_AXIS, rows, width)
    qkv_grad = cube_scatter(qkv_grad.transpose(2, 1, 0, 3, 4), (0, 1))
    qkv_grad = lax.all_to_all(qkv_grad, "ctx", 0, 0, tiled=True)
    qkv_sum = jnp.sum(qkv_grad.reshape(micro, group, 3, rows, width).astype(f32), axis=0)
    qkv_sum = qkv_sum.transpose(1, 2, 0, 3).reshape(3, rows, D)

    blocks = length // BLOCK
    offset_grad = jnp.zeros((own_heads, 2 * length), f32)
    for d in range(blocks):
        first = (blocks - d - 1) * BLOCK
        offset_grad = offset_grad + jnp.pad(
            diag[:, d], ((0, 0), (first, 2 * length - first - 2 * BLOCK))
        )
    offset_grad = jnp.pad(offset_grad[:, 1:], ((0, 0), (0, 1)))
    own_grad = jnp.dot(offset_grad, bucket_hits.astype(f32), precision=highest)
    table_grad = lax.dynamic_update_slice_in_dim(
        jnp.zeros((HEADS, bucket_count), f32), own_grad, head_group * own_heads, 0
    )
    small_grads = jnp.concatenate(
        [
            router_grad.reshape(count, -1), gain_attn_grad.reshape(count, -1),
            gain_mix_grad.reshape(count, -1), table_grad.reshape(count, -1),
        ],
        axis=1,
    )
    small_sum = cube_scatter(small_grads, all_bits)
    gradients = (
        qkv_sum,
        out_sum,
        small_sum[: edges[1]].reshape(rows, experts_all),
        small_sum[edges[1] : edges[2]],
        small_sum[edges[2] : edges[3]],
        small_sum[edges[3] :],
        *expert_sums,
    )
    results = [
        adamw_step(master, gradient, first_old, second_old)
        for master, gradient, first_old, second_old in zip(masters, gradients, firsts, seconds)
    ]
    flat = [result[kind] for kind in range(4) for result in results]
    return (output.reshape(tokens.shape), grad_inputs.reshape(tokens.shape), *flat)


def solution(mesh):
    token_spec = P(None, "exp", "ctx", None)
    weight_specs = (
        P(None, both, None), P(both, None), P(both, None), P(both), P(both), P(both),
        P("exp", "ctx", None), P("exp", "ctx", None), P("exp", "ctx", None),
    )
    return jax.shard_map(
        body,
        mesh=mesh,
        in_specs=(token_spec, token_spec, P(), token_spec) + weight_specs * 3,
        out_specs=(token_spec, token_spec) + weight_specs * 4,
        check_vma=False,
    )
```

```python
from functools import partial

import jax
import jax.numpy as jnp
from jax import lax
from jax.experimental import pallas as pl
from jax.experimental.pallas import tpu as pltpu
from jax.sharding import PartitionSpec as P

D = 1024
HEADS = 16
HEAD_DIM = 64
TOP = 2
BLOCK = 256
STEP = 3
EXP_AXIS = 4

eps_norm = 1e-06
eps_adam = 1e-08
score_scale = 0.125
decay_rate = 0.5
learn_rate = 1.0
weight_decay = 0.1
highest = lax.Precision.HIGHEST
last_dims = (((1,), (1,)), ((), ()))
first_dims = (((0,), (0,)), ((), ()))
bf16 = jnp.bfloat16
f32 = jnp.float32
both = ("ctx", "exp")
MESH = pl.DeviceIdType.MESH


def swap_bit(value, bit):
    count = lax.axis_size("ctx") * EXP_AXIS
    return lax.ppermute(value, both, [(d, d ^ (1 << bit)) for d in range(count)])


def flat_index():
    return lax.axis_index("ctx") * EXP_AXIS + lax.axis_index("exp")


def my_bit(bit):
    return (flat_index() >> bit) & 1


def turn(value):
    count = lax.axis_size("ctx") * EXP_AXIS

    def other(d):
        low, high = d & 1, (d >> 2) & 1
        return (d & ~5) | (low << 2) | high

    got = lax.ppermute(value, both, [(d, other(d)) for d in range(count) if other(d) != d])
    return jnp.where(my_bit(0) == my_bit(2), value, got)


def place_of(flat):
    return (flat // EXP_AXIS, flat % EXP_AXIS)


def greet(partners):
    barrier = pltpu.get_barrier_semaphore()
    for partner in partners:
        pl.semaphore_signal(barrier, inc=1, device_id=place_of(partner), device_id_type=MESH)
    pl.semaphore_wait(barrier, len(partners))


def remote(source, target, send, recv, partner):
    return pltpu.make_async_remote_copy(
        src_ref=source, dst_ref=target, send_sem=send, recv_sem=recv,
        device_id=place_of(partner), device_id_type=MESH,
    )


def exchange_call(kernel, name, number, arrays, shapes, sems):
    vmem = pl.BlockSpec(memory_space=pltpu.VMEM)
    sent = sum(array.size * array.dtype.itemsize for array in arrays)
    return pl.pallas_call(
        kernel,
        in_specs=[vmem] * len(arrays),
        out_specs=[vmem] * len(shapes),
        out_shape=shapes,
        scratch_shapes=[pltpu.SemaphoreType.DMA((size,)) for size in sems],
        compiler_params=pltpu.CompilerParams(
            collective_id=number, has_side_effects=True, vmem_limit_bytes=48 << 20
        ),
        cost_estimate=pl.CostEstimate(flops=0, bytes_accessed=8 * sent, transcendentals=0),
        name=name,
    )(*arrays)


def opening_kernel(cycle, group, tok_ref, col_ref, seq_ref, all_ref, s1, r1, s2, r2, s3, r3):
    me = flat_index()
    ctx, exp = place_of(me)
    greet([me ^ (rel * EXP_AXIS) for rel in range(1, cycle)] + [me ^ rel for rel in range(1, EXP_AXIS)])
    copies = []
    for rel in range(1, cycle):
        peer = ctx ^ rel
        copies.append(
            remote(
                col_ref.at[lax.rem(peer, group)], all_ref.at[exp, ctx], s1.at[rel], r1.at[rel],
                me ^ (rel * EXP_AXIS),
            )
        )
        copies[-1].start()
    tokens = []
    for rel in range(1, cycle):
        peer = ctx ^ rel
        tokens.append(
            remote(
                tok_ref.at[peer // group], seq_ref.at[ctx], s2.at[rel], r2.at[rel],
                me ^ (rel * EXP_AXIS),
            )
        )
        tokens[-1].start()
    all_ref[exp, ctx] = col_ref[lax.rem(ctx, group)]
    seq_ref[ctx] = tok_ref[ctx // group]
    for copy in copies:
        copy.wait()
    forwards = []
    for rel in range(1, EXP_AXIS):
        forwards.append(
            remote(all_ref.at[exp], all_ref.at[exp], s3.at[rel], r3.at[rel], me ^ rel)
        )
        forwards[-1].start()
    for copy in tokens + forwards:
        copy.wait()


def opening(tok, cols):
    cycle = lax.axis_size("ctx")
    group = cycle // tok.shape[0]
    return exchange_call(
        partial(opening_kernel, cycle, group), "opening", 0, [tok, cols],
        [
            jax.ShapeDtypeStruct((cycle,) + tok.shape[1:], tok.dtype),
            jax.ShapeDtypeStruct((EXP_AXIS, cycle) + cols.shape[1:], cols.dtype),
        ],
        [cycle, cycle, cycle, cycle, EXP_AXIS, EXP_AXIS],
    )


def cycle_kernel(cycle, in_ref, out_ref, send, recv):
    me = flat_index()
    ctx, _ = place_of(me)
    greet([me ^ (rel * EXP_AXIS) for rel in range(1, cycle)])
    copies = []
    for rel in range(1, cycle):
        copies.append(
            remote(
                in_ref.at[ctx ^ rel], out_ref.at[ctx], send.at[rel], recv.at[rel],
                me ^ (rel * EXP_AXIS),
            )
        )
        copies[-1].start()
    out_ref[ctx] = in_ref[ctx]
    for copy in copies:
        copy.wait()


def cycle_swap(value, name, number):
    cycle = lax.axis_size("ctx")
    return exchange_call(
        partial(cycle_kernel, cycle), name, number, [value],
        [jax.ShapeDtypeStruct(value.shape, value.dtype)], [cycle, cycle],
    )[0]


def closing_kernel(cycle, col_ref, small_ref, out_ref, all_ref, s1, r1, s2, r2):
    me = flat_index()
    ctx, _ = place_of(me)
    count = cycle * EXP_AXIS
    greet([me ^ rel for rel in range(1, count)])
    copies = []
    for rel in range(1, cycle):
        copies.append(
            remote(
                col_ref.at[ctx ^ rel], out_ref.at[ctx], s1.at[rel], r1.at[rel], me ^ (rel * EXP_AXIS)
            )
        )
        copies[-1].start()
    for rel in range(1, count):
        copies.append(
            remote(small_ref.at[me ^ rel], all_ref.at[me], s2.at[rel], r2.at[rel], me ^ rel)
        )
        copies[-1].start()
    out_ref[ctx] = col_ref[ctx]
    all_ref[me] = small_ref[me]
    for copy in copies:
        copy.wait()


def closing(cols, small):
    cycle = lax.axis_size("ctx")
    count = cycle * EXP_AXIS
    return exchange_call(
        partial(closing_kernel, cycle), "closing", 6, [cols, small],
        [jax.ShapeDtypeStruct(x.shape, x.dtype) for x in (cols, small)],
        [cycle, cycle, count, count],
    )


def plane_kernel(forward, arrays, *refs):
    ins, outs, send, recv = refs[:arrays], refs[arrays : 2 * arrays], refs[-2], refs[-1]
    me = flat_index()
    ctx, exp = place_of(me)
    greet([me ^ rel for rel in range(1, 2 * EXP_AXIS)])
    base = (ctx // 2) * 2
    ctx_low, exp_low = lax.rem(ctx, 2), lax.rem(exp, 2)
    for index in range(arrays):
        for e in range(EXP_AXIS):
            own = jnp.logical_and(exp == e, ctx_low == exp_low)
            sem = index * EXP_AXIS
            if forward:
                to_ctx, to_exp = base + e % 2, (e // 2) * 2 + ctx_low
                slot = exp
            else:
                to_ctx, to_exp = base + exp_low, e
                slot = (exp // 2) * 2 + ctx_low
            copy = remote(
                ins[index].at[e], outs[index].at[slot], send.at[sem + e], recv.at[sem + slot],
                to_ctx * EXP_AXIS + to_exp,
            )

            @pl.when(jnp.logical_not(own))
            def _():
                copy.start()

            @pl.when(own)
            def _():
                outs[index][e] = ins[index][e]

    for index in range(arrays):
        for e in range(EXP_AXIS):
            own = jnp.logical_and(exp == e, ctx_low == exp_low)
            sem = index * EXP_AXIS + e
            done = remote(ins[index].at[e], outs[index].at[e], send.at[sem], recv.at[sem], me ^ 1)

            @pl.when(jnp.logical_not(own))
            def _():
                done.wait()


def plane_swap(values, forward, name, number):
    count = len(values)
    return exchange_call(
        partial(plane_kernel, forward, count), name, number, list(values),
        [jax.ShapeDtypeStruct(x.shape, x.dtype) for x in values],
        [count * EXP_AXIS, count * EXP_AXIS],
    )


def cube_gather(value, bits):
    out = value[None]
    for bit in bits:
        theirs = swap_bit(out, bit)
        low = my_bit(bit) == 0
        out = jnp.concatenate([jnp.where(low, out, theirs), jnp.where(low, theirs, out)], axis=0)
    return out


def cube_gather_high(value, bits):
    out = value[None]
    for bit in reversed(bits):
        theirs = swap_bit(out, bit)
        low = my_bit(bit) == 0
        out = jnp.stack([jnp.where(low, out, theirs), jnp.where(low, theirs, out)], axis=1)
        out = out.reshape((-1,) + value.shape)
    return out


def cube_scatter(value, bits):
    for bit in bits:
        pairs = value.reshape((value.shape[0] // 2, 2) + value.shape[1:])
        mine = lax.dynamic_index_in_dim(pairs, my_bit(bit), 1, keepdims=False)
        theirs = lax.dynamic_index_in_dim(pairs, 1 - my_bit(bit), 1, keepdims=False)
        got = swap_bit(theirs, bit)
        value = (mine.astype(f32) + got.astype(f32)).astype(value.dtype)
    return value[0]


def pair_groups():
    count = lax.axis_size("ctx")
    return [[c for c in range(low, count, 2)] for low in range(2)]


def gather_expert(shard):
    moved = turn(shard)
    mine = lax.all_gather(moved, "ctx", axis=0, axis_index_groups=pair_groups())
    theirs = swap_bit(mine, 0)
    low = my_bit(0) == 0
    whole = jnp.stack([jnp.where(low, mine, theirs), jnp.where(low, theirs, mine)], axis=1)
    return whole.reshape(-1, shard.shape[1])


def scatter_expert(grad):
    half = lax.axis_size("ctx") // 2
    rows = grad.shape[0] // (2 * half)
    value = grad.reshape(half, 2, rows, grad.shape[1])
    mine = lax.dynamic_index_in_dim(value, my_bit(0), 1, keepdims=False)
    theirs = lax.dynamic_index_in_dim(value, 1 - my_bit(0), 1, keepdims=False)
    got = swap_bit(theirs.astype(bf16), 0)
    total = (mine.astype(f32) + got.astype(f32)).astype(bf16)
    part = lax.psum_scatter(total, "ctx", scatter_dimension=0, axis_index_groups=pair_groups())
    return turn(part)


def lane_mask(width, head, dtype):
    lane = lax.broadcasted_iota(jnp.int32, (1, width), 1)
    return ((lane // HEAD_DIM) == head).astype(dtype)


def fill_bias(ob_ref, head, bias, blocks):
    for d in range(blocks):
        first = (blocks - d - 1) * BLOCK
        window = ob_ref[0, pl.ds(head, 1), pl.ds(first, 2 * BLOCK)]
        wide = jnp.broadcast_to(window, (BLOCK, 2 * BLOCK))
        bias[d] = pltpu.roll(wide, 0, 1, stride=1, stride_axis=0)[:, BLOCK:]


def attend_kernel(blocks, heads, qkv_ref, ob_ref, att_ref, summed_ref, total_ref, bias, km, acc, tot):
    width = qkv_ref.shape[2]
    for head in range(heads):
        mask = lane_mask(width, head, bf16)
        wide_mask = lane_mask(width, head, f32)
        fill_bias(ob_ref, head, bias, blocks)
        km[...] = qkv_ref[1] * mask

        @pl.loop(0, blocks)
        def _(qb):
            rows = pl.ds(pl.multiple_of(qb * BLOCK, BLOCK), BLOCK)
            queries = qkv_ref[0, rows, :] * jnp.asarray(score_scale, bf16)
            acc[...] = jnp.zeros_like(acc)
            tot[...] = jnp.zeros_like(tot)

            @pl.loop(0, qb + 1)
            def _(kb):
                cols = pl.ds(pl.multiple_of(kb * BLOCK, BLOCK), BLOCK)
                score = lax.dot_general(queries, km[cols, :], last_dims, preferred_element_type=f32)
                expo = jnp.exp(score + bias[qb - kb])
                tot[...] += expo[:, :128] + expo[:, 128:]
                acc[...] += jnp.dot(
                    expo.astype(bf16), qkv_ref[2, cols, :], preferred_element_type=f32
                )

            total = jnp.sum(tot[...], axis=1, keepdims=True)
            summed = acc[...]
            if head == 0:
                summed_ref[rows, :] = summed * wide_mask
                total_ref[rows, :] = jnp.broadcast_to(total, summed.shape) * wide_mask
            else:
                summed_ref[rows, :] += summed * wide_mask
                total_ref[rows, :] += jnp.broadcast_to(total, summed.shape) * wide_mask

    @pl.loop(0, blocks)
    def _(qb):
        rows = pl.ds(pl.multiple_of(qb * BLOCK, BLOCK), BLOCK)
        att_ref[rows, :] = (summed_ref[rows, :] / total_ref[rows, :]).astype(bf16)


def attend(qkv, ob):
    _, length, width = qkv.shape
    lanes = min(width, 128)
    heads = lanes // HEAD_DIM
    steps = width // lanes
    blocks = length // BLOCK
    rows = pl.BlockSpec((length, lanes), lambda i: (0, i))
    return pl.pallas_call(
        partial(attend_kernel, blocks, heads),
        grid=(steps,),
        in_specs=[
            pl.BlockSpec((3, length, lanes), lambda i: (0, 0, i)),
            pl.BlockSpec((1, heads, 2 * length), lambda i: (i, 0, 0)),
        ],
        out_specs=[rows, rows, rows],
        out_shape=[
            jax.ShapeDtypeStruct((length, width), bf16),
            jax.ShapeDtypeStruct((length, width), f32),
            jax.ShapeDtypeStruct((length, width), f32),
        ],
        scratch_shapes=[
            pltpu.VMEM((blocks, BLOCK, BLOCK), f32),
            pltpu.VMEM((length, lanes), bf16),
            pltpu.VMEM((BLOCK, lanes), f32),
            pltpu.VMEM((BLOCK, 128), f32),
        ],
        compiler_params=pltpu.CompilerParams(vmem_limit_bytes=48 << 20),
        cost_estimate=pl.CostEstimate(
            flops=4 * length * length * width, bytes_accessed=20 * length * width, transcendentals=0
        ),
        name="attend",
    )(qkv, ob.reshape(steps, heads, 2 * length))


def attend_back_kernel(
    blocks, heads, qkv_ref, ob_ref, da_ref, summed_ref, total_ref, dqkv_ref, diag_ref,
    bias, diff, qm, km, dm, dt, acc_q, acc_k, acc_v,
):
    width = qkv_ref.shape[2]
    acc_q[...] = jnp.zeros_like(acc_q)
    acc_k[...] = jnp.zeros_like(acc_k)
    acc_v[...] = jnp.zeros_like(acc_v)
    for head in range(heads):
        mask = lane_mask(width, head, bf16)
        wide_mask = lane_mask(width, head, f32)
        fill_bias(ob_ref, head, bias, blocks)
        diff[...] = jnp.zeros_like(diff)
        qm[...] = qkv_ref[0] * (mask * jnp.asarray(score_scale, bf16))
        km[...] = qkv_ref[1] * mask

        @pl.loop(0, blocks)
        def _(qb):
            rows = pl.ds(pl.multiple_of(qb * BLOCK, BLOCK), BLOCK)
            grad = da_ref[rows, :].astype(f32)
            total = total_ref[rows, :]
            dm[rows, :] = (grad / total * wide_mask).astype(bf16)
            inner = jnp.sum(grad * summed_ref[rows, :] / (total * total) * wide_mask, axis=1, keepdims=True)
            dt[rows, :] = jnp.broadcast_to(-inner, (BLOCK, 128))

        @pl.loop(0, blocks)
        def _(qb):
            rows = pl.ds(pl.multiple_of(qb * BLOCK, BLOCK), BLOCK)
            queries = qm[rows, :]
            grads = dm[rows, :]
            shift = dt[rows, :][:, :1]

            @pl.loop(0, qb + 1)
            def _(kb):
                cols = pl.ds(pl.multiple_of(kb * BLOCK, BLOCK), BLOCK)
                keys = km[cols, :]
                score = lax.dot_general(queries, keys, last_dims, preferred_element_type=f32)
                expo = jnp.exp(score + bias[qb - kb])
                probs = lax.dot_general(
                    grads, qkv_ref[2, cols, :], last_dims, preferred_element_type=f32
                )
                dscore = (expo * (probs + shift)).astype(bf16)
                diff[qb - kb] += dscore.astype(f32)
                acc_q[rows, :] += jnp.dot(dscore, keys, preferred_element_type=f32)
                acc_k[cols, :] += lax.dot_general(
                    dscore, queries, first_dims, preferred_element_type=f32
                )
                acc_v[cols, :] += lax.dot_general(
                    expo.astype(bf16), grads, first_dims, preferred_element_type=f32
                )

        lower = lax.broadcasted_iota(jnp.int32, (8, 2 * BLOCK), 0)
        for d in range(blocks):

            def add_rows(i, fold):
                part = diff[d, pl.ds(pl.multiple_of(i * 8, 8), 8), :]
                wide = jnp.concatenate([jnp.zeros((8, BLOCK), f32), part], axis=1)
                return fold + pltpu.roll(wide, 2 * BLOCK - 8 * i, 1)

            fold = lax.fori_loop(0, BLOCK // 8, add_rows, jnp.zeros((8, 2 * BLOCK), f32))
            for bit in (1, 2, 4):
                fold = jnp.where((lower & bit) != 0, pltpu.roll(fold, 2 * BLOCK - bit, 1), fold)
            diag_ref[0, pl.ds(head * blocks + d, 1), :] = jnp.sum(fold, axis=0, keepdims=True)
    dqkv_ref[0] = (acc_q[...] * score_scale).astype(bf16)
    dqkv_ref[1] = acc_k[...].astype(bf16)
    dqkv_ref[2] = acc_v[...].astype(bf16)


def attend_back(qkv, ob, grad, summed, total):
    _, length, width = qkv.shape
    lanes = min(width, 128)
    heads = lanes // HEAD_DIM
    steps = width // lanes
    blocks = length // BLOCK
    rows = pl.BlockSpec((length, lanes), lambda i: (0, i))
    wide = pl.BlockSpec((3, length, lanes), lambda i: (0, 0, i))
    dqkv, diag = pl.pallas_call(
        partial(attend_back_kernel, blocks, heads),
        grid=(steps,),
        in_specs=[wide, pl.BlockSpec((1, heads, 2 * length), lambda i: (i, 0, 0)), rows, rows, rows],
        out_specs=[wide, pl.BlockSpec((1, heads * blocks, 2 * BLOCK), lambda i: (i, 0, 0))],
        out_shape=[
            jax.ShapeDtypeStruct((3, length, width), bf16),
            jax.ShapeDtypeStruct((steps, heads * blocks, 2 * BLOCK), f32),
        ],
        scratch_shapes=[
            pltpu.VMEM((blocks, BLOCK, BLOCK), f32),
            pltpu.VMEM((blocks, BLOCK, BLOCK), f32),
            pltpu.VMEM((length, lanes), bf16),
            pltpu.VMEM((length, lanes), bf16),
            pltpu.VMEM((length, lanes), bf16),
            pltpu.VMEM((length, 128), f32),
            pltpu.VMEM((length, lanes), f32),
            pltpu.VMEM((length, lanes), f32),
            pltpu.VMEM((length, lanes), f32),
        ],
        compiler_params=pltpu.CompilerParams(vmem_limit_bytes=56 << 20),
        cost_estimate=pl.CostEstimate(
            flops=10 * length * length * width, bytes_accessed=30 * length * width, transcendentals=0
        ),
        name="attend_back",
    )(qkv, ob.reshape(steps, heads, 2 * length), grad, summed, total)
    return dqkv, diag.reshape(steps * heads, blocks, 2 * BLOCK)


def norm_back(norm_input, factor, gain_wide, grad_normed):
    scaled = grad_normed * gain_wide
    gain_grad = jnp.sum(grad_normed * norm_input * factor, axis=(0, 1))
    mean_term = jnp.mean(scaled * norm_input, axis=-1, keepdims=True)
    return (factor * scaled - norm_input * factor * factor * factor * mean_term, gain_grad)


def adamw_step(master, gradient, first_old, second_old):
    first_new = decay_rate * first_old + (1.0 - decay_rate) * gradient
    second_new = decay_rate * second_old + (1.0 - decay_rate) * gradient * gradient
    correct = 1.0 - decay_rate**STEP
    update = -learn_rate * (
        first_new / correct / (jnp.sqrt(second_new / correct) + eps_adam) + weight_decay * master
    )
    return (gradient, first_new, second_new, update)


def body(tokens, cotangent, bucket_ids, routes, *state):
    masters, firsts, seconds = state[:9], state[9:18], state[18:]
    (
        qkv_master, out_master, router_master, gain_attn_master, gain_mix_master, table_master,
        gate_master, up_master, down_master,
    ) = masters
    micro, tok_rows = tokens.shape[0], tokens.shape[2]
    cycle = lax.axis_size("ctx")
    count = cycle * EXP_AXIS
    all_bits = list(range(count.bit_length() - 1))
    length = tok_rows * cycle
    group = cycle // micro
    width = D // group
    place = lax.axis_index("ctx")
    head_group = place % group
    rows = D // count
    table_rows = table_master.shape[0]
    experts_all = router_master.shape[1]
    capacity = 5 * tok_rows * TOP // (4 * experts_all)

    tok = tokens[:, 0]
    cols = qkv_master.astype(bf16).reshape(3 * rows, group, width).transpose(1, 0, 2)
    small = jnp.concatenate(
        [
            router_master.reshape(-1), gain_attn_master, gain_mix_master, table_master,
        ]
    ).astype(bf16)
    small_size = small.shape[0]
    small = jnp.pad(small, (0, 16 * width - small_size)).reshape(1, 16, width)
    cols = jnp.concatenate([cols, jnp.broadcast_to(small, (group, 16, width))], axis=1)
    seq, gathered = opening(tok, cols)
    seq = seq.reshape(length, D)
    w_qkv = gathered[:, :, : 3 * rows].reshape(EXP_AXIS, cycle, 3, rows, width)
    w_qkv = w_qkv.transpose(2, 1, 0, 3, 4).reshape(3, D, width)
    small = gathered[:, :, 3 * rows :].reshape(EXP_AXIS, cycle, 16 * width)[:, :, :small_size]
    small = small.transpose(1, 0, 2).reshape(count, small_size)
    edges = (0, rows * experts_all, rows * (experts_all + 1), rows * (experts_all + 2))
    router_bf = small[:, : edges[1]].reshape(D, experts_all)
    gain_attn = small[:, edges[1] : edges[2]].reshape(D).astype(f32)
    gain_mix = small[:, edges[2] : edges[3]].reshape(D).astype(f32)
    table = small[:, edges[3] :].reshape(HEADS, -1)
    bucket_count = table.shape[1]
    router_wide = router_bf.astype(f32)
    bucket_hits = bucket_ids[:, None] == jnp.arange(bucket_count, dtype=jnp.int32)[None, :]
    own_heads = HEADS // group
    own_table = lax.dynamic_slice_in_dim(table, head_group * own_heads, own_heads, 0)
    offset_bias = lax.dot_general(
        own_table, bucket_hits.astype(bf16), last_dims, preferred_element_type=f32
    )
    offset_bias = jnp.pad(offset_bias, ((0, 0), (1, 0)))[:, :-1]

    w_gate = gather_expert(gate_master[0].astype(bf16))
    w_up = gather_expert(up_master[0].astype(bf16))
    w_out = cube_gather_high(out_master.astype(bf16), all_bits).reshape(D, D)
    w_down = gather_expert(down_master[0].astype(bf16))

    seq_wide = seq.astype(f32)
    seq_factor = lax.rsqrt(jnp.mean(seq_wide * seq_wide, axis=-1, keepdims=True) + eps_norm)
    normed = (seq_wide * seq_factor * gain_attn).astype(bf16)
    qkv = jnp.einsum("td,cde->cte", normed, w_qkv, preferred_element_type=f32).astype(bf16)
    attended, summed, total = attend(qkv, offset_bias)

    back = cycle_swap(attended.reshape(cycle, tok_rows, width), "attended_swap", 1)
    attended_bf = back.reshape(micro, group, tok_rows, width).transpose(0, 2, 1, 3)
    attended_bf = attended_bf.reshape(micro, tok_rows, D)
    inputs = tok.astype(f32)
    factor_attn = lax.rsqrt(jnp.mean(inputs * inputs, axis=-1, keepdims=True) + eps_norm)
    branch = jnp.dot(attended_bf, w_out, preferred_element_type=f32)
    hidden_state = inputs + branch
    factor_mix = lax.rsqrt(jnp.mean(hidden_state * hidden_state, axis=-1, keepdims=True) + eps_norm)
    normed_mix = hidden_state * factor_mix * gain_mix
    normed_bf = normed_mix.astype(bf16)
    logits = jnp.einsum("mtd,de->mte", normed_bf, router_bf, preferred_element_type=f32)
    router_probs = jax.nn.softmax(logits, axis=-1)
    route_rows = routes.reshape(micro, tok_rows, TOP)
    expert_ids = jnp.arange(experts_all, dtype=jnp.int32)
    picked = (route_rows[:, :, :, None] == expert_ids).astype(f32)
    chosen = jnp.sum(picked * router_probs[:, :, None, :], axis=-1)
    chosen_sum = jnp.sum(chosen, axis=-1, keepdims=True)
    gate_share = chosen / chosen_sum
    flat_routes = route_rows.reshape(micro, tok_rows * TOP)
    route_hits = (flat_routes[:, :, None] == expert_ids).astype(jnp.int32)
    before = jnp.cumsum(route_hits, axis=1) - route_hits
    slot_index = flat_routes * capacity + jnp.sum(before * route_hits, axis=-1)
    targets = expert_ids[:, None] * capacity + jnp.arange(capacity, dtype=jnp.int32)[None, :]
    dispatch = (slot_index[:, None, None, :] == targets[None, :, :, None]).astype(bf16)
    entries = jnp.repeat(normed_bf, TOP, axis=1)
    sent_rows = jnp.einsum("mect,mtd->emcd", dispatch, entries, preferred_element_type=f32)
    dy_rows = cotangent.reshape(micro, tok_rows, D).astype(f32)
    scaled_dy = (gate_share[:, :, :, None] * dy_rows[:, :, None, :]).astype(bf16)
    scaled_dy = scaled_dy.reshape(micro, tok_rows * TOP, D)
    sent_grads = jnp.einsum("mect,mtd->emcd", dispatch, scaled_dy, preferred_element_type=f32)

    got_rows, got_grads = plane_swap(
        (sent_rows.astype(bf16), sent_grads.astype(bf16)), True, "dispatch_swap", 2
    )
    slots = got_rows.shape
    flat_rows = got_rows.reshape(-1, D)
    flat_grads = got_grads.reshape(-1, D)
    gate_pre = jnp.dot(flat_rows, w_gate, preferred_element_type=f32)
    up_pre = jnp.dot(flat_rows, w_up, preferred_element_type=f32)
    gelu_out, gelu_pull = jax.vjp(partial(jax.nn.gelu, approximate=True), gate_pre)
    units = (gelu_out * up_pre).astype(bf16)
    out_rows = jnp.dot(units, w_down, preferred_element_type=f32).astype(bf16)
    grad_units = lax.dot_general(flat_grads, w_down, last_dims, preferred_element_type=f32)
    down_grad = lax.dot_general(units, flat_grads, first_dims, preferred_element_type=f32)
    grad_gate = gelu_pull(grad_units * up_pre)[0].astype(bf16)
    grad_up = (grad_units * gelu_out).astype(bf16)
    grad_rows = lax.dot_general(grad_gate, w_gate, last_dims, preferred_element_type=f32)
    grad_rows = grad_rows + lax.dot_general(grad_up, w_up, last_dims, preferred_element_type=f32)
    back_out, back_grad = plane_swap(
        (out_rows.reshape(slots), grad_rows.astype(bf16).reshape(slots)), False, "return_swap", 3
    )
    gate_grad = lax.dot_general(flat_rows, grad_gate, first_dims, preferred_element_type=f32)
    up_grad = lax.dot_general(flat_rows, grad_up, first_dims, preferred_element_type=f32)
    expert_sums = [
        scatter_expert(member.astype(bf16))[None].astype(f32)
        for member in (gate_grad, up_grad, down_grad)
    ]

    returned = jnp.einsum("mect,emcd->mtd", dispatch, back_out, preferred_element_type=f32)
    returned = returned.reshape(micro, tok_rows, TOP, D)
    mix_out = jnp.sum(gate_share[:, :, :, None] * returned, axis=2)
    output = (hidden_state + mix_out).astype(bf16)
    grad_entries = jnp.einsum("mect,emcd->mtd", dispatch, back_grad, preferred_element_type=f32)
    grad_entries = grad_entries.reshape(micro, tok_rows, TOP, D)
    grad_gates = jnp.sum(dy_rows[:, :, None, :] * returned, axis=-1)
    grad_chosen = grad_gates / chosen_sum - jnp.sum(grad_gates * chosen, axis=-1, keepdims=True) / (
        chosen_sum * chosen_sum
    )
    grad_probs = jnp.sum(grad_chosen[:, :, :, None] * picked, axis=2)
    grad_logits = router_probs * (
        grad_probs - jnp.sum(router_probs * grad_probs, axis=-1, keepdims=True)
    )
    router_grad = jnp.einsum("mtd,mte->de", normed_bf.astype(f32), grad_logits, precision=highest)
    grad_normed = jnp.sum(grad_entries, axis=2) + jnp.einsum(
        "mte,de->mtd", grad_logits, router_wide, precision=highest
    )
    grad_hidden, gain_mix_grad = norm_back(hidden_state, factor_mix, gain_mix, grad_normed)
    grad_hidden = grad_hidden + dy_rows
    grad_branch = grad_hidden.astype(bf16)
    grad_attended = jnp.einsum("mte,de->mtd", grad_branch, w_out, preferred_element_type=f32)
    grad_attended = grad_attended.astype(bf16).reshape(micro, tok_rows, group, width)
    grad_attended = grad_attended.transpose(0, 2, 1, 3).reshape(cycle, tok_rows, width)
    grad_attended = cycle_swap(grad_attended, "grad_swap", 4).reshape(length, width)
    out_grad = jnp.einsum("mtd,mte->de", attended_bf, grad_branch, preferred_element_type=f32)
    out_sum = cube_scatter(out_grad.astype(bf16).reshape(count, rows, D), all_bits).astype(f32)

    dqkv, diag = attend_back(qkv, offset_bias, grad_attended, summed, total)
    partial_normed = jnp.einsum("cte,cde->td", dqkv, w_qkv, preferred_element_type=f32)
    partial_normed = partial_normed.astype(bf16).reshape(cycle, tok_rows, D)
    pieces = cycle_swap(partial_normed, "normed_swap", 5)
    grad_normed_attn = jnp.sum(pieces.reshape(micro, group, tok_rows, D).astype(f32), axis=1)
    grad_inputs, gain_attn_grad = norm_back(inputs, factor_attn, gain_attn, grad_normed_attn)
    grad_inputs = grad_inputs + grad_hidden

    qkv_grad = jnp.einsum("td,cte->cde", normed, dqkv, preferred_element_type=f32)
    qkv_grad = qkv_grad.astype(bf16).reshape(3, cycle, EXP_AXIS, rows, width)
    qkv_grad = cube_scatter(qkv_grad.transpose(2, 1, 0, 3, 4), (0, 1))

    blocks = length // BLOCK
    offset_grad = jnp.zeros((own_heads, 2 * length), f32)
    for d in range(blocks):
        first = (blocks - d - 1) * BLOCK
        offset_grad = offset_grad + jnp.pad(
            diag[:, d], ((0, 0), (first, 2 * length - first - 2 * BLOCK))
        )
    offset_grad = jnp.pad(offset_grad[:, 1:], ((0, 0), (0, 1)))
    own_grad = jnp.dot(offset_grad, bucket_hits.astype(f32), precision=highest)
    table_grad = lax.dynamic_update_slice_in_dim(
        jnp.zeros((HEADS, bucket_count), f32), own_grad, head_group * own_heads, 0
    )
    small_grads = jnp.concatenate(
        [
            router_grad.reshape(count, -1), gain_attn_grad.reshape(count, -1),
            gain_mix_grad.reshape(count, -1), table_grad.reshape(count, -1),
        ],
        axis=1,
    )
    small_grads = jnp.pad(small_grads, ((0, 0), (0, -small_grads.shape[1] % 128)))
    qkv_grad, small_parts = closing(qkv_grad, small_grads[:, None])
    qkv_sum = jnp.sum(qkv_grad.reshape(micro, group, 3, rows, width).astype(f32), axis=0)
    qkv_sum = qkv_sum.transpose(1, 2, 0, 3).reshape(3, rows, D)
    small_sum = jnp.sum(small_parts[:, 0], axis=0)[:small_size]
    gradients = (
        qkv_sum,
        out_sum,
        small_sum[: edges[1]].reshape(rows, experts_all),
        small_sum[edges[1] : edges[2]],
        small_sum[edges[2] : edges[3]],
        small_sum[edges[3] :],
        *expert_sums,
    )
    results = [
        adamw_step(master, gradient, first_old, second_old)
        for master, gradient, first_old, second_old in zip(masters, gradients, firsts, seconds)
    ]
    flat = [result[kind] for kind in range(4) for result in results]
    return (output.reshape(tokens.shape), grad_inputs.reshape(tokens.shape), *flat)


def solution(mesh):
    token_spec = P(None, "exp", "ctx", None)
    weight_specs = (
        P(None, both, None), P(both, None), P(both, None), P(both), P(both), P(both),
        P("exp", "ctx", None), P("exp", "ctx", None), P("exp", "ctx", None),
    )
    return jax.shard_map(
        body,
        mesh=mesh,
        in_specs=(token_spec, token_spec, P(), token_spec) + weight_specs * 3,
        out_specs=(token_spec, token_spec) + weight_specs * 4,
        check_vma=False,
    )
```

```python
from functools import partial
import math

import jax
import jax.numpy as jnp
from jax import lax
from jax.experimental import pallas as pl
from jax.experimental.pallas import tpu as pltpu
from jax.sharding import PartitionSpec as P

D = 1024
HEADS = 16
HEAD_DIM = 64
TOP = 2
BLOCK = 256
STEP = 3
EXP_AXIS = 4

eps_norm = 1e-06
eps_adam = 1e-08
score_scale = 0.125
decay_rate = 0.5
learn_rate = 1.0
weight_decay = 0.1
highest = lax.Precision.HIGHEST
last_dims = (((1,), (1,)), ((), ()))
first_dims = (((0,), (0,)), ((), ()))
bf16 = jnp.bfloat16
f32 = jnp.float32
both = ("ctx", "exp")
MESH = pl.DeviceIdType.MESH


def swap_bit(value, bit):
    count = lax.axis_size("ctx") * EXP_AXIS
    return lax.ppermute(value, both, [(d, d ^ (1 << bit)) for d in range(count)])


def flat_index():
    return lax.axis_index("ctx") * EXP_AXIS + lax.axis_index("exp")


def my_bit(bit):
    return (flat_index() >> bit) & 1


def turn(value):
    count = lax.axis_size("ctx") * EXP_AXIS

    def other(d):
        low, high = d & 1, (d >> 2) & 1
        return (d & ~5) | (low << 2) | high

    got = lax.ppermute(value, both, [(d, other(d)) for d in range(count) if other(d) != d])
    return jnp.where(my_bit(0) == my_bit(2), value, got)


def place_of(flat):
    return (flat // EXP_AXIS, flat % EXP_AXIS)


def greet(partners):
    barrier = pltpu.get_barrier_semaphore()
    for partner in partners:
        pl.semaphore_signal(barrier, inc=1, device_id=place_of(partner), device_id_type=MESH)
    pl.semaphore_wait(barrier, len(partners))


def remote(source, target, send, recv, partner):
    return pltpu.make_async_remote_copy(
        src_ref=source, dst_ref=target, send_sem=send, recv_sem=recv,
        device_id=place_of(partner), device_id_type=MESH,
    )


def exchange_call(kernel, number, arrays, shapes, sems):
    vmem = pl.BlockSpec(memory_space=pltpu.VMEM)
    sent = sum(array.size * array.dtype.itemsize for array in arrays)
    return pl.pallas_call(
        kernel,
        in_specs=[vmem] * len(arrays),
        out_specs=[vmem] * len(shapes),
        out_shape=shapes,
        scratch_shapes=[pltpu.SemaphoreType.DMA((size,)) for size in sems],
        compiler_params=pltpu.CompilerParams(
            collective_id=number, has_side_effects=True, vmem_limit_bytes=48 << 20
        ),
        cost_estimate=pl.CostEstimate(flops=0, bytes_accessed=8 * sent, transcendentals=0),
    )(*arrays)


def opening_kernel(cycle, group, tok_ref, col_ref, seq_ref, all_ref, s1, r1, s2, r2, s3, r3, s4, r4):
    me = flat_index()
    ctx, exp = place_of(me)
    greet([me ^ (rel * EXP_AXIS) for rel in range(1, cycle)] + [me ^ rel for rel in range(1, EXP_AXIS)])
    mine = ctx // group
    copies, relays, tokens, forwards = [], [], [], []
    for rel in range(1, cycle):
        peer = ctx ^ rel
        copies.append(
            remote(
                col_ref.at[lax.rem(peer, group)], all_ref.at[exp, ctx], s1.at[rel], r1.at[rel],
                me ^ (rel * EXP_AXIS),
            )
        )
    for far in range(group, cycle, group):
        relays.append(
            remote(
                tok_ref.at[mine ^ (far // group)], seq_ref.at[ctx], s2.at[far // group],
                r2.at[far // group], me ^ (far * EXP_AXIS),
            )
        )
    for rel in range(1, group):
        tokens.append(
            remote(
                tok_ref.at[mine], seq_ref.at[ctx], s3.at[rel], r3.at[rel], me ^ (rel * EXP_AXIS)
            )
        )
    for copy in copies + relays + tokens:
        copy.start()
    all_ref[exp, ctx] = col_ref[lax.rem(ctx, group)]
    seq_ref[ctx] = tok_ref[mine]
    for far, copy in zip(range(group, cycle, group), relays):
        copy.wait_recv()
        for rel in range(1, group):
            slot = far + rel
            tokens.append(
                remote(
                    seq_ref.at[ctx ^ far], seq_ref.at[ctx ^ far], s3.at[slot], r3.at[slot],
                    me ^ (rel * EXP_AXIS),
                )
            )
            tokens[-1].start()
    for copy in copies:
        copy.wait()
    for rel in range(1, EXP_AXIS):
        forwards.append(
            remote(all_ref.at[exp], all_ref.at[exp], s4.at[rel], r4.at[rel], me ^ rel)
        )
        forwards[-1].start()
    for copy in relays:
        copy.wait_send()
    for copy in tokens + forwards:
        copy.wait()


def opening(tok, cols):
    cycle = lax.axis_size("ctx")
    group = cycle // tok.shape[0]
    return exchange_call(
        partial(opening_kernel, cycle, group), 0, [tok, cols],
        [
            jax.ShapeDtypeStruct((cycle,) + tok.shape[1:], tok.dtype),
            jax.ShapeDtypeStruct((EXP_AXIS, cycle) + cols.shape[1:], cols.dtype),
        ],
        [cycle, cycle, cycle, cycle, cycle, cycle, EXP_AXIS, EXP_AXIS],
    )


def cycle_kernel(cycle, in_ref, out_ref, send, recv):
    me = flat_index()
    ctx, _ = place_of(me)
    greet([me ^ (rel * EXP_AXIS) for rel in range(1, cycle)])
    copies = []
    for rel in range(1, cycle):
        copies.append(
            remote(
                in_ref.at[ctx ^ rel], out_ref.at[ctx], send.at[rel], recv.at[rel],
                me ^ (rel * EXP_AXIS),
            )
        )
        copies[-1].start()
    out_ref[ctx] = in_ref[ctx]
    for copy in copies:
        copy.wait()


def cycle_swap(value, number):
    cycle = lax.axis_size("ctx")
    return exchange_call(
        partial(cycle_kernel, cycle), number, [value],
        [jax.ShapeDtypeStruct(value.shape, value.dtype)], [cycle, cycle],
    )[0]


def closing_kernel(cycle, col_ref, out_in, small_ref, col_out, out_out, all_ref, s1, r1, s2, r2, s3, r3):
    me = flat_index()
    ctx, _ = place_of(me)
    count = cycle * EXP_AXIS
    greet([me ^ rel for rel in range(1, count)])
    copies = []
    for source, target, send, recv in ((col_ref, col_out, s1, r1), (out_in, out_out, s2, r2)):
        for rel in range(1, cycle):
            copies.append(
                remote(
                    source.at[ctx ^ rel], target.at[ctx], send.at[rel], recv.at[rel],
                    me ^ (rel * EXP_AXIS),
                )
            )
    for rel in range(1, count):
        copies.append(
            remote(small_ref.at[me ^ rel], all_ref.at[me], s3.at[rel], r3.at[rel], me ^ rel)
        )
    for copy in copies:
        copy.start()
    col_out[ctx] = col_ref[ctx]
    out_out[ctx] = out_in[ctx]
    all_ref[me] = small_ref[me]
    for copy in copies:
        copy.wait()


def closing(cols, out, small):
    cycle = lax.axis_size("ctx")
    count = cycle * EXP_AXIS
    return exchange_call(
        partial(closing_kernel, cycle), 6, [cols, out, small],
        [jax.ShapeDtypeStruct(x.shape, x.dtype) for x in (cols, out, small)],
        [cycle, cycle, cycle, cycle, count, count],
    )


def plane_kernel(forward, arrays, *refs):
    ins, outs, send, recv = refs[:arrays], refs[arrays : 2 * arrays], refs[-2], refs[-1]
    me = flat_index()
    ctx, exp = place_of(me)
    greet([me ^ rel for rel in range(1, 2 * EXP_AXIS)])
    base = (ctx // 2) * 2
    ctx_low, exp_low = lax.rem(ctx, 2), lax.rem(exp, 2)
    for index in range(arrays):
        for e in range(EXP_AXIS):
            own = jnp.logical_and(exp == e, ctx_low == exp_low)
            sem = index * EXP_AXIS
            if forward:
                to_ctx, to_exp = base + e % 2, (e // 2) * 2 + ctx_low
                slot = exp
            else:
                to_ctx, to_exp = base + exp_low, e
                slot = (exp // 2) * 2 + ctx_low
            copy = remote(
                ins[index].at[e], outs[index].at[slot], send.at[sem + e], recv.at[sem + slot],
                to_ctx * EXP_AXIS + to_exp,
            )

            @pl.when(jnp.logical_not(own))
            def _():
                copy.start()

            @pl.when(own)
            def _():
                outs[index][e] = ins[index][e]

    for index in range(arrays):
        for e in range(EXP_AXIS):
            own = jnp.logical_and(exp == e, ctx_low == exp_low)
            sem = index * EXP_AXIS + e
            done = remote(ins[index].at[e], outs[index].at[e], send.at[sem], recv.at[sem], me ^ 1)

            @pl.when(jnp.logical_not(own))
            def _():
                done.wait()


def plane_swap(values, forward, number):
    count = len(values)
    return exchange_call(
        partial(plane_kernel, forward, count), number, list(values),
        [jax.ShapeDtypeStruct(x.shape, x.dtype) for x in values],
        [count * EXP_AXIS, count * EXP_AXIS],
    )


def line_permute(value, step, start):
    size = lax.axis_size("ctx") // 2
    pairs = []
    for a in range(size):
        b = a + step
        if 0 <= b < size and (a >= start if step > 0 else a < size - start):
            for low in range(2 * EXP_AXIS):
                pairs.append((a * 2 * EXP_AXIS + low, b * 2 * EXP_AXIS + low))
    return lax.ppermute(value, both, pairs)


def cube_sum(value, bit):
    mine = lax.dynamic_index_in_dim(value, my_bit(bit), 0, keepdims=False)
    theirs = lax.dynamic_index_in_dim(value, 1 - my_bit(bit), 0, keepdims=False)
    got = swap_bit(theirs, bit)
    return (mine.astype(f32) + got.astype(f32)).astype(value.dtype)


def pair_groups():
    count = lax.axis_size("ctx")
    return [[c for c in range(low, count, 2)] for low in range(2)]


def gather_expert(moved):
    mine = lax.all_gather(moved, "ctx", axis=0, axis_index_groups=pair_groups())
    theirs = swap_bit(mine, 0)
    low = my_bit(0) == 0
    whole = jnp.stack([jnp.where(low, mine, theirs), jnp.where(low, theirs, mine)], axis=1)
    return whole.reshape(-1, moved.shape[1])


def core_sum(grad):
    half = lax.axis_size("ctx") // 2
    value = grad.reshape(half, 2, grad.shape[0] // (2 * half), grad.shape[1])
    mine = lax.dynamic_index_in_dim(value, my_bit(0), 1, keepdims=False)
    theirs = lax.dynamic_index_in_dim(value, 1 - my_bit(0), 1, keepdims=False)
    got = swap_bit(theirs, 0)
    return (mine.astype(f32) + got.astype(f32)).astype(bf16)


class LineScatter:
    def __init__(self, halves):
        self.halves = halves
        self.size = halves[0].shape[0]
        self.place = lax.axis_index("ctx") // 2
        self.got = [[None, None] for _ in halves]

    def part(self, index, place, got):
        own = lax.dynamic_index_in_dim(
            self.halves[index], jnp.clip(place, 0, self.size - 1), 0, keepdims=False
        )
        return own if got is None else (own.astype(f32) + got.astype(f32)).astype(bf16)

    def round(self, step):
        away = self.size - 1 - step
        for index in range(len(self.halves)):
            pair = self.got[index]
            values = (
                self.part(index, self.place + away, pair[0]),
                self.part(index, self.place - away, pair[1]),
            )
            pair[0] = scatter_permute(values[0], 1, step)
            pair[1] = scatter_permute(values[1], -1, step)

    def settle(self, values):
        flat = [x for pair in self.got for x in pair]
        out = lax.optimization_barrier((*values, *flat))
        flat = out[len(values) :]
        self.got = [[flat[2 * k], flat[2 * k + 1]] for k in range(len(self.got))]
        return out[: len(values)]

    def totals(self):
        out = []
        for index, (right, left) in enumerate(self.got):
            own = lax.dynamic_index_in_dim(self.halves[index], self.place, 0, keepdims=False)
            total = own.astype(f32) + right.astype(f32) + left.astype(f32)
            out.append(turn(total.astype(bf16)))
        return out


def scatter_permute(value, step, number):
    size = lax.axis_size("ctx") // 2
    pairs = []
    for a in range(size):
        b = a + step
        if 0 <= b < size and (a <= number if step > 0 else a >= size - 1 - number):
            for low in range(2 * EXP_AXIS):
                pairs.append((a * 2 * EXP_AXIS + low, b * 2 * EXP_AXIS + low))
    return lax.ppermute(value, both, pairs)


def gelu_pair(value):
    inner = math.sqrt(2.0 / math.pi)
    square = value * value
    turned = jnp.tanh(inner * (value + 0.044715 * value * square))
    half = 0.5 * (1.0 + turned)
    slope = half + 0.5 * value * (1.0 - turned * turned) * inner * (1.0 + 3 * 0.044715 * square)
    return value * half, slope


def block_places(count, block):
    me = flat_index()
    line = count // 2
    place, low = me // (2 * EXP_AXIS), lax.rem(me, 2)
    out = []
    for k in range(line):
        for other in range(2):
            index = lax.rem(place + k, line) * 2 + (low + other * (1 - 2 * low))
            out.append(pl.ds(pl.multiple_of(index * block, block), block))
    return out


def expert_front_kernel(count, rows_ref, *refs):
    gates, ups = refs[:count], refs[count : 2 * count]
    units_ref, value_ref, slope_ref, turned = refs[2 * count :]
    block = gates[0].shape[0]

    @pl.when(pl.program_id(0) == 0)
    def _():
        for k, places in enumerate(block_places(count, block)):
            turned[:, k * block : (k + 1) * block] = rows_ref[:, places]

    rows = turned[...]
    gate = jnp.dot(rows, jnp.concatenate([r[...] for r in gates], 0), preferred_element_type=f32)
    up = jnp.dot(rows, jnp.concatenate([r[...] for r in ups], 0), preferred_element_type=f32)
    value, slope = gelu_pair(gate)
    units_ref[...] = (value * up).astype(bf16)
    value_ref[...] = value.astype(bf16)
    slope_ref[...] = (slope * up).astype(bf16)


def expert_front(rows, gates, ups):
    count, cols, tile = len(gates), gates[0].shape[1], 256
    wide = pl.BlockSpec((rows.shape[0], tile), lambda j: (0, j))
    return pl.pallas_call(
        partial(expert_front_kernel, count),
        grid=(cols // tile,),
        in_specs=[pl.BlockSpec(rows.shape, lambda j: (0, 0))]
        + [pl.BlockSpec((gates[0].shape[0], tile), lambda j: (0, j))] * (2 * count),
        out_specs=[wide] * 3,
        out_shape=[jax.ShapeDtypeStruct((rows.shape[0], cols), bf16)] * 3,
        scratch_shapes=[pltpu.VMEM(rows.shape, bf16)],
        compiler_params=pltpu.CompilerParams(vmem_limit_bytes=48 << 20),
        cost_estimate=pl.CostEstimate(
            flops=4 * rows.size * cols, bytes_accessed=4 * D * cols, transcendentals=0
        ),
        name="expert_front",
    )(rows, *gates, *ups)


def expert_middle_kernel(grads_ref, down_ref, value_ref, slope_ref, gate_ref, up_ref):
    grad = lax.dot_general(grads_ref[...], down_ref[...], last_dims, preferred_element_type=f32)
    gate_ref[...] = (grad * slope_ref[...].astype(f32)).astype(bf16)
    up_ref[...] = (grad * value_ref[...].astype(f32)).astype(bf16)


def expert_middle(grads, w_down, value, slope):
    cols, tile = w_down.shape[0], 256
    wide = pl.BlockSpec((grads.shape[0], tile), lambda j: (0, j))
    return pl.pallas_call(
        expert_middle_kernel,
        grid=(cols // tile,),
        in_specs=[
            pl.BlockSpec(grads.shape, lambda j: (0, 0)),
            pl.BlockSpec((tile, w_down.shape[1]), lambda j: (j, 0)),
            wide,
            wide,
        ],
        out_specs=[wide] * 2,
        out_shape=[jax.ShapeDtypeStruct((grads.shape[0], cols), bf16)] * 2,
        compiler_params=pltpu.CompilerParams(vmem_limit_bytes=48 << 20),
        cost_estimate=pl.CostEstimate(
            flops=2 * grads.size * cols, bytes_accessed=2 * D * cols, transcendentals=0
        ),
        name="expert_middle",
    )(grads, w_down, value, slope)


def expert_rear_kernel(count, gate_ref, up_ref, *refs):
    gates, ups = refs[:count], refs[count : 2 * count]
    out_ref, total = refs[2 * count :]
    block = gates[0].shape[0]
    weights = jnp.concatenate(
        [jnp.concatenate([r[...] for r in gates], 0), jnp.concatenate([r[...] for r in ups], 0)], 1
    )
    grads = jnp.concatenate([gate_ref[...], up_ref[...]], 1)
    term = lax.dot_general(grads, weights, last_dims, preferred_element_type=f32)

    @pl.when(pl.program_id(0) == 0)
    def _():
        total[...] = term

    @pl.when(pl.program_id(0) > 0)
    def _():
        total[...] += term

    @pl.when(pl.program_id(0) == pl.num_programs(0) - 1)
    def _():
        for k, places in enumerate(block_places(count, block)):
            out_ref[:, places] = total[:, k * block : (k + 1) * block].astype(bf16)


def expert_rear(grad_gate, grad_up, gates, ups):
    count, cols, tile = len(gates), gates[0].shape[1], 256
    wide = pl.BlockSpec((grad_gate.shape[0], tile), lambda j: (0, j))
    shape = (grad_gate.shape[0], D)
    return pl.pallas_call(
        partial(expert_rear_kernel, count),
        grid=(cols // tile,),
        in_specs=[wide] * 2
        + [pl.BlockSpec((gates[0].shape[0], tile), lambda j: (0, j))] * (2 * count),
        out_specs=pl.BlockSpec(shape, lambda j: (0, 0)),
        out_shape=jax.ShapeDtypeStruct(shape, bf16),
        scratch_shapes=[pltpu.VMEM(shape, f32)],
        compiler_params=pltpu.CompilerParams(vmem_limit_bytes=48 << 20),
        cost_estimate=pl.CostEstimate(
            flops=4 * shape[0] * D * cols, bytes_accessed=4 * D * cols, transcendentals=0
        ),
        name="expert_rear",
    )(grad_gate, grad_up, *gates, *ups)


def lane_mask(width, head, dtype):
    lane = lax.broadcasted_iota(jnp.int32, (1, width), 1)
    return ((lane // HEAD_DIM) == head).astype(dtype)


def fill_bias(ob_ref, head, bias, blocks):
    for d in range(blocks):
        first = (blocks - d - 1) * BLOCK
        window = ob_ref[0, pl.ds(head, 1), pl.ds(first, 2 * BLOCK)]
        wide = jnp.broadcast_to(window, (BLOCK, 2 * BLOCK))
        bias[d] = pltpu.roll(wide, 0, 1, stride=1, stride_axis=0)[:, BLOCK:]


def transposed(value):
    return value.astype(f32).T.astype(bf16)


def attend_kernel(blocks, heads, qkv_ref, ob_ref, att_ref, summed_ref, total_ref, bias, kt):
    width = qkv_ref.shape[2]
    for head in range(heads):
        fill_bias(ob_ref, head, bias.at[head], blocks)
    keep = [lane_mask(width, head, f32) for head in range(heads)]
    row = lax.broadcasted_iota(jnp.int32, (width, 1), 0) // HEAD_DIM
    for kb in range(blocks):
        cols = slice(kb * BLOCK, (kb + 1) * BLOCK)
        turned = transposed(qkv_ref[1, cols, :])
        for head in range(heads):
            kt[head, :, cols] = turned * (row == head).astype(bf16)

    for qb in range(blocks):
        rows = slice(qb * BLOCK, (qb + 1) * BLOCK)
        queries = qkv_ref[0, rows, :] * jnp.asarray(score_scale, bf16)

        def step(kb, carry):
            cols = pl.ds(pl.multiple_of(kb * BLOCK, BLOCK), BLOCK)
            values = qkv_ref[2, cols, :]
            out = []
            for head in range(heads):
                tot, acc = carry[head]
                score = jnp.dot(queries, kt[head, :, cols], preferred_element_type=f32)
                expo = jnp.exp(score + bias[head, qb - kb])
                tot = tot + (expo[:, :128] + expo[:, 128:])
                acc = acc + jnp.dot(expo.astype(bf16), values, preferred_element_type=f32)
                out.append((tot, acc))
            return tuple(out)

        carry = tuple(
            (jnp.zeros((BLOCK, 128), f32), jnp.zeros((BLOCK, width), f32)) for _ in range(heads)
        )
        for kb in range(qb + 1):
            carry = step(kb, carry)
        summed = sum(carry[head][1] * keep[head] for head in range(heads))
        total = sum(
            jnp.sum(carry[head][0], axis=1, keepdims=True) * keep[head] for head in range(heads)
        )
        summed_ref[rows, :] = summed
        total_ref[rows, :] = total
        att_ref[rows, :] = (summed / total).astype(bf16)


def attend(qkv, ob):
    _, length, width = qkv.shape
    lanes = min(width, 128)
    heads = lanes // HEAD_DIM
    steps = width // lanes
    blocks = length // BLOCK
    rows = pl.BlockSpec((length, lanes), lambda i: (0, i))
    return pl.pallas_call(
        partial(attend_kernel, blocks, heads),
        grid=(steps,),
        in_specs=[
            pl.BlockSpec((3, length, lanes), lambda i: (0, 0, i)),
            pl.BlockSpec((1, heads, 2 * length), lambda i: (i, 0, 0)),
        ],
        out_specs=[rows, rows, rows],
        out_shape=[
            jax.ShapeDtypeStruct((length, width), bf16),
            jax.ShapeDtypeStruct((length, width), f32),
            jax.ShapeDtypeStruct((length, width), f32),
        ],
        scratch_shapes=[
            pltpu.VMEM((heads, blocks, BLOCK, BLOCK), f32),
            pltpu.VMEM((heads, lanes, length), bf16),
        ],
        compiler_params=pltpu.CompilerParams(vmem_limit_bytes=48 << 20),
        cost_estimate=pl.CostEstimate(
            flops=4 * length * length * width, bytes_accessed=20 * length * width, transcendentals=0
        ),
        name="attend",
    )(qkv, ob.reshape(steps, heads, 2 * length))


def attend_back_kernel(
    blocks, heads, qkv_ref, ob_ref, da_ref, summed_ref, total_ref, dqkv_ref, diag_ref,
    bias, diff, qt, kt, km, vt, dm, dmt, dt, acc_k, acc_v,
):
    width = qkv_ref.shape[2]
    lanes = [slice(head * HEAD_DIM, (head + 1) * HEAD_DIM) for head in range(heads)]
    for head in range(heads):
        fill_bias(ob_ref, head, bias.at[head], blocks)
    diff[...] = jnp.zeros_like(diff)
    acc_k[...] = jnp.zeros_like(acc_k)
    acc_v[...] = jnp.zeros_like(acc_v)
    row = lax.broadcasted_iota(jnp.int32, (width, 1), 0) // HEAD_DIM
    scale = jnp.asarray(score_scale, bf16)
    for b in range(blocks):
        rows = slice(b * BLOCK, (b + 1) * BLOCK)
        qt[:, rows] = transposed(qkv_ref[0, rows, :]) * scale
        turned = transposed(qkv_ref[1, rows, :])
        vt[:, rows] = transposed(qkv_ref[2, rows, :])
        grad = da_ref[rows, :].astype(f32)
        total = total_ref[rows, :]
        scaled = grad / total
        dmt[:, rows] = transposed(scaled)
        inner = scaled * summed_ref[rows, :] / total
        for head in range(heads):
            mask = lane_mask(width, head, f32)
            kt[head, :, rows] = turned * (row == head).astype(bf16)
            km[head, rows, :] = qkv_ref[1, rows, :] * lane_mask(width, head, bf16)
            dm[head, rows, :] = (scaled * mask).astype(bf16)
            shift = -jnp.sum(inner * mask, axis=1, keepdims=True)
            dt[head, rows, :] = jnp.broadcast_to(shift, (BLOCK, 128))

    for qb in range(blocks):
        rows = slice(qb * BLOCK, (qb + 1) * BLOCK)
        queries = qkv_ref[0, rows, :] * scale
        shifts = [dt[head, rows, :] for head in range(heads)]

        def step(kb, acc_q):
            cols = pl.ds(pl.multiple_of(kb * BLOCK, BLOCK), BLOCK)
            for head in range(heads):
                score = jnp.dot(queries, kt[head, :, cols], preferred_element_type=f32)
                expo = jnp.exp(score + bias[head, qb - kb])
                probs = jnp.dot(dm[head, rows, :], vt[:, cols], preferred_element_type=f32)
                shift = jnp.concatenate([shifts[head]] * (BLOCK // 128), axis=1)
                dscore = (expo * (probs + shift)).astype(bf16)
                diff[head, qb - kb] += dscore.astype(f32)
                acc_q = acc_q + jnp.dot(dscore, km[head, cols, :], preferred_element_type=f32)
                acc_k[lanes[head], cols] += jnp.dot(
                    qt[lanes[head], rows], dscore, preferred_element_type=f32
                )
                acc_v[lanes[head], cols] += jnp.dot(
                    dmt[lanes[head], rows], expo.astype(bf16), preferred_element_type=f32
                )
            return acc_q

        acc_q = jnp.zeros((BLOCK, width), f32)
        for kb in range(qb + 1):
            acc_q = step(kb, acc_q)
        dqkv_ref[0, rows, :] = (acc_q * score_scale).astype(bf16)

    lower = lax.broadcasted_iota(jnp.int32, (8, 2 * BLOCK), 0)
    for head in range(heads):
        for d in range(blocks):

            def add_rows(i, fold):
                part = diff[head, d, pl.ds(pl.multiple_of(i * 8, 8), 8), :]
                wide = jnp.concatenate([jnp.zeros((8, BLOCK), f32), part], axis=1)
                return fold + pltpu.roll(wide, 2 * BLOCK - 8 * i, 1)

            fold = lax.fori_loop(
                0, BLOCK // 8, add_rows, jnp.zeros((8, 2 * BLOCK), f32), unroll=8
            )
            for bit in (1, 2, 4):
                fold = jnp.where((lower & bit) != 0, pltpu.roll(fold, 2 * BLOCK - bit, 1), fold)
            diag_ref[0, pl.ds(head * blocks + d, 1), :] = jnp.sum(fold, axis=0, keepdims=True)
    for b in range(blocks):
        rows = slice(b * BLOCK, (b + 1) * BLOCK)
        dqkv_ref[1, rows, :] = acc_k[:, rows].T.astype(bf16)
        dqkv_ref[2, rows, :] = acc_v[:, rows].T.astype(bf16)


def attend_back(qkv, ob, grad, summed, total):
    _, length, width = qkv.shape
    lanes = min(width, 128)
    heads = lanes // HEAD_DIM
    steps = width // lanes
    blocks = length // BLOCK
    rows = pl.BlockSpec((length, lanes), lambda i: (0, i))
    wide = pl.BlockSpec((3, length, lanes), lambda i: (0, 0, i))
    dqkv, diag = pl.pallas_call(
        partial(attend_back_kernel, blocks, heads),
        grid=(steps,),
        in_specs=[wide, pl.BlockSpec((1, heads, 2 * length), lambda i: (i, 0, 0)), rows, rows, rows],
        out_specs=[wide, pl.BlockSpec((1, heads * blocks, 2 * BLOCK), lambda i: (i, 0, 0))],
        out_shape=[
            jax.ShapeDtypeStruct((3, length, width), bf16),
            jax.ShapeDtypeStruct((steps, heads * blocks, 2 * BLOCK), f32),
        ],
        scratch_shapes=[
            pltpu.VMEM((heads, blocks, BLOCK, BLOCK), f32),
            pltpu.VMEM((heads, blocks, BLOCK, BLOCK), f32),
            pltpu.VMEM((lanes, length), bf16),
            pltpu.VMEM((heads, lanes, length), bf16),
            pltpu.VMEM((heads, length, lanes), bf16),
            pltpu.VMEM((lanes, length), bf16),
            pltpu.VMEM((heads, length, lanes), bf16),
            pltpu.VMEM((lanes, length), bf16),
            pltpu.VMEM((heads, length, 128), f32),
            pltpu.VMEM((lanes, length), f32),
            pltpu.VMEM((lanes, length), f32),
        ],
        compiler_params=pltpu.CompilerParams(vmem_limit_bytes=56 << 20),
        cost_estimate=pl.CostEstimate(
            flops=10 * length * length * width, bytes_accessed=30 * length * width, transcendentals=0
        ),
        name="attend_back",
    )(qkv, ob.reshape(steps, heads, 2 * length), grad, summed, total)
    return dqkv, diag.reshape(steps * heads, blocks, 2 * BLOCK)


def norm_back(norm_input, factor, gain_wide, grad_normed):
    scaled = grad_normed * gain_wide
    gain_grad = jnp.sum(grad_normed * norm_input * factor, axis=0)
    mean_term = jnp.mean(scaled * norm_input, axis=-1, keepdims=True)
    return (factor * scaled - norm_input * factor * factor * factor * mean_term, gain_grad)


def adamw_step(master, gradient, first_old, second_old):
    first_new = decay_rate * first_old + (1.0 - decay_rate) * gradient
    second_new = decay_rate * second_old + (1.0 - decay_rate) * gradient * gradient
    correct = 1.0 - decay_rate**STEP
    update = -learn_rate * (
        first_new / correct / (jnp.sqrt(second_new / correct) + eps_adam) + weight_decay * master
    )
    return (gradient, first_new, second_new, update)


def layer(tokens, cotangent, bucket_ids, routes, *state):
    masters, firsts, seconds = state[:9], state[9:18], state[18:]
    (
        qkv_master, out_master, router_master, gain_attn_master, gain_mix_master, table_master,
        gate_master, up_master, down_master,
    ) = masters
    micro, tok_rows = tokens.shape[0], tokens.shape[2]
    cycle = lax.axis_size("ctx")
    count = cycle * EXP_AXIS
    length = tok_rows * cycle
    group = cycle // micro
    width = D // group
    place = lax.axis_index("ctx")
    head_group = place % group
    line = cycle // 2
    line_place = place // 2
    rows = D // count
    experts_all = router_master.shape[1]
    capacity = 5 * tok_rows * TOP // (4 * experts_all)
    low = my_bit(0) == 0

    tok = tokens[:, 0]
    cols = qkv_master.astype(bf16).reshape(3 * rows, group, width).transpose(1, 0, 2)
    small = jnp.concatenate(
        [
            router_master.reshape(-1), gain_attn_master, gain_mix_master, table_master,
        ]
    ).astype(bf16)
    small_size = small.shape[0]
    small = jnp.pad(small, (0, 16 * width - small_size)).reshape(1, 16, width)
    cols = jnp.concatenate([cols, jnp.broadcast_to(small, (group, 16, width))], axis=1)
    w_out = lax.all_gather(out_master.astype(bf16), both, axis=0, tiled=True)
    gate_own, up_own, down_own = (
        turn(member[0].astype(bf16)) for member in (gate_master, up_master, down_master)
    )
    seq, gathered = opening(tok, cols)
    gate_own, up_own, seq, gathered = lax.optimization_barrier((gate_own, up_own, seq, gathered))
    lines = [[own, own] for own in (gate_own, up_own)]
    right, left = [], []

    def line_round(step):
        for pair in lines:
            pair[0] = line_permute(pair[0], 1, step)
            pair[1] = line_permute(pair[1], -1, step)
        right.append([pair[0] for pair in lines])
        left.append([pair[1] for pair in lines])

    def line_settle(value):
        flat = lax.optimization_barrier((value, *[x for pair in lines for x in pair]))
        lines[0][0], lines[0][1], lines[1][0], lines[1][1] = flat[1:]
        right[-1], left[-1] = [flat[1], flat[3]], [flat[2], flat[4]]
        return flat[0]

    line_round(0)
    seq = seq.reshape(length, D)
    w_qkv = gathered[:, :, : 3 * rows].reshape(EXP_AXIS, cycle, 3, rows, width)
    w_qkv = w_qkv.transpose(2, 1, 0, 3, 4).reshape(3, D, width)
    small = gathered[:, :, 3 * rows :].reshape(EXP_AXIS, cycle, 16 * width)[:, :, :small_size]
    small = small.transpose(1, 0, 2).reshape(count, small_size)
    edges = (0, rows * experts_all, rows * (experts_all + 1), rows * (experts_all + 2))
    router_bf = small[:, : edges[1]].reshape(D, experts_all)
    gain_attn = small[:, edges[1] : edges[2]].reshape(D).astype(f32)
    gain_mix = small[:, edges[2] : edges[3]].reshape(D).astype(f32)
    table = small[:, edges[3] :].reshape(HEADS, -1)
    bucket_count = table.shape[1]
    router_wide = router_bf.astype(f32)
    bucket_hits = bucket_ids[:, None] == jnp.arange(bucket_count, dtype=jnp.int32)[None, :]
    own_heads = HEADS // group
    own_table = lax.dynamic_slice_in_dim(table, head_group * own_heads, own_heads, 0)
    offset_bias = lax.dot_general(
        own_table, bucket_hits.astype(bf16), last_dims, preferred_element_type=f32
    )
    offset_bias = jnp.pad(offset_bias, ((0, 0), (1, 0)))[:, :-1]

    seq_wide = seq.astype(f32)
    seq_factor = lax.rsqrt(jnp.mean(seq_wide * seq_wide, axis=-1, keepdims=True) + eps_norm)
    normed = (seq_wide * seq_factor * gain_attn).astype(bf16)
    qkv = jnp.einsum("td,cde->cte", normed, w_qkv, preferred_element_type=f32).astype(bf16)
    attended, summed, total = attend(qkv, offset_bias)

    attended = line_settle(attended)
    back = cycle_swap(attended.reshape(cycle, tok_rows, width), 1)
    back, down_own = lax.optimization_barrier((line_settle(back), down_own))
    line_round(1)
    toks = micro * tok_rows
    attended_bf = back.reshape(micro, group, tok_rows, width).transpose(0, 2, 1, 3)
    attended_bf = attended_bf.reshape(toks, D)
    inputs = tok.reshape(toks, D).astype(f32)
    factor_attn = lax.rsqrt(jnp.mean(inputs * inputs, axis=-1, keepdims=True) + eps_norm)
    hidden_state = inputs + jnp.dot(attended_bf, w_out, preferred_element_type=f32)
    factor_mix = lax.rsqrt(jnp.mean(hidden_state * hidden_state, axis=-1, keepdims=True) + eps_norm)
    normed_mix = hidden_state * factor_mix * gain_mix
    normed_bf = normed_mix.astype(bf16)
    logits = jnp.dot(normed_bf, router_bf, preferred_element_type=f32)
    router_probs = jax.nn.softmax(logits, axis=-1)
    route_rows = routes.reshape(micro, tok_rows, TOP)
    expert_ids = jnp.arange(experts_all, dtype=jnp.int32)
    picked = (route_rows.reshape(toks, TOP)[:, :, None] == expert_ids).astype(f32)
    chosen = jnp.sum(picked * router_probs[:, None, :], axis=-1)
    chosen_sum = jnp.sum(chosen, axis=-1, keepdims=True)
    gate_share = chosen / chosen_sum
    flat_routes = route_rows.reshape(micro, tok_rows * TOP)
    route_hits = (flat_routes[:, :, None] == expert_ids).astype(jnp.int32)
    before = jnp.cumsum(route_hits, axis=1) - route_hits
    micro_ids = jnp.arange(micro, dtype=jnp.int32)[:, None]
    slot_index = (flat_routes * micro + micro_ids) * capacity + jnp.sum(before * route_hits, axis=-1)
    slot_index = slot_index.reshape(toks, TOP)
    slot_count = experts_all * micro * capacity
    slot_ids = jnp.arange(slot_count, dtype=jnp.int32)
    hits = [(slot_index[:, choice, None] == slot_ids).astype(bf16) for choice in range(TOP)]
    slots = (experts_all, micro, capacity, D)
    sent_rows = lax.dot_general(sum(hits), normed_bf, first_dims, preferred_element_type=f32)
    dy_rows = cotangent.reshape(toks, D).astype(f32)
    scaled_dy = [
        (gate_share[:, choice, None] * dy_rows).astype(bf16) for choice in range(TOP)
    ]
    sent_grads = lax.dot_general(
        jnp.concatenate(hits, axis=0), jnp.concatenate(scaled_dy, axis=0), first_dims,
        preferred_element_type=f32,
    )
    sent_rows = line_settle(sent_rows.astype(bf16))
    if line > 3:
        line_round(2)
    got_rows, got_grads = plane_swap(
        (sent_rows.reshape(slots), sent_grads.astype(bf16).reshape(slots)), True, 2
    )
    for step in range(3, line - 1):
        line_round(step)
    flat_rows = got_rows.reshape(-1, D)
    flat_grads = got_grads.reshape(-1, D)

    def blocks_of(index, own):
        blocks = [own] + [
            jnp.where(line_place + k < line, left[k - 1][index], right[line - 1 - k][index])
            for k in range(1, line)
        ]
        return [block for mine in blocks for block in (mine, swap_bit(mine, 0))]

    gates, ups = blocks_of(0, gate_own), blocks_of(1, up_own)
    w_down = gather_expert(down_own)
    kernels = gate_own.shape[0] % 128 == 0
    if kernels:
        units, value, slope = expert_front(flat_rows, gates, ups)
    else:

        def whole(blocks):
            pieces = []
            for mine, theirs in zip(blocks[::2], blocks[1::2]):
                pieces += [jnp.where(low, mine, theirs), jnp.where(low, theirs, mine)]
            return jnp.concatenate(pieces, axis=0)

        def turned(value, shift):
            twice = jnp.concatenate([value, value], axis=1)
            return lax.dynamic_slice_in_dim(twice, shift * (D // line), D, 1)

        w_gate, w_up = whole(gates), whole(ups)
        turned_rows = turned(flat_rows, line_place)
        gate_pre = jnp.dot(turned_rows, w_gate, preferred_element_type=f32)
        up_pre = jnp.dot(turned_rows, w_up, preferred_element_type=f32)
        value, slope = gelu_pair(gate_pre)
        units, slope = (value * up_pre).astype(bf16), slope * up_pre
    down_grad = lax.dot_general(units, flat_grads, first_dims, preferred_element_type=f32)
    down_line = LineScatter([core_sum(down_grad.astype(bf16))])
    down_line.round(0)
    grad_gate, grad_up = expert_middle(flat_grads, w_down, value, slope)
    (grad_up,) = down_line.settle((grad_up,))
    down_line.round(1)
    up_grad = lax.dot_general(flat_rows, grad_up, first_dims, preferred_element_type=f32)
    gate_grad = lax.dot_general(flat_rows, grad_gate, first_dims, preferred_element_type=f32)
    both_line = LineScatter([core_sum(up_grad.astype(bf16)), core_sum(gate_grad.astype(bf16))])
    (grad_gate,) = down_line.settle((grad_gate,))
    for step in range(2, line - 1):
        down_line.round(step)
    both_line.round(0)
    out_rows = jnp.dot(units, w_down, preferred_element_type=f32).astype(bf16)
    if kernels:
        grad_rows = expert_rear(grad_gate, grad_up, gates, ups)
    else:
        grad_rows = lax.dot_general(grad_gate, w_gate, last_dims, preferred_element_type=f32)
        grad_rows = grad_rows + lax.dot_general(
            grad_up, w_up, last_dims, preferred_element_type=f32
        )
        grad_rows = turned(grad_rows.astype(bf16), line - line_place)
    back_out, back_grad = plane_swap((out_rows.reshape(slots), grad_rows.reshape(slots)), False, 3)
    back_out, back_grad = both_line.settle((back_out, back_grad))
    both_line.round(1)
    back_out, back_grad = back_out.reshape(slot_count, D), back_grad.reshape(slot_count, D)

    returned = [jnp.dot(hit, back_out, preferred_element_type=f32) for hit in hits]
    mix_out = sum(gate_share[:, c, None] * returned[c] for c in range(TOP))
    output = (hidden_state + mix_out).astype(bf16)
    grad_gates = jnp.stack([jnp.sum(dy_rows * returned[c], axis=-1) for c in range(TOP)], axis=1)
    grad_chosen = grad_gates / chosen_sum - jnp.sum(grad_gates * chosen, axis=-1, keepdims=True) / (
        chosen_sum * chosen_sum
    )
    grad_probs = jnp.sum(grad_chosen[:, :, None] * picked, axis=1)
    grad_logits = router_probs * (
        grad_probs - jnp.sum(router_probs * grad_probs, axis=-1, keepdims=True)
    )
    router_grad = lax.dot_general(
        normed_bf.astype(f32), grad_logits, first_dims, precision=highest
    )
    grad_normed = jnp.dot(sum(hits), back_grad, preferred_element_type=f32) + lax.dot_general(
        grad_logits, router_wide, last_dims, precision=highest
    )
    grad_hidden, gain_mix_grad = norm_back(hidden_state, factor_mix, gain_mix, grad_normed)
    grad_hidden = grad_hidden + dy_rows
    grad_branch = grad_hidden.astype(bf16)
    grad_attended = lax.dot_general(grad_branch, w_out, last_dims, preferred_element_type=f32)
    grad_attended = grad_attended.astype(bf16).reshape(micro, tok_rows, group, width)
    grad_attended = grad_attended.transpose(0, 2, 1, 3).reshape(cycle, tok_rows, width)
    (grad_attended,) = both_line.settle((grad_attended,))
    grad_attended = cycle_swap(grad_attended, 4).reshape(length, width)
    for step in range(2, line - 1):
        both_line.round(step)
    out_grad = lax.dot_general(attended_bf, grad_branch, first_dims, preferred_element_type=f32)
    out_grad = out_grad.astype(bf16).reshape(cycle, 2, 2, rows, D).transpose(2, 1, 0, 3, 4)
    out_grad = cube_sum(out_grad, 0)
    out_grad = cube_sum(out_grad, 1)

    dqkv, diag = attend_back(qkv, offset_bias, grad_attended, summed, total)
    qkv_grad = jnp.einsum("td,cte->cde", normed, dqkv, preferred_element_type=f32)
    qkv_grad = qkv_grad.astype(bf16).reshape(3, cycle, 2, 2, rows, width)
    qkv_grad = qkv_grad.transpose(3, 2, 1, 0, 4, 5)
    qkv_grad = cube_sum(qkv_grad, 0)
    qkv_grad = cube_sum(qkv_grad, 1)
    partial_normed = jnp.einsum("cte,cde->td", dqkv, w_qkv, preferred_element_type=f32)
    (partial_normed,) = both_line.settle((partial_normed.astype(bf16),))
    partial_normed = partial_normed.reshape(cycle, tok_rows, D)
    pieces = cycle_swap(partial_normed, 5)
    grad_normed_attn = jnp.sum(pieces.reshape(micro, group, tok_rows, D).astype(f32), axis=1)
    grad_inputs, gain_attn_grad = norm_back(
        inputs, factor_attn, gain_attn, grad_normed_attn.reshape(toks, D)
    )
    grad_inputs = grad_inputs + grad_hidden

    (down_sum,) = down_line.totals()
    up_sum, gate_sum = both_line.totals()
    blocks = length // BLOCK
    offset_grad = jnp.zeros((own_heads, 2 * length), f32)
    for d in range(blocks):
        first = (blocks - d - 1) * BLOCK
        offset_grad = offset_grad + jnp.pad(
            diag[:, d], ((0, 0), (first, 2 * length - first - 2 * BLOCK))
        )
    offset_grad = jnp.pad(offset_grad[:, 1:], ((0, 0), (0, 1)))
    own_grad = jnp.dot(offset_grad, bucket_hits.astype(f32), precision=highest)
    table_grad = lax.dynamic_update_slice_in_dim(
        jnp.zeros((HEADS, bucket_count), f32), own_grad, head_group * own_heads, 0
    )
    small_grads = jnp.concatenate(
        [
            router_grad.reshape(count, -1), gain_attn_grad.reshape(count, -1),
            gain_mix_grad.reshape(count, -1), table_grad.reshape(count, -1),
        ],
        axis=1,
    )
    small_grads = jnp.pad(small_grads, ((0, 0), (0, -small_grads.shape[1] % 128)))
    qkv_grad, out_grad, small_parts = closing(qkv_grad, out_grad, small_grads[:, None])
    qkv_sum = jnp.sum(qkv_grad.reshape(micro, group, 3, rows, width).astype(f32), axis=0)
    qkv_sum = qkv_sum.transpose(1, 2, 0, 3).reshape(3, rows, D)
    out_sum = jnp.sum(out_grad.astype(f32), axis=0)
    small_sum = jnp.sum(small_parts[:, 0], axis=0)[:small_size]
    gradients = (
        qkv_sum,
        out_sum,
        small_sum[: edges[1]].reshape(rows, experts_all),
        small_sum[edges[1] : edges[2]],
        small_sum[edges[2] : edges[3]],
        small_sum[edges[3] :],
        *(total[None].astype(f32) for total in (gate_sum, up_sum, down_sum)),
    )
    results = [
        adamw_step(master, gradient, first_old, second_old)
        for master, gradient, first_old, second_old in zip(masters, gradients, firsts, seconds)
    ]
    flat = [result[kind] for kind in range(4) for result in results]
    return (output.reshape(tokens.shape), grad_inputs.reshape(tokens.shape), *flat)


def solution(mesh):
    token_spec = P(None, "exp", "ctx", None)
    weight_specs = (
        P(None, both, None), P(both, None), P(both, None), P(both), P(both), P(both),
        P("exp", "ctx", None), P("exp", "ctx", None), P("exp", "ctx", None),
    )
    return jax.shard_map(
        layer,
        mesh=mesh,
        in_specs=(token_spec, token_spec, P(), token_spec) + weight_specs * 3,
        out_specs=(token_spec, token_spec) + weight_specs * 4,
        check_vma=False,
    )
```

```python
from functools import partial
import math

import jax
import jax.numpy as jnp
from jax import lax
from jax.experimental import pallas as pl
from jax.experimental.pallas import tpu as pltpu
from jax.sharding import PartitionSpec as P

D = 1024
HEADS = 16
HEAD_DIM = 64
TOP = 2
BLOCK = 256
STEP = 3
EXP_AXIS = 4

eps_norm = 1e-06
eps_adam = 1e-08
score_scale = 0.125
decay_rate = 0.5
learn_rate = 1.0
weight_decay = 0.1
highest = lax.Precision.HIGHEST
last_dims = (((1,), (1,)), ((), ()))
first_dims = (((0,), (0,)), ((), ()))
bf16 = jnp.bfloat16
f32 = jnp.float32
both = ("ctx", "exp")
MESH = pl.DeviceIdType.MESH


def swap_bit(value, bit):
    count = lax.axis_size("ctx") * EXP_AXIS
    return lax.ppermute(value, both, [(d, d ^ (1 << bit)) for d in range(count)])


def flat_index():
    return lax.axis_index("ctx") * EXP_AXIS + lax.axis_index("exp")


def my_bit(bit):
    return (flat_index() >> bit) & 1


def turn(value):
    count = lax.axis_size("ctx") * EXP_AXIS

    def other(d):
        low, high = d & 1, (d >> 2) & 1
        return (d & ~5) | (low << 2) | high

    got = lax.ppermute(value, both, [(d, other(d)) for d in range(count) if other(d) != d])
    return jnp.where(my_bit(0) == my_bit(2), value, got)


def place_of(flat):
    return (flat // EXP_AXIS, flat % EXP_AXIS)


def greet(partners):
    barrier = pltpu.get_barrier_semaphore()
    for partner in partners:
        pl.semaphore_signal(barrier, inc=1, device_id=place_of(partner), device_id_type=MESH)
    pl.semaphore_wait(barrier, len(partners))


def remote(source, target, send, recv, partner):
    return pltpu.make_async_remote_copy(
        src_ref=source, dst_ref=target, send_sem=send, recv_sem=recv,
        device_id=place_of(partner), device_id_type=MESH,
    )


def exchange_call(kernel, number, arrays, shapes, sems):
    vmem = pl.BlockSpec(memory_space=pltpu.VMEM)
    sent = sum(array.size * array.dtype.itemsize for array in arrays)
    return pl.pallas_call(
        kernel,
        in_specs=[vmem] * len(arrays),
        out_specs=[vmem] * len(shapes),
        out_shape=shapes,
        scratch_shapes=[pltpu.SemaphoreType.DMA((size,)) for size in sems],
        compiler_params=pltpu.CompilerParams(
            collective_id=number, has_side_effects=True, vmem_limit_bytes=48 << 20
        ),
        cost_estimate=pl.CostEstimate(flops=0, bytes_accessed=8 * sent, transcendentals=0),
    )(*arrays)


def opening_kernel(cycle, group, tok_ref, col_ref, seq_ref, all_ref, s1, r1, s2, r2, s3, r3, s4, r4):
    me = flat_index()
    ctx, exp = place_of(me)
    greet([me ^ (rel * EXP_AXIS) for rel in range(1, cycle)] + [me ^ rel for rel in range(1, EXP_AXIS)])
    mine = ctx // group
    copies, relays, tokens, forwards = [], [], [], []
    for rel in range(1, cycle):
        peer = ctx ^ rel
        copies.append(
            remote(
                col_ref.at[lax.rem(peer, group)], all_ref.at[exp, ctx], s1.at[rel], r1.at[rel],
                me ^ (rel * EXP_AXIS),
            )
        )
    for far in range(group, cycle, group):
        relays.append(
            remote(
                tok_ref.at[mine ^ (far // group)], seq_ref.at[ctx], s2.at[far // group],
                r2.at[far // group], me ^ (far * EXP_AXIS),
            )
        )
    for rel in range(1, group):
        tokens.append(
            remote(
                tok_ref.at[mine], seq_ref.at[ctx], s3.at[rel], r3.at[rel], me ^ (rel * EXP_AXIS)
            )
        )
    for copy in copies + relays + tokens:
        copy.start()
    all_ref[exp, ctx] = col_ref[lax.rem(ctx, group)]
    seq_ref[ctx] = tok_ref[mine]
    for far, copy in zip(range(group, cycle, group), relays):
        copy.wait_recv()
        for rel in range(1, group):
            slot = far + rel
            tokens.append(
                remote(
                    seq_ref.at[ctx ^ far], seq_ref.at[ctx ^ far], s3.at[slot], r3.at[slot],
                    me ^ (rel * EXP_AXIS),
                )
            )
            tokens[-1].start()
    for copy in copies:
        copy.wait()
    for rel in range(1, EXP_AXIS):
        forwards.append(
            remote(all_ref.at[exp], all_ref.at[exp], s4.at[rel], r4.at[rel], me ^ rel)
        )
        forwards[-1].start()
    for copy in relays:
        copy.wait_send()
    for copy in tokens + forwards:
        copy.wait()


def opening(tok, cols):
    cycle = lax.axis_size("ctx")
    group = cycle // tok.shape[0]
    return exchange_call(
        partial(opening_kernel, cycle, group), 0, [tok, cols],
        [
            jax.ShapeDtypeStruct((cycle,) + tok.shape[1:], tok.dtype),
            jax.ShapeDtypeStruct((EXP_AXIS, cycle) + cols.shape[1:], cols.dtype),
        ],
        [cycle, cycle, cycle, cycle, cycle, cycle, EXP_AXIS, EXP_AXIS],
    )


def cycle_kernel(cycle, in_ref, out_ref, send, recv):
    me = flat_index()
    ctx, _ = place_of(me)
    greet([me ^ (rel * EXP_AXIS) for rel in range(1, cycle)])
    copies = []
    for rel in range(1, cycle):
        copies.append(
            remote(
                in_ref.at[ctx ^ rel], out_ref.at[ctx], send.at[rel], recv.at[rel],
                me ^ (rel * EXP_AXIS),
            )
        )
        copies[-1].start()
    out_ref[ctx] = in_ref[ctx]
    for copy in copies:
        copy.wait()


def cycle_swap(value, number):
    cycle = lax.axis_size("ctx")
    return exchange_call(
        partial(cycle_kernel, cycle), number, [value],
        [jax.ShapeDtypeStruct(value.shape, value.dtype)], [cycle, cycle],
    )[0]


def closing_kernel(
    cycle, col_ref, out_in, small_ref, col_out, out_out, mid_ref, all_ref, s1, r1, s2, r2, s3, r3, s4, r4
):
    me = flat_index()
    ctx, exp = place_of(me)
    greet([me ^ (rel * EXP_AXIS) for rel in range(1, cycle)] + [me ^ rel for rel in range(1, EXP_AXIS)])
    smalls, copies = [], []
    for source, target, send, recv, out in (
        (small_ref, mid_ref, s3, r3, smalls), (col_ref, col_out, s1, r1, copies),
        (out_in, out_out, s2, r2, copies),
    ):
        for rel in range(1, cycle):
            out.append(
                remote(
                    source.at[ctx ^ rel], target.at[ctx], send.at[rel], recv.at[rel],
                    me ^ (rel * EXP_AXIS),
                )
            )
            out[-1].start()
    mid_ref[ctx] = small_ref[ctx]
    col_out[ctx] = col_ref[ctx]
    out_out[ctx] = out_in[ctx]
    for copy in smalls:
        copy.wait()
    for rel in range(1, EXP_AXIS):
        copies.append(remote(mid_ref, all_ref.at[exp], s4.at[rel], r4.at[rel], me ^ rel))
        copies[-1].start()
    all_ref[exp] = mid_ref[...]
    for copy in copies:
        copy.wait()


def closing(cols, out, small):
    cycle = lax.axis_size("ctx")
    results = exchange_call(
        partial(closing_kernel, cycle), 6, [cols, out, small],
        [jax.ShapeDtypeStruct(x.shape, x.dtype) for x in (cols, out, small)]
        + [jax.ShapeDtypeStruct((EXP_AXIS,) + small.shape, small.dtype)],
        [cycle] * 6 + [EXP_AXIS] * 2,
    )
    return results[0], results[1], results[3]


def plane_kernel(forward, arrays, *refs):
    ins, outs, send, recv = refs[:arrays], refs[arrays : 2 * arrays], refs[-2], refs[-1]
    me = flat_index()
    ctx, exp = place_of(me)
    greet([me ^ rel for rel in range(1, 2 * EXP_AXIS)])
    base = (ctx // 2) * 2
    ctx_low, exp_low = lax.rem(ctx, 2), lax.rem(exp, 2)
    for index in range(arrays):
        for e in range(EXP_AXIS):
            own = jnp.logical_and(exp == e, ctx_low == exp_low)
            sem = index * EXP_AXIS
            if forward:
                to_ctx, to_exp = base + e % 2, (e // 2) * 2 + ctx_low
                slot = exp
            else:
                to_ctx, to_exp = base + exp_low, e
                slot = (exp // 2) * 2 + ctx_low
            copy = remote(
                ins[index].at[e], outs[index].at[slot], send.at[sem + e], recv.at[sem + slot],
                to_ctx * EXP_AXIS + to_exp,
            )

            @pl.when(jnp.logical_not(own))
            def _():
                copy.start()

            @pl.when(own)
            def _():
                outs[index][e] = ins[index][e]

    for index in range(arrays):
        for e in range(EXP_AXIS):
            own = jnp.logical_and(exp == e, ctx_low == exp_low)
            sem = index * EXP_AXIS + e
            done = remote(ins[index].at[e], outs[index].at[e], send.at[sem], recv.at[sem], me ^ 1)

            @pl.when(jnp.logical_not(own))
            def _():
                done.wait()


def plane_swap(values, forward, number):
    count = len(values)
    return exchange_call(
        partial(plane_kernel, forward, count), number, list(values),
        [jax.ShapeDtypeStruct(x.shape, x.dtype) for x in values],
        [count * EXP_AXIS, count * EXP_AXIS],
    )


def line_permute(value, step, start):
    size = lax.axis_size("ctx") // 2
    pairs = []
    for a in range(size):
        b = a + step
        if 0 <= b < size and (a >= start if step > 0 else a < size - start):
            for low in range(2 * EXP_AXIS):
                pairs.append((a * 2 * EXP_AXIS + low, b * 2 * EXP_AXIS + low))
    return lax.ppermute(value, both, pairs)


def cube_sum(value, bit):
    mine = lax.dynamic_index_in_dim(value, my_bit(bit), 0, keepdims=False)
    theirs = lax.dynamic_index_in_dim(value, 1 - my_bit(bit), 0, keepdims=False)
    got = swap_bit(theirs, bit)
    return (mine.astype(f32) + got.astype(f32)).astype(value.dtype)


def pair_groups():
    count = lax.axis_size("ctx")
    return [[c for c in range(low, count, 2)] for low in range(2)]


def gather_expert(moved):
    mine = lax.all_gather(moved, "ctx", axis=0, axis_index_groups=pair_groups())
    theirs = swap_bit(mine, 0)
    low = my_bit(0) == 0
    whole = jnp.stack([jnp.where(low, mine, theirs), jnp.where(low, theirs, mine)], axis=1)
    return whole.reshape(-1, moved.shape[1])


def core_sum(grad):
    half = lax.axis_size("ctx") // 2
    value = grad.reshape(half, 2, grad.shape[0] // (2 * half), grad.shape[1])
    mine = lax.dynamic_index_in_dim(value, my_bit(0), 1, keepdims=False)
    theirs = lax.dynamic_index_in_dim(value, 1 - my_bit(0), 1, keepdims=False)
    got = swap_bit(theirs, 0)
    return (mine.astype(f32) + got.astype(f32)).astype(bf16)


def scatter_expert(half):
    part = lax.psum_scatter(half, "ctx", scatter_dimension=0, axis_index_groups=pair_groups())
    return turn(part)


def gelu_pair(value):
    inner = math.sqrt(2.0 / math.pi)
    square = value * value
    turned = jnp.tanh(inner * (value + 0.044715 * value * square))
    half = 0.5 * (1.0 + turned)
    slope = half + 0.5 * value * (1.0 - turned * turned) * inner * (1.0 + 3 * 0.044715 * square)
    return value * half, slope


def block_places(count, block):
    me = flat_index()
    line = count // 2
    place, low = me // (2 * EXP_AXIS), lax.rem(me, 2)
    out = []
    for k in range(line):
        for other in range(2):
            index = lax.rem(place + k, line) * 2 + (low + other * (1 - 2 * low))
            out.append(pl.ds(pl.multiple_of(index * block, block), block))
    return out


def expert_front_kernel(count, rows_ref, *refs):
    blocks = refs[:count]
    units_ref, value_ref, slope_ref, turned = refs[count:]
    block = blocks[0].shape[1]

    @pl.when(pl.program_id(0) == 0)
    def _():
        for k, places in enumerate(block_places(count, block)):
            turned[:, k * block : (k + 1) * block] = rows_ref[:, places]

    rows = turned[...]
    gate = jnp.dot(rows, jnp.concatenate([r[0] for r in blocks], 0), preferred_element_type=f32)
    up = jnp.dot(rows, jnp.concatenate([r[1] for r in blocks], 0), preferred_element_type=f32)
    value, slope = gelu_pair(gate)
    units_ref[...] = (value * up).astype(bf16)
    value_ref[...] = value.astype(bf16)
    slope_ref[...] = (slope * up).astype(bf16)


def expert_front(rows, blocks):
    count, cols, tile = len(blocks), blocks[0].shape[2], 256
    wide = pl.BlockSpec((rows.shape[0], tile), lambda j: (0, j))
    return pl.pallas_call(
        partial(expert_front_kernel, count),
        grid=(cols // tile,),
        in_specs=[pl.BlockSpec(rows.shape, lambda j: (0, 0))]
        + [pl.BlockSpec(blocks[0].shape[:2] + (tile,), lambda j: (0, 0, j))] * count,
        out_specs=[wide] * 3,
        out_shape=[jax.ShapeDtypeStruct((rows.shape[0], cols), bf16)] * 3,
        scratch_shapes=[pltpu.VMEM(rows.shape, bf16)],
        compiler_params=pltpu.CompilerParams(vmem_limit_bytes=48 << 20),
        cost_estimate=pl.CostEstimate(
            flops=4 * rows.size * cols, bytes_accessed=4 * D * cols, transcendentals=0
        ),
        name="expert_front",
    )(rows, *blocks)


def expert_middle_kernel(grads_ref, down_ref, value_ref, slope_ref, gate_ref, up_ref):
    grad = lax.dot_general(grads_ref[...], down_ref[...], last_dims, preferred_element_type=f32)
    gate_ref[...] = (grad * slope_ref[...].astype(f32)).astype(bf16)
    up_ref[...] = (grad * value_ref[...].astype(f32)).astype(bf16)


def expert_middle(grads, w_down, value, slope):
    cols, tile = w_down.shape[0], 256
    wide = pl.BlockSpec((grads.shape[0], tile), lambda j: (0, j))
    return pl.pallas_call(
        expert_middle_kernel,
        grid=(cols // tile,),
        in_specs=[
            pl.BlockSpec(grads.shape, lambda j: (0, 0)),
            pl.BlockSpec((tile, w_down.shape[1]), lambda j: (j, 0)),
            wide,
            wide,
        ],
        out_specs=[wide] * 2,
        out_shape=[jax.ShapeDtypeStruct((grads.shape[0], cols), bf16)] * 2,
        compiler_params=pltpu.CompilerParams(vmem_limit_bytes=48 << 20),
        cost_estimate=pl.CostEstimate(
            flops=2 * grads.size * cols, bytes_accessed=2 * D * cols, transcendentals=0
        ),
        name="expert_middle",
    )(grads, w_down, value, slope)


def expert_rear_kernel(count, gate_ref, up_ref, *refs):
    blocks = refs[:count]
    out_ref, total = refs[count:]
    block = blocks[0].shape[1]
    weights = jnp.concatenate(
        [jnp.concatenate([r[part] for r in blocks], 0) for part in range(2)], 1
    )
    grads = jnp.concatenate([gate_ref[...], up_ref[...]], 1)
    term = lax.dot_general(grads, weights, last_dims, preferred_element_type=f32)

    @pl.when(pl.program_id(0) == 0)
    def _():
        total[...] = term

    @pl.when(pl.program_id(0) > 0)
    def _():
        total[...] += term

    @pl.when(pl.program_id(0) == pl.num_programs(0) - 1)
    def _():
        for k, places in enumerate(block_places(count, block)):
            out_ref[:, places] = total[:, k * block : (k + 1) * block].astype(bf16)


def expert_rear(grad_gate, grad_up, blocks):
    count, cols, tile = len(blocks), blocks[0].shape[2], 256
    wide = pl.BlockSpec((grad_gate.shape[0], tile), lambda j: (0, j))
    shape = (grad_gate.shape[0], D)
    return pl.pallas_call(
        partial(expert_rear_kernel, count),
        grid=(cols // tile,),
        in_specs=[wide] * 2
        + [pl.BlockSpec(blocks[0].shape[:2] + (tile,), lambda j: (0, 0, j))] * count,
        out_specs=pl.BlockSpec(shape, lambda j: (0, 0)),
        out_shape=jax.ShapeDtypeStruct(shape, bf16),
        scratch_shapes=[pltpu.VMEM(shape, f32)],
        compiler_params=pltpu.CompilerParams(vmem_limit_bytes=48 << 20),
        cost_estimate=pl.CostEstimate(
            flops=4 * shape[0] * D * cols, bytes_accessed=4 * D * cols, transcendentals=0
        ),
        name="expert_rear",
    )(grad_gate, grad_up, *blocks)


def lane_mask(width, head, dtype):
    lane = lax.broadcasted_iota(jnp.int32, (1, width), 1)
    return ((lane // HEAD_DIM) == head).astype(dtype)


def fill_bias(ob_ref, head, bias, blocks):
    for d in range(blocks):
        first = (blocks - d - 1) * BLOCK
        window = ob_ref[0, pl.ds(head, 1), pl.ds(first, 2 * BLOCK)]
        wide = jnp.broadcast_to(window, (BLOCK, 2 * BLOCK))
        bias[d] = pltpu.roll(wide, 0, 1, stride=1, stride_axis=0)[:, BLOCK:]


def transposed(value):
    return value.astype(f32).T.astype(bf16)


def attend_kernel(blocks, heads, qkv_ref, ob_ref, att_ref, summed_ref, total_ref, bias, kt):
    width = qkv_ref.shape[2]
    for head in range(heads):
        fill_bias(ob_ref, head, bias.at[head], blocks)
    keep = [lane_mask(width, head, f32) for head in range(heads)]
    row = lax.broadcasted_iota(jnp.int32, (width, 1), 0) // HEAD_DIM
    for kb in range(blocks):
        cols = slice(kb * BLOCK, (kb + 1) * BLOCK)
        turned = transposed(qkv_ref[1, cols, :])
        for head in range(heads):
            kt[head, :, cols] = turned * (row == head).astype(bf16)

    for qb in range(blocks):
        rows = slice(qb * BLOCK, (qb + 1) * BLOCK)
        queries = qkv_ref[0, rows, :] * jnp.asarray(score_scale, bf16)

        def step(kb, carry):
            cols = pl.ds(pl.multiple_of(kb * BLOCK, BLOCK), BLOCK)
            values = qkv_ref[2, cols, :]
            out = []
            for head in range(heads):
                tot, acc = carry[head]
                score = jnp.dot(queries, kt[head, :, cols], preferred_element_type=f32)
                expo = jnp.exp(score + bias[head, qb - kb])
                tot = tot + (expo[:, :128] + expo[:, 128:])
                acc = acc + jnp.dot(expo.astype(bf16), values, preferred_element_type=f32)
                out.append((tot, acc))
            return tuple(out)

        carry = tuple(
            (jnp.zeros((BLOCK, 128), f32), jnp.zeros((BLOCK, width), f32)) for _ in range(heads)
        )
        for kb in range(qb + 1):
            carry = step(kb, carry)
        summed = sum(carry[head][1] * keep[head] for head in range(heads))
        total = sum(
            jnp.sum(carry[head][0], axis=1, keepdims=True) * keep[head] for head in range(heads)
        )
        summed_ref[rows, :] = summed
        total_ref[rows, :] = total
        att_ref[rows, :] = (summed / total).astype(bf16)


def attend(qkv, ob):
    _, length, width = qkv.shape
    lanes = min(width, 128)
    heads = lanes // HEAD_DIM
    steps = width // lanes
    blocks = length // BLOCK
    rows = pl.BlockSpec((length, lanes), lambda i: (0, i))
    return pl.pallas_call(
        partial(attend_kernel, blocks, heads),
        grid=(steps,),
        in_specs=[
            pl.BlockSpec((3, length, lanes), lambda i: (0, 0, i)),
            pl.BlockSpec((1, heads, 2 * length), lambda i: (i, 0, 0)),
        ],
        out_specs=[rows, rows, rows],
        out_shape=[
            jax.ShapeDtypeStruct((length, width), bf16),
            jax.ShapeDtypeStruct((length, width), f32),
            jax.ShapeDtypeStruct((length, width), f32),
        ],
        scratch_shapes=[
            pltpu.VMEM((heads, blocks, BLOCK, BLOCK), f32),
            pltpu.VMEM((heads, lanes, length), bf16),
        ],
        compiler_params=pltpu.CompilerParams(vmem_limit_bytes=48 << 20),
        cost_estimate=pl.CostEstimate(
            flops=4 * length * length * width, bytes_accessed=20 * length * width, transcendentals=0
        ),
        name="attend",
    )(qkv, ob.reshape(steps, heads, 2 * length))


def attend_back_kernel(
    blocks, heads, qkv_ref, ob_ref, da_ref, summed_ref, total_ref, dqkv_ref, diag_ref,
    bias, diff, qt, kt, km, vt, dm, dmt, dt, acc_k, acc_v,
):
    width = qkv_ref.shape[2]
    lanes = [slice(head * HEAD_DIM, (head + 1) * HEAD_DIM) for head in range(heads)]
    for head in range(heads):
        fill_bias(ob_ref, head, bias.at[head], blocks)
    diff[...] = jnp.zeros_like(diff)
    acc_k[...] = jnp.zeros_like(acc_k)
    acc_v[...] = jnp.zeros_like(acc_v)
    row = lax.broadcasted_iota(jnp.int32, (width, 1), 0) // HEAD_DIM
    scale = jnp.asarray(score_scale, bf16)
    for b in range(blocks):
        rows = slice(b * BLOCK, (b + 1) * BLOCK)
        qt[:, rows] = transposed(qkv_ref[0, rows, :]) * scale
        turned = transposed(qkv_ref[1, rows, :])
        vt[:, rows] = transposed(qkv_ref[2, rows, :])
        grad = da_ref[rows, :].astype(f32)
        total = total_ref[rows, :]
        scaled = grad / total
        dmt[:, rows] = transposed(scaled)
        inner = scaled * summed_ref[rows, :] / total
        for head in range(heads):
            mask = lane_mask(width, head, f32)
            kt[head, :, rows] = turned * (row == head).astype(bf16)
            km[head, rows, :] = qkv_ref[1, rows, :] * lane_mask(width, head, bf16)
            dm[head, rows, :] = (scaled * mask).astype(bf16)
            shift = -jnp.sum(inner * mask, axis=1, keepdims=True)
            dt[head, rows, :] = jnp.broadcast_to(shift, (BLOCK, 128))

    for qb in range(blocks):
        rows = slice(qb * BLOCK, (qb + 1) * BLOCK)
        queries = qkv_ref[0, rows, :] * scale
        shifts = [dt[head, rows, :] for head in range(heads)]

        def step(kb, acc_q):
            cols = pl.ds(pl.multiple_of(kb * BLOCK, BLOCK), BLOCK)
            for head in range(heads):
                score = jnp.dot(queries, kt[head, :, cols], preferred_element_type=f32)
                expo = jnp.exp(score + bias[head, qb - kb])
                probs = jnp.dot(dm[head, rows, :], vt[:, cols], preferred_element_type=f32)
                shift = jnp.concatenate([shifts[head]] * (BLOCK // 128), axis=1)
                dscore = (expo * (probs + shift)).astype(bf16)
                diff[head, qb - kb] += dscore.astype(f32)
                acc_q = acc_q + jnp.dot(dscore, km[head, cols, :], preferred_element_type=f32)
                acc_k[lanes[head], cols] += jnp.dot(
                    qt[lanes[head], rows], dscore, preferred_element_type=f32
                )
                acc_v[lanes[head], cols] += jnp.dot(
                    dmt[lanes[head], rows], expo.astype(bf16), preferred_element_type=f32
                )
            return acc_q

        acc_q = jnp.zeros((BLOCK, width), f32)
        for kb in range(qb + 1):
            acc_q = step(kb, acc_q)
        dqkv_ref[0, rows, :] = (acc_q * score_scale).astype(bf16)

    lower = lax.broadcasted_iota(jnp.int32, (8, 2 * BLOCK), 0)
    for head in range(heads):
        for d in range(blocks):

            def add_rows(i, fold):
                part = diff[head, d, pl.ds(pl.multiple_of(i * 8, 8), 8), :]
                wide = jnp.concatenate([jnp.zeros((8, BLOCK), f32), part], axis=1)
                return fold + pltpu.roll(wide, 2 * BLOCK - 8 * i, 1)

            fold = lax.fori_loop(
                0, BLOCK // 8, add_rows, jnp.zeros((8, 2 * BLOCK), f32), unroll=8
            )
            for bit in (1, 2, 4):
                fold = jnp.where((lower & bit) != 0, pltpu.roll(fold, 2 * BLOCK - bit, 1), fold)
            diag_ref[0, pl.ds(head * blocks + d, 1), :] = jnp.sum(fold, axis=0, keepdims=True)
    for b in range(blocks):
        rows = slice(b * BLOCK, (b + 1) * BLOCK)
        dqkv_ref[1, rows, :] = acc_k[:, rows].T.astype(bf16)
        dqkv_ref[2, rows, :] = acc_v[:, rows].T.astype(bf16)


def attend_back(qkv, ob, grad, summed, total):
    _, length, width = qkv.shape
    lanes = min(width, 128)
    heads = lanes // HEAD_DIM
    steps = width // lanes
    blocks = length // BLOCK
    rows = pl.BlockSpec((length, lanes), lambda i: (0, i))
    wide = pl.BlockSpec((3, length, lanes), lambda i: (0, 0, i))
    dqkv, diag = pl.pallas_call(
        partial(attend_back_kernel, blocks, heads),
        grid=(steps,),
        in_specs=[wide, pl.BlockSpec((1, heads, 2 * length), lambda i: (i, 0, 0)), rows, rows, rows],
        out_specs=[wide, pl.BlockSpec((1, heads * blocks, 2 * BLOCK), lambda i: (i, 0, 0))],
        out_shape=[
            jax.ShapeDtypeStruct((3, length, width), bf16),
            jax.ShapeDtypeStruct((steps, heads * blocks, 2 * BLOCK), f32),
        ],
        scratch_shapes=[
            pltpu.VMEM((heads, blocks, BLOCK, BLOCK), f32),
            pltpu.VMEM((heads, blocks, BLOCK, BLOCK), f32),
            pltpu.VMEM((lanes, length), bf16),
            pltpu.VMEM((heads, lanes, length), bf16),
            pltpu.VMEM((heads, length, lanes), bf16),
            pltpu.VMEM((lanes, length), bf16),
            pltpu.VMEM((heads, length, lanes), bf16),
            pltpu.VMEM((lanes, length), bf16),
            pltpu.VMEM((heads, length, 128), f32),
            pltpu.VMEM((lanes, length), f32),
            pltpu.VMEM((lanes, length), f32),
        ],
        compiler_params=pltpu.CompilerParams(vmem_limit_bytes=56 << 20),
        cost_estimate=pl.CostEstimate(
            flops=10 * length * length * width, bytes_accessed=30 * length * width, transcendentals=0
        ),
        name="attend_back",
    )(qkv, ob.reshape(steps, heads, 2 * length), grad, summed, total)
    return dqkv, diag.reshape(steps * heads, blocks, 2 * BLOCK)


def norm_back(norm_input, factor, gain_wide, grad_normed):
    scaled = grad_normed * gain_wide
    gain_grad = jnp.sum(grad_normed * norm_input * factor, axis=0)
    mean_term = jnp.mean(scaled * norm_input, axis=-1, keepdims=True)
    return (factor * scaled - norm_input * factor * factor * factor * mean_term, gain_grad)


def adamw_step(master, gradient, first_old, second_old):
    first_new = decay_rate * first_old + (1.0 - decay_rate) * gradient
    second_new = decay_rate * second_old + (1.0 - decay_rate) * gradient * gradient
    correct = 1.0 - decay_rate**STEP
    update = -learn_rate * (
        first_new / correct / (jnp.sqrt(second_new / correct) + eps_adam) + weight_decay * master
    )
    return (gradient, first_new, second_new, update)


def layer(tokens, cotangent, bucket_ids, routes, *state):
    masters, firsts, seconds = state[:9], state[9:18], state[18:]
    (
        qkv_master, out_master, router_master, gain_attn_master, gain_mix_master, table_master,
        gate_master, up_master, down_master,
    ) = masters
    micro, tok_rows = tokens.shape[0], tokens.shape[2]
    cycle = lax.axis_size("ctx")
    count = cycle * EXP_AXIS
    length = tok_rows * cycle
    group = cycle // micro
    width = D // group
    place = lax.axis_index("ctx")
    head_group = place % group
    line = cycle // 2
    line_place = place // 2
    rows = D // count
    experts_all = router_master.shape[1]
    capacity = 5 * tok_rows * TOP // (4 * experts_all)
    low = my_bit(0) == 0

    tok = tokens[:, 0]
    cols = qkv_master.astype(bf16).reshape(3 * rows, group, width).transpose(1, 0, 2)
    small = jnp.concatenate(
        [
            router_master.reshape(-1), gain_attn_master, gain_mix_master, table_master,
        ]
    ).astype(bf16)
    small_size = small.shape[0]
    small = jnp.pad(small, (0, 16 * width - small_size)).reshape(1, 16, width)
    cols = jnp.concatenate([cols, jnp.broadcast_to(small, (group, 16, width))], axis=1)
    w_out = lax.all_gather(out_master.astype(bf16), both, axis=0, tiled=True)
    pair_own = turn(jnp.concatenate([gate_master, up_master], axis=0).astype(bf16))
    down_own = turn(down_master[0].astype(bf16))
    seq, gathered = opening(tok, cols)
    pair_own, seq, gathered = lax.optimization_barrier((pair_own, seq, gathered))
    right, left = [pair_own], [pair_own]

    def line_round(step):
        right.append(line_permute(right[-1], 1, step))
        left.append(line_permute(left[-1], -1, step))

    def line_settle(value):
        value, right[-1], left[-1] = lax.optimization_barrier((value, right[-1], left[-1]))
        return value

    line_round(0)
    seq = seq.reshape(length, D)
    w_qkv = gathered[:, :, : 3 * rows].reshape(EXP_AXIS, cycle, 3, rows, width)
    w_qkv = w_qkv.transpose(2, 1, 0, 3, 4).reshape(3, D, width)
    small = gathered[:, :, 3 * rows :].reshape(EXP_AXIS, cycle, 16 * width)[:, :, :small_size]
    small = small.transpose(1, 0, 2).reshape(count, small_size)
    edges = (0, rows * experts_all, rows * (experts_all + 1), rows * (experts_all + 2))
    router_bf = small[:, : edges[1]].reshape(D, experts_all)
    gain_attn = small[:, edges[1] : edges[2]].reshape(D).astype(f32)
    gain_mix = small[:, edges[2] : edges[3]].reshape(D).astype(f32)
    table = small[:, edges[3] :].reshape(HEADS, -1)
    bucket_count = table.shape[1]
    router_wide = router_bf.astype(f32)
    bucket_hits = bucket_ids[:, None] == jnp.arange(bucket_count, dtype=jnp.int32)[None, :]
    own_heads = HEADS // group
    own_table = lax.dynamic_slice_in_dim(table, head_group * own_heads, own_heads, 0)
    offset_bias = lax.dot_general(
        own_table, bucket_hits.astype(bf16), last_dims, preferred_element_type=f32
    )
    offset_bias = jnp.pad(offset_bias, ((0, 0), (1, 0)))[:, :-1]

    seq_wide = seq.astype(f32)
    seq_factor = lax.rsqrt(jnp.mean(seq_wide * seq_wide, axis=-1, keepdims=True) + eps_norm)
    normed = (seq_wide * seq_factor * gain_attn).astype(bf16)
    qkv = jnp.einsum("td,cde->cte", normed, w_qkv, preferred_element_type=f32).astype(bf16)
    attended, summed, total = attend(qkv, offset_bias)

    attended = line_settle(attended)
    back = cycle_swap(attended.reshape(cycle, tok_rows, width), 1)
    back = line_settle(back)
    line_round(1)
    toks = micro * tok_rows
    attended_bf = back.reshape(micro, group, tok_rows, width).transpose(0, 2, 1, 3)
    attended_bf = attended_bf.reshape(toks, D)
    inputs = tok.reshape(toks, D).astype(f32)
    factor_attn = lax.rsqrt(jnp.mean(inputs * inputs, axis=-1, keepdims=True) + eps_norm)
    hidden_state = inputs + jnp.dot(attended_bf, w_out, preferred_element_type=f32)
    factor_mix = lax.rsqrt(jnp.mean(hidden_state * hidden_state, axis=-1, keepdims=True) + eps_norm)
    normed_mix = hidden_state * factor_mix * gain_mix
    normed_bf = normed_mix.astype(bf16)
    logits = jnp.dot(normed_bf, router_bf, preferred_element_type=f32)
    router_probs = jax.nn.softmax(logits, axis=-1)
    route_rows = routes.reshape(micro, tok_rows, TOP)
    expert_ids = jnp.arange(experts_all, dtype=jnp.int32)
    picked = (route_rows.reshape(toks, TOP)[:, :, None] == expert_ids).astype(f32)
    chosen = jnp.sum(picked * router_probs[:, None, :], axis=-1)
    chosen_sum = jnp.sum(chosen, axis=-1, keepdims=True)
    gate_share = chosen / chosen_sum
    flat_routes = route_rows.reshape(micro, tok_rows * TOP)
    route_hits = (flat_routes[:, :, None] == expert_ids).astype(jnp.int32)
    before = jnp.cumsum(route_hits, axis=1) - route_hits
    micro_ids = jnp.arange(micro, dtype=jnp.int32)[:, None]
    slot_index = (flat_routes * micro + micro_ids) * capacity + jnp.sum(before * route_hits, axis=-1)
    slot_index = slot_index.reshape(toks, TOP)
    slot_count = experts_all * micro * capacity
    slot_ids = jnp.arange(slot_count, dtype=jnp.int32)
    hits = [(slot_index[:, choice, None] == slot_ids).astype(bf16) for choice in range(TOP)]
    slots = (experts_all, micro, capacity, D)
    sent_rows = lax.dot_general(sum(hits), normed_bf, first_dims, preferred_element_type=f32)
    dy_rows = cotangent.reshape(toks, D).astype(f32)
    scaled_dy = [
        (gate_share[:, choice, None] * dy_rows).astype(bf16) for choice in range(TOP)
    ]
    sent_grads = lax.dot_general(
        jnp.concatenate(hits, axis=0), jnp.concatenate(scaled_dy, axis=0), first_dims,
        preferred_element_type=f32,
    )
    sent_rows, down_own = lax.optimization_barrier((line_settle(sent_rows.astype(bf16)), down_own))
    if line > 3:
        line_round(2)
    got_rows, got_grads = plane_swap(
        (sent_rows.reshape(slots), sent_grads.astype(bf16).reshape(slots)), True, 2
    )
    for step in range(3, line - 1):
        line_round(step)
    flat_rows = got_rows.reshape(-1, D)
    flat_grads = got_grads.reshape(-1, D)

    blocks = []
    for k in range(line):
        mine = pair_own
        if k:
            mine = jnp.where(line_place + k < line, left[k], right[line - k])
        blocks += [mine, swap_bit(mine, 0)]
    w_down = gather_expert(down_own)
    kernels = pair_own.shape[1] % 128 == 0
    if kernels:
        units, value, slope = expert_front(flat_rows, blocks)
    else:

        def whole(part):
            pieces = []
            for mine, theirs in zip(blocks[::2], blocks[1::2]):
                pieces += [jnp.where(low, mine, theirs)[part], jnp.where(low, theirs, mine)[part]]
            return jnp.concatenate(pieces, axis=0)

        def turned(value, shift):
            twice = jnp.concatenate([value, value], axis=1)
            return lax.dynamic_slice_in_dim(twice, shift * (D // line), D, 1)

        w_gate, w_up = whole(0), whole(1)
        turned_rows = turned(flat_rows, line_place)
        gate_pre = jnp.dot(turned_rows, w_gate, preferred_element_type=f32)
        up_pre = jnp.dot(turned_rows, w_up, preferred_element_type=f32)
        value, slope = gelu_pair(gate_pre)
        units, slope = (value * up_pre).astype(bf16), slope * up_pre
    down_grad = lax.dot_general(units, flat_grads, first_dims, preferred_element_type=f32)
    down_sum = scatter_expert(core_sum(down_grad.astype(bf16)))
    grad_gate, grad_up = expert_middle(flat_grads, w_down, value, slope)
    up_grad = lax.dot_general(flat_rows, grad_up, first_dims, preferred_element_type=f32)
    up_sum = scatter_expert(core_sum(up_grad.astype(bf16)))
    gate_grad = lax.dot_general(flat_rows, grad_gate, first_dims, preferred_element_type=f32)
    gate_sum = scatter_expert(core_sum(gate_grad.astype(bf16)))
    out_rows = jnp.dot(units, w_down, preferred_element_type=f32).astype(bf16)
    if kernels:
        grad_rows = expert_rear(grad_gate, grad_up, blocks)
    else:
        grad_rows = lax.dot_general(grad_gate, w_gate, last_dims, preferred_element_type=f32)
        grad_rows = grad_rows + lax.dot_general(
            grad_up, w_up, last_dims, preferred_element_type=f32
        )
        grad_rows = turned(grad_rows.astype(bf16), line - line_place)
    back_out, back_grad = plane_swap((out_rows.reshape(slots), grad_rows.reshape(slots)), False, 3)
    back_out, back_grad = back_out.reshape(slot_count, D), back_grad.reshape(slot_count, D)

    returned = [jnp.dot(hit, back_out, preferred_element_type=f32) for hit in hits]
    mix_out = sum(gate_share[:, c, None] * returned[c] for c in range(TOP))
    output = (hidden_state + mix_out).astype(bf16)
    grad_gates = jnp.stack([jnp.sum(dy_rows * returned[c], axis=-1) for c in range(TOP)], axis=1)
    grad_chosen = grad_gates / chosen_sum - jnp.sum(grad_gates * chosen, axis=-1, keepdims=True) / (
        chosen_sum * chosen_sum
    )
    grad_probs = jnp.sum(grad_chosen[:, :, None] * picked, axis=1)
    grad_logits = router_probs * (
        grad_probs - jnp.sum(router_probs * grad_probs, axis=-1, keepdims=True)
    )
    router_grad = lax.dot_general(
        normed_bf.astype(f32), grad_logits, first_dims, precision=highest
    )
    grad_normed = jnp.dot(sum(hits), back_grad, preferred_element_type=f32) + lax.dot_general(
        grad_logits, router_wide, last_dims, precision=highest
    )
    grad_hidden, gain_mix_grad = norm_back(hidden_state, factor_mix, gain_mix, grad_normed)
    grad_hidden = grad_hidden + dy_rows
    grad_branch = grad_hidden.astype(bf16)
    grad_attended = lax.dot_general(grad_branch, w_out, last_dims, preferred_element_type=f32)
    grad_attended = grad_attended.astype(bf16).reshape(micro, tok_rows, group, width)
    grad_attended = grad_attended.transpose(0, 2, 1, 3).reshape(cycle, tok_rows, width)
    grad_attended = cycle_swap(grad_attended, 4).reshape(length, width)
    out_grad = lax.dot_general(attended_bf, grad_branch, first_dims, preferred_element_type=f32)
    out_grad = out_grad.astype(bf16).reshape(cycle, 2, 2, rows, D).transpose(2, 1, 0, 3, 4)
    out_grad = cube_sum(out_grad, 0)
    out_grad = cube_sum(out_grad, 1)

    dqkv, diag = attend_back(qkv, offset_bias, grad_attended, summed, total)
    qkv_grad = jnp.einsum("td,cte->cde", normed, dqkv, preferred_element_type=f32)
    qkv_grad = qkv_grad.astype(bf16).reshape(3, cycle, 2, 2, rows, width)
    qkv_grad = qkv_grad.transpose(3, 2, 1, 0, 4, 5)
    qkv_grad = cube_sum(qkv_grad, 0)
    qkv_grad = cube_sum(qkv_grad, 1)
    partial_normed = jnp.einsum("cte,cde->td", dqkv, w_qkv, preferred_element_type=f32)
    partial_normed = partial_normed.astype(bf16).reshape(cycle, tok_rows, D)
    pieces = cycle_swap(partial_normed, 5)
    grad_normed_attn = jnp.sum(pieces.reshape(micro, group, tok_rows, D).astype(f32), axis=1)
    grad_inputs, gain_attn_grad = norm_back(
        inputs, factor_attn, gain_attn, grad_normed_attn.reshape(toks, D)
    )
    grad_inputs = grad_inputs + grad_hidden

    blocks = length // BLOCK
    offset_grad = jnp.zeros((own_heads, 2 * length), f32)
    for d in range(blocks):
        first = (blocks - d - 1) * BLOCK
        offset_grad = offset_grad + jnp.pad(
            diag[:, d], ((0, 0), (first, 2 * length - first - 2 * BLOCK))
        )
    offset_grad = jnp.pad(offset_grad[:, 1:], ((0, 0), (0, 1)))
    own_grad = jnp.dot(offset_grad, bucket_hits.astype(f32), precision=highest)
    table_grad = lax.dynamic_update_slice_in_dim(
        jnp.zeros((HEADS, bucket_count), f32), own_grad, head_group * own_heads, 0
    )
    small_grads = jnp.concatenate(
        [
            router_grad.reshape(count, -1), gain_attn_grad.reshape(count, -1),
            gain_mix_grad.reshape(count, -1), table_grad.reshape(count, -1),
        ],
        axis=1,
    )
    small_grads = jnp.pad(small_grads, ((0, 0), (0, -small_grads.shape[1] % 128)))
    small_grads = small_grads.reshape(cycle, EXP_AXIS, 1, -1)
    qkv_grad, out_grad, small_parts = closing(qkv_grad, out_grad, small_grads)
    qkv_sum = jnp.sum(qkv_grad.reshape(micro, group, 3, rows, width).astype(f32), axis=0)
    qkv_sum = qkv_sum.transpose(1, 2, 0, 3).reshape(3, rows, D)
    out_sum = jnp.sum(out_grad.astype(f32), axis=0)
    small_sum = jnp.sum(small_parts, axis=(0, 1))
    small_sum = lax.dynamic_index_in_dim(small_sum, lax.axis_index("exp"), 0, keepdims=False)
    small_sum = small_sum[0, :small_size]
    gradients = (
        qkv_sum,
        out_sum,
        small_sum[: edges[1]].reshape(rows, experts_all),
        small_sum[edges[1] : edges[2]],
        small_sum[edges[2] : edges[3]],
        small_sum[edges[3] :],
        *(total[None].astype(f32) for total in (gate_sum, up_sum, down_sum)),
    )
    results = [
        adamw_step(master, gradient, first_old, second_old)
        for master, gradient, first_old, second_old in zip(masters, gradients, firsts, seconds)
    ]
    flat = [result[kind] for kind in range(4) for result in results]
    return (output.reshape(tokens.shape), grad_inputs.reshape(tokens.shape), *flat)


def solution(mesh):
    token_spec = P(None, "exp", "ctx", None)
    weight_specs = (
        P(None, both, None), P(both, None), P(both, None), P(both), P(both), P(both),
        P("exp", "ctx", None), P("exp", "ctx", None), P("exp", "ctx", None),
    )
    return jax.shard_map(
        layer,
        mesh=mesh,
        in_specs=(token_spec, token_spec, P(), token_spec) + weight_specs * 3,
        out_specs=(token_spec, token_spec) + weight_specs * 4,
        check_vma=False,
    )
```

```python
from functools import partial
import math

import jax
import jax.numpy as jnp
from jax import lax
from jax.experimental import pallas as pl
from jax.experimental.pallas import tpu as pltpu
from jax.sharding import PartitionSpec as P

D = 1024
HEADS = 16
HEAD_DIM = 64
TOP = 2
BLOCK = 256
STEP = 3
EXP_AXIS = 4

eps_norm = 1e-06
eps_adam = 1e-08
score_scale = 0.125
decay_rate = 0.5
learn_rate = 1.0
weight_decay = 0.1
highest = lax.Precision.HIGHEST
last_dims = (((1,), (1,)), ((), ()))
first_dims = (((0,), (0,)), ((), ()))
bf16 = jnp.bfloat16
f32 = jnp.float32
both = ("ctx", "exp")
MESH = pl.DeviceIdType.MESH


def swap_bit(value, bit):
    count = lax.axis_size("ctx") * EXP_AXIS
    return lax.ppermute(value, both, [(d, d ^ (1 << bit)) for d in range(count)])


def flat_index():
    return lax.axis_index("ctx") * EXP_AXIS + lax.axis_index("exp")


def my_bit(bit):
    return (flat_index() >> bit) & 1


def turn(value):
    count = lax.axis_size("ctx") * EXP_AXIS

    def other(d):
        low, high = d & 1, (d >> 2) & 1
        return (d & ~5) | (low << 2) | high

    got = lax.ppermute(value, both, [(d, other(d)) for d in range(count) if other(d) != d])
    return jnp.where(my_bit(0) == my_bit(2), value, got)


def place_of(flat):
    return (flat // EXP_AXIS, flat % EXP_AXIS)


def greet(partners):
    barrier = pltpu.get_barrier_semaphore()
    for partner in partners:
        pl.semaphore_signal(barrier, inc=1, device_id=place_of(partner), device_id_type=MESH)
    pl.semaphore_wait(barrier, len(partners))


def remote(source, target, send, recv, partner):
    return pltpu.make_async_remote_copy(
        src_ref=source, dst_ref=target, send_sem=send, recv_sem=recv,
        device_id=place_of(partner), device_id_type=MESH,
    )


def exchange_call(kernel, number, arrays, shapes, sems):
    vmem = pl.BlockSpec(memory_space=pltpu.VMEM)
    sent = sum(array.size * array.dtype.itemsize for array in arrays)
    return pl.pallas_call(
        kernel,
        in_specs=[vmem] * len(arrays),
        out_specs=[vmem] * len(shapes),
        out_shape=shapes,
        scratch_shapes=[pltpu.SemaphoreType.DMA((size,)) for size in sems],
        compiler_params=pltpu.CompilerParams(
            collective_id=number, has_side_effects=True, vmem_limit_bytes=48 << 20
        ),
        cost_estimate=pl.CostEstimate(flops=0, bytes_accessed=8 * sent, transcendentals=0),
    )(*arrays)


def opening_kernel(cycle, group, tok_ref, col_ref, seq_ref, all_ref, s1, r1, s2, r2, s3, r3, s4, r4):
    me = flat_index()
    ctx, exp = place_of(me)
    greet([me ^ (rel * EXP_AXIS) for rel in range(1, cycle)] + [me ^ rel for rel in range(1, EXP_AXIS)])
    mine = ctx // group
    copies, relays, tokens, forwards = [], [], [], []
    for rel in range(1, cycle):
        peer = ctx ^ rel
        copies.append(
            remote(
                col_ref.at[lax.rem(peer, group)], all_ref.at[exp, ctx], s1.at[rel], r1.at[rel],
                me ^ (rel * EXP_AXIS),
            )
        )
    for far in range(group, cycle, group):
        relays.append(
            remote(
                tok_ref.at[mine ^ (far // group)], seq_ref.at[ctx], s2.at[far // group],
                r2.at[far // group], me ^ (far * EXP_AXIS),
            )
        )
    for rel in range(1, group):
        tokens.append(
            remote(
                tok_ref.at[mine], seq_ref.at[ctx], s3.at[rel], r3.at[rel], me ^ (rel * EXP_AXIS)
            )
        )
    for copy in copies + relays + tokens:
        copy.start()
    all_ref[exp, ctx] = col_ref[lax.rem(ctx, group)]
    seq_ref[ctx] = tok_ref[mine]
    for far, copy in zip(range(group, cycle, group), relays):
        copy.wait_recv()
        for rel in range(1, group):
            slot = far + rel
            tokens.append(
                remote(
                    seq_ref.at[ctx ^ far], seq_ref.at[ctx ^ far], s3.at[slot], r3.at[slot],
                    me ^ (rel * EXP_AXIS),
                )
            )
            tokens[-1].start()
    for copy in copies:
        copy.wait()
    for rel in range(1, EXP_AXIS):
        forwards.append(
            remote(all_ref.at[exp], all_ref.at[exp], s4.at[rel], r4.at[rel], me ^ rel)
        )
        forwards[-1].start()
    for copy in relays:
        copy.wait_send()
    for copy in tokens + forwards:
        copy.wait()


def opening(tok, cols):
    cycle = lax.axis_size("ctx")
    group = cycle // tok.shape[0]
    return exchange_call(
        partial(opening_kernel, cycle, group), 0, [tok, cols],
        [
            jax.ShapeDtypeStruct((cycle,) + tok.shape[1:], tok.dtype),
            jax.ShapeDtypeStruct((EXP_AXIS, cycle) + cols.shape[1:], cols.dtype),
        ],
        [cycle, cycle, cycle, cycle, cycle, cycle, EXP_AXIS, EXP_AXIS],
    )


def cycle_kernel(cycle, in_ref, out_ref, send, recv):
    me = flat_index()
    ctx, _ = place_of(me)
    greet([me ^ (rel * EXP_AXIS) for rel in range(1, cycle)])
    copies = []
    for rel in range(1, cycle):
        copies.append(
            remote(
                in_ref.at[ctx ^ rel], out_ref.at[ctx], send.at[rel], recv.at[rel],
                me ^ (rel * EXP_AXIS),
            )
        )
        copies[-1].start()
    out_ref[ctx] = in_ref[ctx]
    for copy in copies:
        copy.wait()


def cycle_swap(value, number):
    cycle = lax.axis_size("ctx")
    return exchange_call(
        partial(cycle_kernel, cycle), number, [value],
        [jax.ShapeDtypeStruct(value.shape, value.dtype)], [cycle, cycle],
    )[0]


def closing_kernel(
    cycle, col_ref, out_in, small_ref, col_out, out_out, mid_ref, all_ref, s1, r1, s2, r2, s3, r3, s4, r4
):
    me = flat_index()
    ctx, exp = place_of(me)
    greet([me ^ (rel * EXP_AXIS) for rel in range(1, cycle)] + [me ^ rel for rel in range(1, EXP_AXIS)])
    smalls, copies = [], []
    for source, target, send, recv, out in (
        (small_ref, mid_ref, s3, r3, smalls), (col_ref, col_out, s1, r1, copies),
        (out_in, out_out, s2, r2, copies),
    ):
        for rel in range(1, cycle):
            out.append(
                remote(
                    source.at[ctx ^ rel], target.at[ctx], send.at[rel], recv.at[rel],
                    me ^ (rel * EXP_AXIS),
                )
            )
            out[-1].start()
    mid_ref[ctx] = small_ref[ctx]
    col_out[ctx] = col_ref[ctx]
    out_out[ctx] = out_in[ctx]
    for copy in smalls:
        copy.wait()
    for rel in range(1, EXP_AXIS):
        copies.append(remote(mid_ref, all_ref.at[exp], s4.at[rel], r4.at[rel], me ^ rel))
        copies[-1].start()
    all_ref[exp] = mid_ref[...]
    for copy in copies:
        copy.wait()


def closing(cols, out, small):
    cycle = lax.axis_size("ctx")
    results = exchange_call(
        partial(closing_kernel, cycle), 6, [cols, out, small],
        [jax.ShapeDtypeStruct(x.shape, x.dtype) for x in (cols, out, small)]
        + [jax.ShapeDtypeStruct((EXP_AXIS,) + small.shape, small.dtype)],
        [cycle] * 6 + [EXP_AXIS] * 2,
    )
    return results[0], results[1], results[3]


def plane_kernel(forward, arrays, *refs):
    ins, outs, send, recv = refs[:arrays], refs[arrays : 2 * arrays], refs[-2], refs[-1]
    me = flat_index()
    ctx, exp = place_of(me)
    greet([me ^ rel for rel in range(1, 2 * EXP_AXIS)])
    base = (ctx // 2) * 2
    ctx_low, exp_low = lax.rem(ctx, 2), lax.rem(exp, 2)
    for index in range(arrays):
        for e in range(EXP_AXIS):
            own = jnp.logical_and(exp == e, ctx_low == exp_low)
            sem = index * EXP_AXIS
            if forward:
                to_ctx, to_exp = base + e % 2, (e // 2) * 2 + ctx_low
                slot = exp
            else:
                to_ctx, to_exp = base + exp_low, e
                slot = (exp // 2) * 2 + ctx_low
            copy = remote(
                ins[index].at[e], outs[index].at[slot], send.at[sem + e], recv.at[sem + slot],
                to_ctx * EXP_AXIS + to_exp,
            )

            @pl.when(jnp.logical_not(own))
            def _():
                copy.start()

            @pl.when(own)
            def _():
                outs[index][e] = ins[index][e]

    for index in range(arrays):
        for e in range(EXP_AXIS):
            own = jnp.logical_and(exp == e, ctx_low == exp_low)
            sem = index * EXP_AXIS + e
            done = remote(ins[index].at[e], outs[index].at[e], send.at[sem], recv.at[sem], me ^ 1)

            @pl.when(jnp.logical_not(own))
            def _():
                done.wait()


def plane_swap(values, forward, number):
    count = len(values)
    return exchange_call(
        partial(plane_kernel, forward, count), number, list(values),
        [jax.ShapeDtypeStruct(x.shape, x.dtype) for x in values],
        [count * EXP_AXIS, count * EXP_AXIS],
    )


def line_permute(value, step, start):
    size = lax.axis_size("ctx") // 2
    pairs = []
    for a in range(size):
        b = a + step
        if 0 <= b < size and (a >= start if step > 0 else a < size - start):
            for low in range(2 * EXP_AXIS):
                pairs.append((a * 2 * EXP_AXIS + low, b * 2 * EXP_AXIS + low))
    return lax.ppermute(value, both, pairs)


def cube_sum(value, bit):
    mine = lax.dynamic_index_in_dim(value, my_bit(bit), 0, keepdims=False)
    theirs = lax.dynamic_index_in_dim(value, 1 - my_bit(bit), 0, keepdims=False)
    got = swap_bit(theirs, bit)
    return (mine.astype(f32) + got.astype(f32)).astype(value.dtype)


def pair_groups():
    count = lax.axis_size("ctx")
    return [[c for c in range(low, count, 2)] for low in range(2)]


def gather_expert(moved):
    mine = lax.all_gather(moved, "ctx", axis=0, axis_index_groups=pair_groups())
    theirs = swap_bit(mine, 0)
    low = my_bit(0) == 0
    whole = jnp.stack([jnp.where(low, mine, theirs), jnp.where(low, theirs, mine)], axis=1)
    return whole.reshape(-1, moved.shape[1])


def core_sum(grad):
    half = lax.axis_size("ctx") // 2
    value = grad.reshape(half, 2, grad.shape[0] // (2 * half), grad.shape[1])
    mine = lax.dynamic_index_in_dim(value, my_bit(0), 1, keepdims=False)
    theirs = lax.dynamic_index_in_dim(value, 1 - my_bit(0), 1, keepdims=False)
    got = swap_bit(theirs, 0)
    return (mine.astype(f32) + got.astype(f32)).astype(bf16)


def scatter_expert(half):
    part = lax.psum_scatter(half, "ctx", scatter_dimension=0, axis_index_groups=pair_groups())
    return turn(part)


def gelu_pair(value):
    inner = math.sqrt(2.0 / math.pi)
    square = value * value
    turned = jnp.tanh(inner * (value + 0.044715 * value * square))
    half = 0.5 * (1.0 + turned)
    slope = half + 0.5 * value * (1.0 - turned * turned) * inner * (1.0 + 3 * 0.044715 * square)
    return value * half, slope


def block_places(count, block):
    me = flat_index()
    line = count // 2
    place, low = me // (2 * EXP_AXIS), lax.rem(me, 2)
    out = []
    for k in range(line):
        for other in range(2):
            index = lax.rem(place + k, line) * 2 + (low + other * (1 - 2 * low))
            out.append(pl.ds(pl.multiple_of(index * block, block), block))
    return out


def expert_front_kernel(count, rows_ref, *refs):
    blocks = refs[:count]
    units_ref, value_ref, slope_ref, turned = refs[count:]
    block = blocks[0].shape[1]

    @pl.when(pl.program_id(0) == 0)
    def _():
        for k, places in enumerate(block_places(count, block)):
            turned[:, k * block : (k + 1) * block] = rows_ref[:, places]

    rows = turned[...]
    gate = jnp.dot(rows, jnp.concatenate([r[0] for r in blocks], 0), preferred_element_type=f32)
    up = jnp.dot(rows, jnp.concatenate([r[1] for r in blocks], 0), preferred_element_type=f32)
    value, slope = gelu_pair(gate)
    units_ref[...] = (value * up).astype(bf16)
    value_ref[...] = value.astype(bf16)
    slope_ref[...] = (slope * up).astype(bf16)


def expert_front(rows, blocks):
    count, cols, tile = len(blocks), blocks[0].shape[2], 256
    wide = pl.BlockSpec((rows.shape[0], tile), lambda j: (0, j))
    return pl.pallas_call(
        partial(expert_front_kernel, count),
        grid=(cols // tile,),
        in_specs=[pl.BlockSpec(rows.shape, lambda j: (0, 0))]
        + [pl.BlockSpec(blocks[0].shape[:2] + (tile,), lambda j: (0, 0, j))] * count,
        out_specs=[wide] * 3,
        out_shape=[jax.ShapeDtypeStruct((rows.shape[0], cols), bf16)] * 3,
        scratch_shapes=[pltpu.VMEM(rows.shape, bf16)],
        compiler_params=pltpu.CompilerParams(vmem_limit_bytes=48 << 20),
        cost_estimate=pl.CostEstimate(
            flops=4 * rows.size * cols, bytes_accessed=4 * D * cols, transcendentals=0
        ),
        name="expert_front",
    )(rows, *blocks)


def expert_middle_kernel(grads_ref, down_ref, value_ref, slope_ref, gate_ref, up_ref):
    grad = lax.dot_general(grads_ref[...], down_ref[...], last_dims, preferred_element_type=f32)
    gate_ref[...] = (grad * slope_ref[...].astype(f32)).astype(bf16)
    up_ref[...] = (grad * value_ref[...].astype(f32)).astype(bf16)


def expert_middle(grads, w_down, value, slope):
    cols, tile = w_down.shape[0], 256
    wide = pl.BlockSpec((grads.shape[0], tile), lambda j: (0, j))
    return pl.pallas_call(
        expert_middle_kernel,
        grid=(cols // tile,),
        in_specs=[
            pl.BlockSpec(grads.shape, lambda j: (0, 0)),
            pl.BlockSpec((tile, w_down.shape[1]), lambda j: (j, 0)),
            wide,
            wide,
        ],
        out_specs=[wide] * 2,
        out_shape=[jax.ShapeDtypeStruct((grads.shape[0], cols), bf16)] * 2,
        compiler_params=pltpu.CompilerParams(vmem_limit_bytes=48 << 20),
        cost_estimate=pl.CostEstimate(
            flops=2 * grads.size * cols, bytes_accessed=2 * D * cols, transcendentals=0
        ),
        name="expert_middle",
    )(grads, w_down, value, slope)


def expert_rear_kernel(count, gate_ref, up_ref, *refs):
    blocks = refs[:count]
    out_ref, total = refs[count:]
    block = blocks[0].shape[1]
    weights = jnp.concatenate(
        [jnp.concatenate([r[part] for r in blocks], 0) for part in range(2)], 1
    )
    grads = jnp.concatenate([gate_ref[...], up_ref[...]], 1)
    term = lax.dot_general(grads, weights, last_dims, preferred_element_type=f32)

    @pl.when(pl.program_id(0) == 0)
    def _():
        total[...] = term

    @pl.when(pl.program_id(0) > 0)
    def _():
        total[...] += term

    @pl.when(pl.program_id(0) == pl.num_programs(0) - 1)
    def _():
        for k, places in enumerate(block_places(count, block)):
            out_ref[:, places] = total[:, k * block : (k + 1) * block].astype(bf16)


def expert_rear(grad_gate, grad_up, blocks):
    count, cols, tile = len(blocks), blocks[0].shape[2], 256
    wide = pl.BlockSpec((grad_gate.shape[0], tile), lambda j: (0, j))
    shape = (grad_gate.shape[0], D)
    return pl.pallas_call(
        partial(expert_rear_kernel, count),
        grid=(cols // tile,),
        in_specs=[wide] * 2
        + [pl.BlockSpec(blocks[0].shape[:2] + (tile,), lambda j: (0, 0, j))] * count,
        out_specs=pl.BlockSpec(shape, lambda j: (0, 0)),
        out_shape=jax.ShapeDtypeStruct(shape, bf16),
        scratch_shapes=[pltpu.VMEM(shape, f32)],
        compiler_params=pltpu.CompilerParams(vmem_limit_bytes=48 << 20),
        cost_estimate=pl.CostEstimate(
            flops=4 * shape[0] * D * cols, bytes_accessed=4 * D * cols, transcendentals=0
        ),
        name="expert_rear",
    )(grad_gate, grad_up, *blocks)


def lane_mask(width, head, dtype):
    lane = lax.broadcasted_iota(jnp.int32, (1, width), 1)
    return ((lane // HEAD_DIM) == head).astype(dtype)


def fill_bias(ob_ref, head, bias, blocks):
    for d in range(blocks):
        first = (blocks - d - 1) * BLOCK
        window = ob_ref[0, pl.ds(head, 1), pl.ds(first, 2 * BLOCK)]
        wide = jnp.broadcast_to(window, (BLOCK, 2 * BLOCK))
        bias[d] = pltpu.roll(wide, 0, 1, stride=1, stride_axis=0)[:, BLOCK:]


def transposed(value):
    return value.astype(f32).T.astype(bf16)


def attend_kernel(blocks, heads, qkv_ref, ob_ref, att_ref, summed_ref, total_ref, bias, kt):
    width = qkv_ref.shape[2]
    for head in range(heads):
        fill_bias(ob_ref, head, bias.at[head], blocks)
    keep = [lane_mask(width, head, f32) for head in range(heads)]
    row = lax.broadcasted_iota(jnp.int32, (width, 1), 0) // HEAD_DIM
    for kb in range(blocks):
        cols = slice(kb * BLOCK, (kb + 1) * BLOCK)
        turned = transposed(qkv_ref[1, cols, :])
        for head in range(heads):
            kt[head, :, cols] = turned * (row == head).astype(bf16)

    for qb in range(blocks):
        rows = slice(qb * BLOCK, (qb + 1) * BLOCK)
        queries = qkv_ref[0, rows, :] * jnp.asarray(score_scale, bf16)

        def step(kb, carry):
            cols = pl.ds(pl.multiple_of(kb * BLOCK, BLOCK), BLOCK)
            values = qkv_ref[2, cols, :]
            out = []
            for head in range(heads):
                tot, acc = carry[head]
                score = jnp.dot(queries, kt[head, :, cols], preferred_element_type=f32)
                expo = jnp.exp(score + bias[head, qb - kb])
                tot = tot + (expo[:, :128] + expo[:, 128:])
                acc = acc + jnp.dot(expo.astype(bf16), values, preferred_element_type=f32)
                out.append((tot, acc))
            return tuple(out)

        carry = tuple(
            (jnp.zeros((BLOCK, 128), f32), jnp.zeros((BLOCK, width), f32)) for _ in range(heads)
        )
        for kb in range(qb + 1):
            carry = step(kb, carry)
        summed = sum(carry[head][1] * keep[head] for head in range(heads))
        total = sum(
            jnp.sum(carry[head][0], axis=1, keepdims=True) * keep[head] for head in range(heads)
        )
        summed_ref[rows, :] = summed
        total_ref[rows, :] = total
        att_ref[rows, :] = (summed / total).astype(bf16)


def attend(qkv, ob):
    _, length, width = qkv.shape
    lanes = min(width, 128)
    heads = lanes // HEAD_DIM
    steps = width // lanes
    blocks = length // BLOCK
    rows = pl.BlockSpec((length, lanes), lambda i: (0, i))
    return pl.pallas_call(
        partial(attend_kernel, blocks, heads),
        grid=(steps,),
        in_specs=[
            pl.BlockSpec((3, length, lanes), lambda i: (0, 0, i)),
            pl.BlockSpec((1, heads, 2 * length), lambda i: (i, 0, 0)),
        ],
        out_specs=[rows, rows, rows],
        out_shape=[
            jax.ShapeDtypeStruct((length, width), bf16),
            jax.ShapeDtypeStruct((length, width), f32),
            jax.ShapeDtypeStruct((length, width), f32),
        ],
        scratch_shapes=[
            pltpu.VMEM((heads, blocks, BLOCK, BLOCK), f32),
            pltpu.VMEM((heads, lanes, length), bf16),
        ],
        compiler_params=pltpu.CompilerParams(vmem_limit_bytes=48 << 20),
        cost_estimate=pl.CostEstimate(
            flops=4 * length * length * width, bytes_accessed=20 * length * width, transcendentals=0
        ),
        name="attend",
    )(qkv, ob.reshape(steps, heads, 2 * length))


def attend_back_kernel(
    blocks, heads, qkv_ref, ob_ref, da_ref, summed_ref, total_ref, dqkv_ref, diag_ref,
    bias, diff, qt, kt, km, vt, dm, dmt, dt, acc_k, acc_v,
):
    width = qkv_ref.shape[2]
    lanes = [slice(head * HEAD_DIM, (head + 1) * HEAD_DIM) for head in range(heads)]
    for head in range(heads):
        fill_bias(ob_ref, head, bias.at[head], blocks)
    diff[...] = jnp.zeros_like(diff)
    acc_k[...] = jnp.zeros_like(acc_k)
    acc_v[...] = jnp.zeros_like(acc_v)
    row = lax.broadcasted_iota(jnp.int32, (width, 1), 0) // HEAD_DIM
    scale = jnp.asarray(score_scale, bf16)
    for b in range(blocks):
        rows = slice(b * BLOCK, (b + 1) * BLOCK)
        qt[:, rows] = transposed(qkv_ref[0, rows, :]) * scale
        turned = transposed(qkv_ref[1, rows, :])
        vt[:, rows] = transposed(qkv_ref[2, rows, :])
        grad = da_ref[rows, :].astype(f32)
        total = total_ref[rows, :]
        scaled = grad / total
        dmt[:, rows] = transposed(scaled)
        inner = scaled * summed_ref[rows, :] / total
        for head in range(heads):
            mask = lane_mask(width, head, f32)
            kt[head, :, rows] = turned * (row == head).astype(bf16)
            km[head, rows, :] = qkv_ref[1, rows, :] * lane_mask(width, head, bf16)
            dm[head, rows, :] = (scaled * mask).astype(bf16)
            shift = -jnp.sum(inner * mask, axis=1, keepdims=True)
            dt[head, rows, :] = jnp.broadcast_to(shift, (BLOCK, 128))

    for qb in range(blocks):
        rows = slice(qb * BLOCK, (qb + 1) * BLOCK)
        queries = qkv_ref[0, rows, :] * scale
        shifts = [dt[head, rows, :] for head in range(heads)]

        def step(kb, acc_q):
            cols = pl.ds(pl.multiple_of(kb * BLOCK, BLOCK), BLOCK)
            for head in range(heads):
                score = jnp.dot(queries, kt[head, :, cols], preferred_element_type=f32)
                expo = jnp.exp(score + bias[head, qb - kb])
                probs = jnp.dot(dm[head, rows, :], vt[:, cols], preferred_element_type=f32)
                shift = jnp.concatenate([shifts[head]] * (BLOCK // 128), axis=1)
                dscore = (expo * (probs + shift)).astype(bf16)
                diff[head, qb - kb] += dscore.astype(f32)
                acc_q = acc_q + jnp.dot(dscore, km[head, cols, :], preferred_element_type=f32)
                acc_k[lanes[head], cols] += jnp.dot(
                    qt[lanes[head], rows], dscore, preferred_element_type=f32
                )
                acc_v[lanes[head], cols] += jnp.dot(
                    dmt[lanes[head], rows], expo.astype(bf16), preferred_element_type=f32
                )
            return acc_q

        acc_q = jnp.zeros((BLOCK, width), f32)
        for kb in range(qb + 1):
            acc_q = step(kb, acc_q)
        dqkv_ref[0, rows, :] = (acc_q * score_scale).astype(bf16)

    lower = lax.broadcasted_iota(jnp.int32, (8, 2 * BLOCK), 0)
    for head in range(heads):
        for d in range(blocks):

            def add_rows(i, fold):
                part = diff[head, d, pl.ds(pl.multiple_of(i * 8, 8), 8), :]
                wide = jnp.concatenate([jnp.zeros((8, BLOCK), f32), part], axis=1)
                return fold + pltpu.roll(wide, 2 * BLOCK - 8 * i, 1)

            fold = lax.fori_loop(
                0, BLOCK // 8, add_rows, jnp.zeros((8, 2 * BLOCK), f32), unroll=8
            )
            for bit in (1, 2, 4):
                fold = jnp.where((lower & bit) != 0, pltpu.roll(fold, 2 * BLOCK - bit, 1), fold)
            diag_ref[0, pl.ds(head * blocks + d, 1), :] = jnp.sum(fold, axis=0, keepdims=True)
    for b in range(blocks):
        rows = slice(b * BLOCK, (b + 1) * BLOCK)
        dqkv_ref[1, rows, :] = acc_k[:, rows].T.astype(bf16)
        dqkv_ref[2, rows, :] = acc_v[:, rows].T.astype(bf16)


def attend_back(qkv, ob, grad, summed, total):
    _, length, width = qkv.shape
    lanes = min(width, 128)
    heads = lanes // HEAD_DIM
    steps = width // lanes
    blocks = length // BLOCK
    rows = pl.BlockSpec((length, lanes), lambda i: (0, i))
    wide = pl.BlockSpec((3, length, lanes), lambda i: (0, 0, i))
    dqkv, diag = pl.pallas_call(
        partial(attend_back_kernel, blocks, heads),
        grid=(steps,),
        in_specs=[wide, pl.BlockSpec((1, heads, 2 * length), lambda i: (i, 0, 0)), rows, rows, rows],
        out_specs=[wide, pl.BlockSpec((1, heads * blocks, 2 * BLOCK), lambda i: (i, 0, 0))],
        out_shape=[
            jax.ShapeDtypeStruct((3, length, width), bf16),
            jax.ShapeDtypeStruct((steps, heads * blocks, 2 * BLOCK), f32),
        ],
        scratch_shapes=[
            pltpu.VMEM((heads, blocks, BLOCK, BLOCK), f32),
            pltpu.VMEM((heads, blocks, BLOCK, BLOCK), f32),
            pltpu.VMEM((lanes, length), bf16),
            pltpu.VMEM((heads, lanes, length), bf16),
            pltpu.VMEM((heads, length, lanes), bf16),
            pltpu.VMEM((lanes, length), bf16),
            pltpu.VMEM((heads, length, lanes), bf16),
            pltpu.VMEM((lanes, length), bf16),
            pltpu.VMEM((heads, length, 128), f32),
            pltpu.VMEM((lanes, length), f32),
            pltpu.VMEM((lanes, length), f32),
        ],
        compiler_params=pltpu.CompilerParams(vmem_limit_bytes=56 << 20),
        cost_estimate=pl.CostEstimate(
            flops=10 * length * length * width, bytes_accessed=30 * length * width, transcendentals=0
        ),
        name="attend_back",
    )(qkv, ob.reshape(steps, heads, 2 * length), grad, summed, total)
    return dqkv, diag.reshape(steps * heads, blocks, 2 * BLOCK)


def norm_back(norm_input, factor, gain_wide, grad_normed):
    scaled = grad_normed * gain_wide
    gain_grad = jnp.sum(grad_normed * norm_input * factor, axis=0)
    mean_term = jnp.mean(scaled * norm_input, axis=-1, keepdims=True)
    return (factor * scaled - norm_input * factor * factor * factor * mean_term, gain_grad)


def adamw_step(master, gradient, first_old, second_old):
    first_new = decay_rate * first_old + (1.0 - decay_rate) * gradient
    second_new = decay_rate * second_old + (1.0 - decay_rate) * gradient * gradient
    correct = 1.0 - decay_rate**STEP
    update = -learn_rate * (
        first_new / correct / (jnp.sqrt(second_new / correct) + eps_adam) + weight_decay * master
    )
    return (gradient, first_new, second_new, update)


def layer(tokens, cotangent, bucket_ids, routes, *state):
    masters, firsts, seconds = state[:9], state[9:18], state[18:]
    (
        qkv_master, out_master, router_master, gain_attn_master, gain_mix_master, table_master,
        gate_master, up_master, down_master,
    ) = masters
    micro, tok_rows = tokens.shape[0], tokens.shape[2]
    cycle = lax.axis_size("ctx")
    count = cycle * EXP_AXIS
    length = tok_rows * cycle
    group = cycle // micro
    width = D // group
    place = lax.axis_index("ctx")
    head_group = place % group
    line = cycle // 2
    line_place = place // 2
    rows = D // count
    experts_all = router_master.shape[1]
    capacity = 5 * tok_rows * TOP // (4 * experts_all)
    low = my_bit(0) == 0

    tok = tokens[:, 0]
    cols = qkv_master.astype(bf16).reshape(3 * rows, group, width).transpose(1, 0, 2)
    small = jnp.concatenate(
        [
            router_master.reshape(-1), gain_attn_master, gain_mix_master, table_master,
        ]
    ).astype(bf16)
    small_size = small.shape[0]
    small = jnp.pad(small, (0, 16 * width - small_size)).reshape(1, 16, width)
    cols = jnp.concatenate([cols, jnp.broadcast_to(small, (group, 16, width))], axis=1)
    w_out = lax.all_gather(out_master.astype(bf16), both, axis=0, tiled=True)
    pair_own = turn(jnp.concatenate([gate_master, up_master], axis=0).astype(bf16))
    down_own = turn(down_master[0].astype(bf16))
    right, left = [pair_own], [pair_own]

    def line_round(step):
        right.append(line_permute(right[-1], 1, step))
        left.append(line_permute(left[-1], -1, step))

    def line_settle(value):
        value, right[-1], left[-1] = lax.optimization_barrier((value, right[-1], left[-1]))
        return value

    line_round(0)
    seq, gathered = opening(tok, cols)
    seq = line_settle(seq)
    line_round(1)
    seq = seq.reshape(length, D)
    w_qkv = gathered[:, :, : 3 * rows].reshape(EXP_AXIS, cycle, 3, rows, width)
    w_qkv = w_qkv.transpose(2, 1, 0, 3, 4).reshape(3, D, width)
    small = gathered[:, :, 3 * rows :].reshape(EXP_AXIS, cycle, 16 * width)[:, :, :small_size]
    small = small.transpose(1, 0, 2).reshape(count, small_size)
    edges = (0, rows * experts_all, rows * (experts_all + 1), rows * (experts_all + 2))
    router_bf = small[:, : edges[1]].reshape(D, experts_all)
    gain_attn = small[:, edges[1] : edges[2]].reshape(D).astype(f32)
    gain_mix = small[:, edges[2] : edges[3]].reshape(D).astype(f32)
    table = small[:, edges[3] :].reshape(HEADS, -1)
    bucket_count = table.shape[1]
    router_wide = router_bf.astype(f32)
    bucket_hits = bucket_ids[:, None] == jnp.arange(bucket_count, dtype=jnp.int32)[None, :]
    own_heads = HEADS // group
    own_table = lax.dynamic_slice_in_dim(table, head_group * own_heads, own_heads, 0)
    offset_bias = lax.dot_general(
        own_table, bucket_hits.astype(bf16), last_dims, preferred_element_type=f32
    )
    offset_bias = jnp.pad(offset_bias, ((0, 0), (1, 0)))[:, :-1]

    seq_wide = seq.astype(f32)
    seq_factor = lax.rsqrt(jnp.mean(seq_wide * seq_wide, axis=-1, keepdims=True) + eps_norm)
    normed = (seq_wide * seq_factor * gain_attn).astype(bf16)
    qkv = jnp.einsum("td,cde->cte", normed, w_qkv, preferred_element_type=f32).astype(bf16)
    attended, summed, total = attend(qkv, offset_bias)

    back = cycle_swap(attended.reshape(cycle, tok_rows, width), 1)
    back = line_settle(back)
    if line > 3:
        line_round(2)
    toks = micro * tok_rows
    attended_bf = back.reshape(micro, group, tok_rows, width).transpose(0, 2, 1, 3)
    attended_bf = attended_bf.reshape(toks, D)
    inputs = tok.reshape(toks, D).astype(f32)
    factor_attn = lax.rsqrt(jnp.mean(inputs * inputs, axis=-1, keepdims=True) + eps_norm)
    hidden_state = inputs + jnp.dot(attended_bf, w_out, preferred_element_type=f32)
    factor_mix = lax.rsqrt(jnp.mean(hidden_state * hidden_state, axis=-1, keepdims=True) + eps_norm)
    normed_mix = hidden_state * factor_mix * gain_mix
    normed_bf = normed_mix.astype(bf16)
    logits = jnp.dot(normed_bf, router_bf, preferred_element_type=f32)
    router_probs = jax.nn.softmax(logits, axis=-1)
    route_rows = routes.reshape(micro, tok_rows, TOP)
    expert_ids = jnp.arange(experts_all, dtype=jnp.int32)
    picked = (route_rows.reshape(toks, TOP)[:, :, None] == expert_ids).astype(f32)
    chosen = jnp.sum(picked * router_probs[:, None, :], axis=-1)
    chosen_sum = jnp.sum(chosen, axis=-1, keepdims=True)
    gate_share = chosen / chosen_sum
    flat_routes = route_rows.reshape(micro, tok_rows * TOP)
    route_hits = (flat_routes[:, :, None] == expert_ids).astype(jnp.int32)
    before = jnp.cumsum(route_hits, axis=1) - route_hits
    micro_ids = jnp.arange(micro, dtype=jnp.int32)[:, None]
    slot_index = (flat_routes * micro + micro_ids) * capacity + jnp.sum(before * route_hits, axis=-1)
    slot_index = slot_index.reshape(toks, TOP)
    slot_count = experts_all * micro * capacity
    slot_ids = jnp.arange(slot_count, dtype=jnp.int32)
    hits = [(slot_index[:, choice, None] == slot_ids).astype(bf16) for choice in range(TOP)]
    slots = (experts_all, micro, capacity, D)
    sent_rows = lax.dot_general(sum(hits), normed_bf, first_dims, preferred_element_type=f32)
    dy_rows = cotangent.reshape(toks, D).astype(f32)
    scaled_dy = [
        (gate_share[:, choice, None] * dy_rows).astype(bf16) for choice in range(TOP)
    ]
    sent_grads = lax.dot_general(
        jnp.concatenate(hits, axis=0), jnp.concatenate(scaled_dy, axis=0), first_dims,
        preferred_element_type=f32,
    )
    sent_rows = sent_rows.astype(bf16)
    sent_grads = line_settle(sent_grads.astype(bf16))
    sent_grads, down_own = lax.optimization_barrier((sent_grads, down_own))
    got_rows, got_grads = plane_swap((sent_rows.reshape(slots), sent_grads.reshape(slots)), True, 2)
    for step in range(3, line - 1):
        line_round(step)
    flat_rows = got_rows.reshape(-1, D)
    flat_grads = got_grads.reshape(-1, D)

    blocks = []
    for k in range(line):
        mine = pair_own
        if k:
            mine = jnp.where(line_place + k < line, left[k], right[line - k])
        blocks += [mine, swap_bit(mine, 0)]
    w_down = gather_expert(down_own)
    kernels = pair_own.shape[1] % 128 == 0
    if kernels:
        units, value, slope = expert_front(flat_rows, blocks)
    else:

        def whole(part):
            pieces = []
            for mine, theirs in zip(blocks[::2], blocks[1::2]):
                pieces += [jnp.where(low, mine, theirs)[part], jnp.where(low, theirs, mine)[part]]
            return jnp.concatenate(pieces, axis=0)

        def turned(value, shift):
            twice = jnp.concatenate([value, value], axis=1)
            return lax.dynamic_slice_in_dim(twice, shift * (D // line), D, 1)

        w_gate, w_up = whole(0), whole(1)
        turned_rows = turned(flat_rows, line_place)
        gate_pre = jnp.dot(turned_rows, w_gate, preferred_element_type=f32)
        up_pre = jnp.dot(turned_rows, w_up, preferred_element_type=f32)
        value, slope = gelu_pair(gate_pre)
        units, slope = (value * up_pre).astype(bf16), slope * up_pre
    down_grad = lax.dot_general(units, flat_grads, first_dims, preferred_element_type=f32)
    down_sum = scatter_expert(core_sum(down_grad.astype(bf16)))
    grad_gate, grad_up = expert_middle(flat_grads, w_down, value, slope)
    up_grad = lax.dot_general(flat_rows, grad_up, first_dims, preferred_element_type=f32)
    up_sum = scatter_expert(core_sum(up_grad.astype(bf16)))
    gate_grad = lax.dot_general(flat_rows, grad_gate, first_dims, preferred_element_type=f32)
    gate_sum = scatter_expert(core_sum(gate_grad.astype(bf16)))
    out_rows = jnp.dot(units, w_down, preferred_element_type=f32).astype(bf16)
    if kernels:
        grad_rows = expert_rear(grad_gate, grad_up, blocks)
    else:
        grad_rows = lax.dot_general(grad_gate, w_gate, last_dims, preferred_element_type=f32)
        grad_rows = grad_rows + lax.dot_general(
            grad_up, w_up, last_dims, preferred_element_type=f32
        )
        grad_rows = turned(grad_rows.astype(bf16), line - line_place)
    back_out, back_grad = plane_swap((out_rows.reshape(slots), grad_rows.reshape(slots)), False, 3)
    back_out, back_grad = back_out.reshape(slot_count, D), back_grad.reshape(slot_count, D)

    returned = [jnp.dot(hit, back_out, preferred_element_type=f32) for hit in hits]
    mix_out = sum(gate_share[:, c, None] * returned[c] for c in range(TOP))
    output = (hidden_state + mix_out).astype(bf16)
    grad_gates = jnp.stack([jnp.sum(dy_rows * returned[c], axis=-1) for c in range(TOP)], axis=1)
    grad_chosen = grad_gates / chosen_sum - jnp.sum(grad_gates * chosen, axis=-1, keepdims=True) / (
        chosen_sum * chosen_sum
    )
    grad_probs = jnp.sum(grad_chosen[:, :, None] * picked, axis=1)
    grad_logits = router_probs * (
        grad_probs - jnp.sum(router_probs * grad_probs, axis=-1, keepdims=True)
    )
    router_grad = lax.dot_general(
        normed_bf.astype(f32), grad_logits, first_dims, precision=highest
    )
    grad_normed = jnp.dot(sum(hits), back_grad, preferred_element_type=f32) + lax.dot_general(
        grad_logits, router_wide, last_dims, precision=highest
    )
    grad_hidden, gain_mix_grad = norm_back(hidden_state, factor_mix, gain_mix, grad_normed)
    grad_hidden = grad_hidden + dy_rows
    grad_branch = grad_hidden.astype(bf16)
    grad_attended = lax.dot_general(grad_branch, w_out, last_dims, preferred_element_type=f32)
    grad_attended = grad_attended.astype(bf16).reshape(micro, tok_rows, group, width)
    grad_attended = grad_attended.transpose(0, 2, 1, 3).reshape(cycle, tok_rows, width)
    grad_attended = cycle_swap(grad_attended, 4).reshape(length, width)
    out_grad = lax.dot_general(attended_bf, grad_branch, first_dims, preferred_element_type=f32)
    out_grad = out_grad.astype(bf16).reshape(cycle, 2, 2, rows, D).transpose(2, 1, 0, 3, 4)
    out_grad = cube_sum(out_grad, 0)
    out_grad = cube_sum(out_grad, 1)

    dqkv, diag = attend_back(qkv, offset_bias, grad_attended, summed, total)
    partial_normed = jnp.einsum("cte,cde->td", dqkv, w_qkv, preferred_element_type=f32)
    partial_normed = partial_normed.astype(bf16).reshape(cycle, tok_rows, D)
    pieces = lax.all_to_all(partial_normed, "ctx", 0, 0, tiled=True)
    qkv_grad = jnp.einsum("td,cte->cde", normed, dqkv, preferred_element_type=f32)
    qkv_grad = qkv_grad.astype(bf16).reshape(3, cycle, 2, 2, rows, width)
    qkv_grad = qkv_grad.transpose(3, 2, 1, 0, 4, 5)
    qkv_grad = cube_sum(qkv_grad, 0)
    qkv_grad = cube_sum(qkv_grad, 1)
    grad_normed_attn = jnp.sum(pieces.reshape(micro, group, tok_rows, D).astype(f32), axis=1)
    grad_inputs, gain_attn_grad = norm_back(
        inputs, factor_attn, gain_attn, grad_normed_attn.reshape(toks, D)
    )
    grad_inputs = grad_inputs + grad_hidden

    blocks = length // BLOCK
    offset_grad = jnp.zeros((own_heads, 2 * length), f32)
    for d in range(blocks):
        first = (blocks - d - 1) * BLOCK
        offset_grad = offset_grad + jnp.pad(
            diag[:, d], ((0, 0), (first, 2 * length - first - 2 * BLOCK))
        )
    offset_grad = jnp.pad(offset_grad[:, 1:], ((0, 0), (0, 1)))
    own_grad = jnp.dot(offset_grad, bucket_hits.astype(f32), precision=highest)
    table_grad = lax.dynamic_update_slice_in_dim(
        jnp.zeros((HEADS, bucket_count), f32), own_grad, head_group * own_heads, 0
    )
    small_grads = jnp.concatenate(
        [
            router_grad.reshape(count, -1), gain_attn_grad.reshape(count, -1),
            gain_mix_grad.reshape(count, -1), table_grad.reshape(count, -1),
        ],
        axis=1,
    )
    small_grads = jnp.pad(small_grads, ((0, 0), (0, -small_grads.shape[1] % 128)))
    small_grads = small_grads.reshape(cycle, EXP_AXIS, 1, -1)
    qkv_grad, out_grad, small_parts = closing(qkv_grad, out_grad, small_grads)
    qkv_sum = jnp.sum(qkv_grad.reshape(micro, group, 3, rows, width).astype(f32), axis=0)
    qkv_sum = qkv_sum.transpose(1, 2, 0, 3).reshape(3, rows, D)
    out_sum = jnp.sum(out_grad.astype(f32), axis=0)
    small_sum = jnp.sum(small_parts, axis=(0, 1))
    small_sum = lax.dynamic_index_in_dim(small_sum, lax.axis_index("exp"), 0, keepdims=False)
    small_sum = small_sum[0, :small_size]
    gradients = (
        qkv_sum,
        out_sum,
        small_sum[: edges[1]].reshape(rows, experts_all),
        small_sum[edges[1] : edges[2]],
        small_sum[edges[2] : edges[3]],
        small_sum[edges[3] :],
        *(total[None].astype(f32) for total in (gate_sum, up_sum, down_sum)),
    )
    results = [
        adamw_step(master, gradient, first_old, second_old)
        for master, gradient, first_old, second_old in zip(masters, gradients, firsts, seconds)
    ]
    flat = [result[kind] for kind in range(4) for result in results]
    return (output.reshape(tokens.shape), grad_inputs.reshape(tokens.shape), *flat)


def solution(mesh):
    token_spec = P(None, "exp", "ctx", None)
    weight_specs = (
        P(None, both, None), P(both, None), P(both, None), P(both), P(both), P(both),
        P("exp", "ctx", None), P("exp", "ctx", None), P("exp", "ctx", None),
    )
    return jax.shard_map(
        layer,
        mesh=mesh,
        in_specs=(token_spec, token_spec, P(), token_spec) + weight_specs * 3,
        out_specs=(token_spec, token_spec) + weight_specs * 4,
        check_vma=False,
    )
```

```python
from functools import partial
import math

import jax
import jax.numpy as jnp
from jax import lax
from jax.experimental import pallas as pl
from jax.experimental.pallas import tpu as pltpu
from jax.sharding import PartitionSpec as P

D = 1024
HEADS = 16
HEAD_DIM = 64
TOP = 2
BLOCK = 256
STEP = 3
EXP_AXIS = 4

eps_norm = 1e-06
eps_adam = 1e-08
score_scale = 0.125
decay_rate = 0.5
learn_rate = 1.0
weight_decay = 0.1
highest = lax.Precision.HIGHEST
last_dims = (((1,), (1,)), ((), ()))
first_dims = (((0,), (0,)), ((), ()))
bf16 = jnp.bfloat16
f32 = jnp.float32
both = ("ctx", "exp")
MESH = pl.DeviceIdType.MESH


def swap_bit(value, bit):
    count = lax.axis_size("ctx") * EXP_AXIS
    return lax.ppermute(value, both, [(d, d ^ (1 << bit)) for d in range(count)])


def flat_index():
    return lax.axis_index("ctx") * EXP_AXIS + lax.axis_index("exp")


def my_bit(bit):
    return (flat_index() >> bit) & 1


def turn(value):
    count = lax.axis_size("ctx") * EXP_AXIS

    def other(d):
        low, high = d & 1, (d >> 2) & 1
        return (d & ~5) | (low << 2) | high

    got = lax.ppermute(value, both, [(d, other(d)) for d in range(count) if other(d) != d])
    return jnp.where(my_bit(0) == my_bit(2), value, got)


def place_of(flat):
    return (flat // EXP_AXIS, flat % EXP_AXIS)


def greet(partners):
    barrier = pltpu.get_barrier_semaphore()
    for partner in partners:
        pl.semaphore_signal(barrier, inc=1, device_id=place_of(partner), device_id_type=MESH)
    pl.semaphore_wait(barrier, len(partners))


def remote(source, target, send, recv, partner):
    return pltpu.make_async_remote_copy(
        src_ref=source, dst_ref=target, send_sem=send, recv_sem=recv,
        device_id=place_of(partner), device_id_type=MESH,
    )


def exchange_call(kernel, number, arrays, shapes, sems):
    vmem = pl.BlockSpec(memory_space=pltpu.VMEM)
    sent = sum(array.size * array.dtype.itemsize for array in arrays)
    return pl.pallas_call(
        kernel,
        in_specs=[vmem] * len(arrays),
        out_specs=[vmem] * len(shapes),
        out_shape=shapes,
        scratch_shapes=[pltpu.SemaphoreType.DMA((size,)) for size in sems],
        compiler_params=pltpu.CompilerParams(
            collective_id=number, has_side_effects=True, vmem_limit_bytes=48 << 20
        ),
        cost_estimate=pl.CostEstimate(flops=0, bytes_accessed=8 * sent, transcendentals=0),
    )(*arrays)


def opening_kernel(cycle, group, tok_ref, col_ref, seq_ref, all_ref, s1, r1, s2, r2, s3, r3, s4, r4):
    me = flat_index()
    ctx, exp = place_of(me)
    greet([me ^ (rel * EXP_AXIS) for rel in range(1, cycle)] + [me ^ rel for rel in range(1, EXP_AXIS)])
    mine = ctx // group
    copies, relays, tokens, forwards = [], [], [], []
    for rel in range(1, cycle):
        peer = ctx ^ rel
        copies.append(
            remote(
                col_ref.at[lax.rem(peer, group)], all_ref.at[exp, ctx], s1.at[rel], r1.at[rel],
                me ^ (rel * EXP_AXIS),
            )
        )
    for far in range(group, cycle, group):
        relays.append(
            remote(
                tok_ref.at[mine ^ (far // group)], seq_ref.at[ctx], s2.at[far // group],
                r2.at[far // group], me ^ (far * EXP_AXIS),
            )
        )
    for rel in range(1, group):
        tokens.append(
            remote(
                tok_ref.at[mine], seq_ref.at[ctx], s3.at[rel], r3.at[rel], me ^ (rel * EXP_AXIS)
            )
        )
    for copy in copies + relays + tokens:
        copy.start()
    all_ref[exp, ctx] = col_ref[lax.rem(ctx, group)]
    seq_ref[ctx] = tok_ref[mine]
    for far, copy in zip(range(group, cycle, group), relays):
        copy.wait_recv()
        for rel in range(1, group):
            slot = far + rel
            tokens.append(
                remote(
                    seq_ref.at[ctx ^ far], seq_ref.at[ctx ^ far], s3.at[slot], r3.at[slot],
                    me ^ (rel * EXP_AXIS),
                )
            )
            tokens[-1].start()
    for copy in copies:
        copy.wait()
    for rel in range(1, EXP_AXIS):
        forwards.append(
            remote(all_ref.at[exp], all_ref.at[exp], s4.at[rel], r4.at[rel], me ^ rel)
        )
        forwards[-1].start()
    for copy in relays:
        copy.wait_send()
    for copy in tokens + forwards:
        copy.wait()


def opening(tok, cols):
    cycle = lax.axis_size("ctx")
    group = cycle // tok.shape[0]
    return exchange_call(
        partial(opening_kernel, cycle, group), 0, [tok, cols],
        [
            jax.ShapeDtypeStruct((cycle,) + tok.shape[1:], tok.dtype),
            jax.ShapeDtypeStruct((EXP_AXIS, cycle) + cols.shape[1:], cols.dtype),
        ],
        [cycle, cycle, cycle, cycle, cycle, cycle, EXP_AXIS, EXP_AXIS],
    )


def cycle_kernel(cycle, in_ref, out_ref, send, recv):
    me = flat_index()
    ctx, _ = place_of(me)
    greet([me ^ (rel * EXP_AXIS) for rel in range(1, cycle)])
    copies = []
    for rel in range(1, cycle):
        copies.append(
            remote(
                in_ref.at[ctx ^ rel], out_ref.at[ctx], send.at[rel], recv.at[rel],
                me ^ (rel * EXP_AXIS),
            )
        )
        copies[-1].start()
    out_ref[ctx] = in_ref[ctx]
    for copy in copies:
        copy.wait()


def cycle_swap(value, number):
    cycle = lax.axis_size("ctx")
    return exchange_call(
        partial(cycle_kernel, cycle), number, [value],
        [jax.ShapeDtypeStruct(value.shape, value.dtype)], [cycle, cycle],
    )[0]


def closing_kernel(
    cycle, col_ref, out_in, small_ref, col_out, out_out, mid_ref, all_ref, s1, r1, s2, r2, s3, r3, s4, r4
):
    me = flat_index()
    ctx, exp = place_of(me)
    greet([me ^ (rel * EXP_AXIS) for rel in range(1, cycle)] + [me ^ rel for rel in range(1, EXP_AXIS)])
    smalls, copies = [], []
    for source, target, send, recv, out in (
        (small_ref, mid_ref, s3, r3, smalls), (col_ref, col_out, s1, r1, copies),
        (out_in, out_out, s2, r2, copies),
    ):
        for rel in range(1, cycle):
            out.append(
                remote(
                    source.at[ctx ^ rel], target.at[ctx], send.at[rel], recv.at[rel],
                    me ^ (rel * EXP_AXIS),
                )
            )
            out[-1].start()
    mid_ref[ctx] = small_ref[ctx]
    col_out[ctx] = col_ref[ctx]
    out_out[ctx] = out_in[ctx]
    for copy in smalls:
        copy.wait()
    for rel in range(1, EXP_AXIS):
        copies.append(remote(mid_ref, all_ref.at[exp], s4.at[rel], r4.at[rel], me ^ rel))
        copies[-1].start()
    all_ref[exp] = mid_ref[...]
    for copy in copies:
        copy.wait()


def closing(cols, out, small):
    cycle = lax.axis_size("ctx")
    results = exchange_call(
        partial(closing_kernel, cycle), 6, [cols, out, small],
        [jax.ShapeDtypeStruct(x.shape, x.dtype) for x in (cols, out, small)]
        + [jax.ShapeDtypeStruct((EXP_AXIS,) + small.shape, small.dtype)],
        [cycle] * 6 + [EXP_AXIS] * 2,
    )
    return results[0], results[1], results[3]


def plane_kernel(forward, arrays, *refs):
    ins, outs, send, recv = refs[:arrays], refs[arrays : 2 * arrays], refs[-2], refs[-1]
    me = flat_index()
    ctx, exp = place_of(me)
    greet([me ^ rel for rel in range(1, 2 * EXP_AXIS)])
    base = (ctx // 2) * 2
    ctx_low, exp_low = lax.rem(ctx, 2), lax.rem(exp, 2)
    for index in range(arrays):
        for e in range(EXP_AXIS):
            own = jnp.logical_and(exp == e, ctx_low == exp_low)
            sem = index * EXP_AXIS
            if forward:
                to_ctx, to_exp = base + e % 2, (e // 2) * 2 + ctx_low
                slot = exp
            else:
                to_ctx, to_exp = base + exp_low, e
                slot = (exp // 2) * 2 + ctx_low
            copy = remote(
                ins[index].at[e], outs[index].at[slot], send.at[sem + e], recv.at[sem + slot],
                to_ctx * EXP_AXIS + to_exp,
            )

            @pl.when(jnp.logical_not(own))
            def _():
                copy.start()

            @pl.when(own)
            def _():
                outs[index][e] = ins[index][e]

    for index in range(arrays):
        for e in range(EXP_AXIS):
            own = jnp.logical_and(exp == e, ctx_low == exp_low)
            sem = index * EXP_AXIS + e
            done = remote(ins[index].at[e], outs[index].at[e], send.at[sem], recv.at[sem], me ^ 1)

            @pl.when(jnp.logical_not(own))
            def _():
                done.wait()


def plane_swap(values, forward, number):
    count = len(values)
    return exchange_call(
        partial(plane_kernel, forward, count), number, list(values),
        [jax.ShapeDtypeStruct(x.shape, x.dtype) for x in values],
        [count * EXP_AXIS, count * EXP_AXIS],
    )


def line_permute(value, step, start):
    size = lax.axis_size("ctx") // 2
    pairs = []
    for a in range(size):
        b = a + step
        if 0 <= b < size and (a >= start if step > 0 else a < size - start):
            for low in range(2 * EXP_AXIS):
                pairs.append((a * 2 * EXP_AXIS + low, b * 2 * EXP_AXIS + low))
    return lax.ppermute(value, both, pairs)


def cube_sum(value, bit):
    mine = lax.dynamic_index_in_dim(value, my_bit(bit), 0, keepdims=False)
    theirs = lax.dynamic_index_in_dim(value, 1 - my_bit(bit), 0, keepdims=False)
    got = swap_bit(theirs, bit)
    return (mine.astype(f32) + got.astype(f32)).astype(value.dtype)


def pair_groups():
    count = lax.axis_size("ctx")
    return [[c for c in range(low, count, 2)] for low in range(2)]


def gather_expert(moved):
    mine = lax.all_gather(moved, "ctx", axis=0, axis_index_groups=pair_groups())
    theirs = swap_bit(mine, 0)
    low = my_bit(0) == 0
    whole = jnp.stack([jnp.where(low, mine, theirs), jnp.where(low, theirs, mine)], axis=1)
    return whole.reshape(-1, moved.shape[1])


def core_sum(grad):
    half = lax.axis_size("ctx") // 2
    value = grad.reshape(half, 2, grad.shape[0] // (2 * half), grad.shape[1])
    mine = lax.dynamic_index_in_dim(value, my_bit(0), 1, keepdims=False)
    theirs = lax.dynamic_index_in_dim(value, 1 - my_bit(0), 1, keepdims=False)
    got = swap_bit(theirs, 0)
    return (mine.astype(f32) + got.astype(f32)).astype(bf16)


def scatter_expert(half):
    part = lax.psum_scatter(half, "ctx", scatter_dimension=0, axis_index_groups=pair_groups())
    return turn(part)


def gelu_pair(value):
    inner = math.sqrt(2.0 / math.pi)
    square = value * value
    turned = jnp.tanh(inner * (value + 0.044715 * value * square))
    half = 0.5 * (1.0 + turned)
    slope = half + 0.5 * value * (1.0 - turned * turned) * inner * (1.0 + 3 * 0.044715 * square)
    return value * half, slope


def block_places(count, block):
    me = flat_index()
    line = count // 2
    place, low = me // (2 * EXP_AXIS), lax.rem(me, 2)
    out = []
    for k in range(line):
        for other in range(2):
            index = lax.rem(place + k, line) * 2 + (low + other * (1 - 2 * low))
            out.append(pl.ds(pl.multiple_of(index * block, block), block))
    return out


def expert_front_kernel(count, rows_ref, *refs):
    blocks = refs[:count]
    units_ref, value_ref, slope_ref, turned = refs[count:]
    block = blocks[0].shape[1]

    @pl.when(pl.program_id(0) == 0)
    def _():
        for k, places in enumerate(block_places(count, block)):
            turned[:, k * block : (k + 1) * block] = rows_ref[:, places]

    rows = turned[...]
    gate = jnp.dot(rows, jnp.concatenate([r[0] for r in blocks], 0), preferred_element_type=f32)
    up = jnp.dot(rows, jnp.concatenate([r[1] for r in blocks], 0), preferred_element_type=f32)
    value, slope = gelu_pair(gate)
    units_ref[...] = (value * up).astype(bf16)
    value_ref[...] = value.astype(bf16)
    slope_ref[...] = (slope * up).astype(bf16)


def expert_front(rows, blocks):
    count, cols, tile = len(blocks), blocks[0].shape[2], 256
    wide = pl.BlockSpec((rows.shape[0], tile), lambda j: (0, j))
    return pl.pallas_call(
        partial(expert_front_kernel, count),
        grid=(cols // tile,),
        in_specs=[pl.BlockSpec(rows.shape, lambda j: (0, 0))]
        + [pl.BlockSpec(blocks[0].shape[:2] + (tile,), lambda j: (0, 0, j))] * count,
        out_specs=[wide] * 3,
        out_shape=[jax.ShapeDtypeStruct((rows.shape[0], cols), bf16)] * 3,
        scratch_shapes=[pltpu.VMEM(rows.shape, bf16)],
        compiler_params=pltpu.CompilerParams(vmem_limit_bytes=48 << 20),
        cost_estimate=pl.CostEstimate(
            flops=4 * rows.size * cols, bytes_accessed=4 * D * cols, transcendentals=0
        ),
        name="expert_front",
    )(rows, *blocks)


def expert_middle_kernel(grads_ref, down_ref, value_ref, slope_ref, gate_ref, up_ref):
    grad = lax.dot_general(grads_ref[...], down_ref[...], last_dims, preferred_element_type=f32)
    gate_ref[...] = (grad * slope_ref[...].astype(f32)).astype(bf16)
    up_ref[...] = (grad * value_ref[...].astype(f32)).astype(bf16)


def expert_middle(grads, w_down, value, slope):
    cols, tile = w_down.shape[0], 256
    wide = pl.BlockSpec((grads.shape[0], tile), lambda j: (0, j))
    return pl.pallas_call(
        expert_middle_kernel,
        grid=(cols // tile,),
        in_specs=[
            pl.BlockSpec(grads.shape, lambda j: (0, 0)),
            pl.BlockSpec((tile, w_down.shape[1]), lambda j: (j, 0)),
            wide,
            wide,
        ],
        out_specs=[wide] * 2,
        out_shape=[jax.ShapeDtypeStruct((grads.shape[0], cols), bf16)] * 2,
        compiler_params=pltpu.CompilerParams(vmem_limit_bytes=48 << 20),
        cost_estimate=pl.CostEstimate(
            flops=2 * grads.size * cols, bytes_accessed=2 * D * cols, transcendentals=0
        ),
        name="expert_middle",
    )(grads, w_down, value, slope)


def expert_rear_kernel(count, gate_ref, up_ref, *refs):
    blocks = refs[:count]
    out_ref, total = refs[count:]
    block = blocks[0].shape[1]
    weights = jnp.concatenate(
        [jnp.concatenate([r[part] for r in blocks], 0) for part in range(2)], 1
    )
    grads = jnp.concatenate([gate_ref[...], up_ref[...]], 1)
    term = lax.dot_general(grads, weights, last_dims, preferred_element_type=f32)

    @pl.when(pl.program_id(0) == 0)
    def _():
        total[...] = term

    @pl.when(pl.program_id(0) > 0)
    def _():
        total[...] += term

    @pl.when(pl.program_id(0) == pl.num_programs(0) - 1)
    def _():
        for k, places in enumerate(block_places(count, block)):
            out_ref[:, places] = total[:, k * block : (k + 1) * block].astype(bf16)


def expert_rear(grad_gate, grad_up, blocks):
    count, cols, tile = len(blocks), blocks[0].shape[2], 256
    wide = pl.BlockSpec((grad_gate.shape[0], tile), lambda j: (0, j))
    shape = (grad_gate.shape[0], D)
    return pl.pallas_call(
        partial(expert_rear_kernel, count),
        grid=(cols // tile,),
        in_specs=[wide] * 2
        + [pl.BlockSpec(blocks[0].shape[:2] + (tile,), lambda j: (0, 0, j))] * count,
        out_specs=pl.BlockSpec(shape, lambda j: (0, 0)),
        out_shape=jax.ShapeDtypeStruct(shape, bf16),
        scratch_shapes=[pltpu.VMEM(shape, f32)],
        compiler_params=pltpu.CompilerParams(vmem_limit_bytes=48 << 20),
        cost_estimate=pl.CostEstimate(
            flops=4 * shape[0] * D * cols, bytes_accessed=4 * D * cols, transcendentals=0
        ),
        name="expert_rear",
    )(grad_gate, grad_up, *blocks)


def lane_mask(width, head, dtype):
    lane = lax.broadcasted_iota(jnp.int32, (1, width), 1)
    return ((lane // HEAD_DIM) == head).astype(dtype)


def fill_bias(ob_ref, head, bias, blocks):
    for d in range(blocks):
        first = (blocks - d - 1) * BLOCK
        window = ob_ref[0, pl.ds(head, 1), pl.ds(first, 2 * BLOCK)]
        wide = jnp.broadcast_to(window, (BLOCK, 2 * BLOCK))
        bias[d] = pltpu.roll(wide, 0, 1, stride=1, stride_axis=0)[:, BLOCK:]


def transposed(value):
    return value.astype(f32).T.astype(bf16)


def attend_kernel(blocks, heads, qkv_ref, ob_ref, att_ref, summed_ref, total_ref, bias, kt):
    width = qkv_ref.shape[2]
    for head in range(heads):
        fill_bias(ob_ref, head, bias.at[head], blocks)
    keep = [lane_mask(width, head, f32) for head in range(heads)]
    row = lax.broadcasted_iota(jnp.int32, (width, 1), 0) // HEAD_DIM
    for kb in range(blocks):
        cols = slice(kb * BLOCK, (kb + 1) * BLOCK)
        turned = transposed(qkv_ref[1, cols, :])
        for head in range(heads):
            kt[head, :, cols] = turned * (row == head).astype(bf16)

    for qb in range(blocks):
        rows = slice(qb * BLOCK, (qb + 1) * BLOCK)
        queries = qkv_ref[0, rows, :] * jnp.asarray(score_scale, bf16)

        def step(kb, carry):
            cols = pl.ds(pl.multiple_of(kb * BLOCK, BLOCK), BLOCK)
            values = qkv_ref[2, cols, :]
            out = []
            for head in range(heads):
                tot, acc = carry[head]
                score = jnp.dot(queries, kt[head, :, cols], preferred_element_type=f32)
                expo = jnp.exp(score + bias[head, qb - kb])
                tot = tot + (expo[:, :128] + expo[:, 128:])
                acc = acc + jnp.dot(expo.astype(bf16), values, preferred_element_type=f32)
                out.append((tot, acc))
            return tuple(out)

        carry = tuple(
            (jnp.zeros((BLOCK, 128), f32), jnp.zeros((BLOCK, width), f32)) for _ in range(heads)
        )
        for kb in range(qb + 1):
            carry = step(kb, carry)
        summed = sum(carry[head][1] * keep[head] for head in range(heads))
        total = sum(
            jnp.sum(carry[head][0], axis=1, keepdims=True) * keep[head] for head in range(heads)
        )
        summed_ref[rows, :] = summed
        total_ref[rows, :] = total
        att_ref[rows, :] = (summed / total).astype(bf16)


def attend(qkv, ob):
    _, length, width = qkv.shape
    lanes = min(width, 128)
    heads = lanes // HEAD_DIM
    steps = width // lanes
    blocks = length // BLOCK
    rows = pl.BlockSpec((length, lanes), lambda i: (0, i))
    return pl.pallas_call(
        partial(attend_kernel, blocks, heads),
        grid=(steps,),
        in_specs=[
            pl.BlockSpec((3, length, lanes), lambda i: (0, 0, i)),
            pl.BlockSpec((1, heads, 2 * length), lambda i: (i, 0, 0)),
        ],
        out_specs=[rows, rows, rows],
        out_shape=[
            jax.ShapeDtypeStruct((length, width), bf16),
            jax.ShapeDtypeStruct((length, width), f32),
            jax.ShapeDtypeStruct((length, width), f32),
        ],
        scratch_shapes=[
            pltpu.VMEM((heads, blocks, BLOCK, BLOCK), f32),
            pltpu.VMEM((heads, lanes, length), bf16),
        ],
        compiler_params=pltpu.CompilerParams(vmem_limit_bytes=48 << 20),
        cost_estimate=pl.CostEstimate(
            flops=4 * length * length * width, bytes_accessed=20 * length * width, transcendentals=0
        ),
        name="attend",
    )(qkv, ob.reshape(steps, heads, 2 * length))


def attend_back_kernel(
    blocks, heads, qkv_ref, ob_ref, da_ref, summed_ref, total_ref, dqkv_ref, diag_ref,
    bias, diff, qt, kt, km, vt, dm, dmt, dt, acc_k, acc_v,
):
    width = qkv_ref.shape[2]
    lanes = [slice(head * HEAD_DIM, (head + 1) * HEAD_DIM) for head in range(heads)]
    for head in range(heads):
        fill_bias(ob_ref, head, bias.at[head], blocks)
    diff[...] = jnp.zeros_like(diff)
    acc_k[...] = jnp.zeros_like(acc_k)
    acc_v[...] = jnp.zeros_like(acc_v)
    row = lax.broadcasted_iota(jnp.int32, (width, 1), 0) // HEAD_DIM
    scale = jnp.asarray(score_scale, bf16)
    for b in range(blocks):
        rows = slice(b * BLOCK, (b + 1) * BLOCK)
        qt[:, rows] = transposed(qkv_ref[0, rows, :]) * scale
        turned = transposed(qkv_ref[1, rows, :])
        vt[:, rows] = transposed(qkv_ref[2, rows, :])
        grad = da_ref[rows, :].astype(f32)
        total = total_ref[rows, :]
        scaled = grad / total
        dmt[:, rows] = transposed(scaled)
        inner = scaled * summed_ref[rows, :] / total
        for head in range(heads):
            mask = lane_mask(width, head, f32)
            kt[head, :, rows] = turned * (row == head).astype(bf16)
            km[head, rows, :] = qkv_ref[1, rows, :] * lane_mask(width, head, bf16)
            dm[head, rows, :] = (scaled * mask).astype(bf16)
            shift = -jnp.sum(inner * mask, axis=1, keepdims=True)
            dt[head, rows, :] = jnp.broadcast_to(shift, (BLOCK, 128))

    for qb in range(blocks):
        rows = slice(qb * BLOCK, (qb + 1) * BLOCK)
        queries = qkv_ref[0, rows, :] * scale
        shifts = [dt[head, rows, :] for head in range(heads)]

        def step(kb, acc_q):
            cols = pl.ds(pl.multiple_of(kb * BLOCK, BLOCK), BLOCK)
            for head in range(heads):
                score = jnp.dot(queries, kt[head, :, cols], preferred_element_type=f32)
                expo = jnp.exp(score + bias[head, qb - kb])
                probs = jnp.dot(dm[head, rows, :], vt[:, cols], preferred_element_type=f32)
                shift = jnp.concatenate([shifts[head]] * (BLOCK // 128), axis=1)
                dscore = (expo * (probs + shift)).astype(bf16)
                diff[head, qb - kb] += dscore.astype(f32)
                acc_q = acc_q + jnp.dot(dscore, km[head, cols, :], preferred_element_type=f32)
                acc_k[lanes[head], cols] += jnp.dot(
                    qt[lanes[head], rows], dscore, preferred_element_type=f32
                )
                acc_v[lanes[head], cols] += jnp.dot(
                    dmt[lanes[head], rows], expo.astype(bf16), preferred_element_type=f32
                )
            return acc_q

        acc_q = jnp.zeros((BLOCK, width), f32)
        for kb in range(qb + 1):
            acc_q = step(kb, acc_q)
        dqkv_ref[0, rows, :] = (acc_q * score_scale).astype(bf16)

    lower = lax.broadcasted_iota(jnp.int32, (8, 2 * BLOCK), 0)
    for head in range(heads):
        for d in range(blocks):

            def add_rows(i, fold):
                part = diff[head, d, pl.ds(pl.multiple_of(i * 8, 8), 8), :]
                wide = jnp.concatenate([jnp.zeros((8, BLOCK), f32), part], axis=1)
                return fold + pltpu.roll(wide, 2 * BLOCK - 8 * i, 1)

            fold = lax.fori_loop(
                0, BLOCK // 8, add_rows, jnp.zeros((8, 2 * BLOCK), f32), unroll=8
            )
            for bit in (1, 2, 4):
                fold = jnp.where((lower & bit) != 0, pltpu.roll(fold, 2 * BLOCK - bit, 1), fold)
            diag_ref[0, pl.ds(head * blocks + d, 1), :] = jnp.sum(fold, axis=0, keepdims=True)
    for b in range(blocks):
        rows = slice(b * BLOCK, (b + 1) * BLOCK)
        dqkv_ref[1, rows, :] = acc_k[:, rows].T.astype(bf16)
        dqkv_ref[2, rows, :] = acc_v[:, rows].T.astype(bf16)


def attend_back(qkv, ob, grad, summed, total):
    _, length, width = qkv.shape
    lanes = min(width, 128)
    heads = lanes // HEAD_DIM
    steps = width // lanes
    blocks = length // BLOCK
    rows = pl.BlockSpec((length, lanes), lambda i: (0, i))
    wide = pl.BlockSpec((3, length, lanes), lambda i: (0, 0, i))
    dqkv, diag = pl.pallas_call(
        partial(attend_back_kernel, blocks, heads),
        grid=(steps,),
        in_specs=[wide, pl.BlockSpec((1, heads, 2 * length), lambda i: (i, 0, 0)), rows, rows, rows],
        out_specs=[wide, pl.BlockSpec((1, heads * blocks, 2 * BLOCK), lambda i: (i, 0, 0))],
        out_shape=[
            jax.ShapeDtypeStruct((3, length, width), bf16),
            jax.ShapeDtypeStruct((steps, heads * blocks, 2 * BLOCK), f32),
        ],
        scratch_shapes=[
            pltpu.VMEM((heads, blocks, BLOCK, BLOCK), f32),
            pltpu.VMEM((heads, blocks, BLOCK, BLOCK), f32),
            pltpu.VMEM((lanes, length), bf16),
            pltpu.VMEM((heads, lanes, length), bf16),
            pltpu.VMEM((heads, length, lanes), bf16),
            pltpu.VMEM((lanes, length), bf16),
            pltpu.VMEM((heads, length, lanes), bf16),
            pltpu.VMEM((lanes, length), bf16),
            pltpu.VMEM((heads, length, 128), f32),
            pltpu.VMEM((lanes, length), f32),
            pltpu.VMEM((lanes, length), f32),
        ],
        compiler_params=pltpu.CompilerParams(vmem_limit_bytes=56 << 20),
        cost_estimate=pl.CostEstimate(
            flops=10 * length * length * width, bytes_accessed=30 * length * width, transcendentals=0
        ),
        name="attend_back",
    )(qkv, ob.reshape(steps, heads, 2 * length), grad, summed, total)
    return dqkv, diag.reshape(steps * heads, blocks, 2 * BLOCK)


def norm_back(norm_input, factor, gain_wide, grad_normed):
    scaled = grad_normed * gain_wide
    gain_grad = jnp.sum(grad_normed * norm_input * factor, axis=0)
    mean_term = jnp.mean(scaled * norm_input, axis=-1, keepdims=True)
    return (factor * scaled - norm_input * factor * factor * factor * mean_term, gain_grad)


def adamw_step(master, gradient, first_old, second_old):
    first_new = decay_rate * first_old + (1.0 - decay_rate) * gradient
    second_new = decay_rate * second_old + (1.0 - decay_rate) * gradient * gradient
    correct = 1.0 - decay_rate**STEP
    update = -learn_rate * (
        first_new / correct / (jnp.sqrt(second_new / correct) + eps_adam) + weight_decay * master
    )
    return (gradient, first_new, second_new, update)


def layer(tokens, cotangent, bucket_ids, routes, *state):
    masters, firsts, seconds = state[:9], state[9:18], state[18:]
    (
        qkv_master, out_master, router_master, gain_attn_master, gain_mix_master, table_master,
        gate_master, up_master, down_master,
    ) = masters
    micro, tok_rows = tokens.shape[0], tokens.shape[2]
    cycle = lax.axis_size("ctx")
    count = cycle * EXP_AXIS
    length = tok_rows * cycle
    group = cycle // micro
    width = D // group
    place = lax.axis_index("ctx")
    head_group = place % group
    line = cycle // 2
    line_place = place // 2
    rows = D // count
    experts_all = router_master.shape[1]
    capacity = 5 * tok_rows * TOP // (4 * experts_all)
    low = my_bit(0) == 0

    tok = tokens[:, 0]
    cols = qkv_master.astype(bf16).reshape(3 * rows, group, width).transpose(1, 0, 2)
    small = jnp.concatenate(
        [
            router_master.reshape(-1), gain_attn_master, gain_mix_master, table_master,
        ]
    ).astype(bf16)
    small_size = small.shape[0]
    small = jnp.pad(small, (0, 16 * width - small_size)).reshape(1, 16, width)
    cols = jnp.concatenate([cols, jnp.broadcast_to(small, (group, 16, width))], axis=1)
    w_out = lax.all_gather(out_master.astype(bf16), both, axis=0, tiled=True)
    pair_own = turn(jnp.concatenate([gate_master, up_master], axis=0).astype(bf16))
    down_own = turn(down_master[0].astype(bf16))
    right, left = [pair_own], [pair_own]

    def line_round(step):
        right.append(line_permute(right[-1], 1, step))
        left.append(line_permute(left[-1], -1, step))

    def line_settle(value):
        value, right[-1], left[-1] = lax.optimization_barrier((value, right[-1], left[-1]))
        return value

    line_round(0)
    seq, gathered = opening(tok, cols)
    seq = line_settle(seq)
    seq, pair_late = lax.optimization_barrier((seq, pair_own))
    line_round(1)
    seq = seq.reshape(length, D)
    w_qkv = gathered[:, :, : 3 * rows].reshape(EXP_AXIS, cycle, 3, rows, width)
    w_qkv = w_qkv.transpose(2, 1, 0, 3, 4).reshape(3, D, width)
    small = gathered[:, :, 3 * rows :].reshape(EXP_AXIS, cycle, 16 * width)[:, :, :small_size]
    small = small.transpose(1, 0, 2).reshape(count, small_size)
    edges = (0, rows * experts_all, rows * (experts_all + 1), rows * (experts_all + 2))
    router_bf = small[:, : edges[1]].reshape(D, experts_all)
    gain_attn = small[:, edges[1] : edges[2]].reshape(D).astype(f32)
    gain_mix = small[:, edges[2] : edges[3]].reshape(D).astype(f32)
    table = small[:, edges[3] :].reshape(HEADS, -1)
    bucket_count = table.shape[1]
    router_wide = router_bf.astype(f32)
    bucket_hits = bucket_ids[:, None] == jnp.arange(bucket_count, dtype=jnp.int32)[None, :]
    own_heads = HEADS // group
    own_table = lax.dynamic_slice_in_dim(table, head_group * own_heads, own_heads, 0)
    offset_bias = lax.dot_general(
        own_table, bucket_hits.astype(bf16), last_dims, preferred_element_type=f32
    )
    offset_bias = jnp.pad(offset_bias, ((0, 0), (1, 0)))[:, :-1]

    seq_wide = seq.astype(f32)
    seq_factor = lax.rsqrt(jnp.mean(seq_wide * seq_wide, axis=-1, keepdims=True) + eps_norm)
    normed = (seq_wide * seq_factor * gain_attn).astype(bf16)
    qkv = jnp.einsum("td,cde->cte", normed, w_qkv, preferred_element_type=f32).astype(bf16)
    attended, summed, total = attend(qkv, offset_bias)

    back = cycle_swap(attended.reshape(cycle, tok_rows, width), 1)
    back = line_settle(back)
    if line > 3:
        line_round(2)
    toks = micro * tok_rows
    attended_bf = back.reshape(micro, group, tok_rows, width).transpose(0, 2, 1, 3)
    attended_bf = attended_bf.reshape(toks, D)
    inputs = tok.reshape(toks, D).astype(f32)
    factor_attn = lax.rsqrt(jnp.mean(inputs * inputs, axis=-1, keepdims=True) + eps_norm)
    hidden_state = inputs + jnp.dot(attended_bf, w_out, preferred_element_type=f32)
    factor_mix = lax.rsqrt(jnp.mean(hidden_state * hidden_state, axis=-1, keepdims=True) + eps_norm)
    normed_mix = hidden_state * factor_mix * gain_mix
    normed_bf = normed_mix.astype(bf16)
    logits = jnp.dot(normed_bf, router_bf, preferred_element_type=f32)
    router_probs = jax.nn.softmax(logits, axis=-1)
    route_rows = routes.reshape(micro, tok_rows, TOP)
    expert_ids = jnp.arange(experts_all, dtype=jnp.int32)
    picked = (route_rows.reshape(toks, TOP)[:, :, None] == expert_ids).astype(f32)
    chosen = jnp.sum(picked * router_probs[:, None, :], axis=-1)
    chosen_sum = jnp.sum(chosen, axis=-1, keepdims=True)
    gate_share = chosen / chosen_sum
    flat_routes = route_rows.reshape(micro, tok_rows * TOP)
    route_hits = (flat_routes[:, :, None] == expert_ids).astype(jnp.int32)
    before = jnp.cumsum(route_hits, axis=1) - route_hits
    micro_ids = jnp.arange(micro, dtype=jnp.int32)[:, None]
    slot_index = (flat_routes * micro + micro_ids) * capacity + jnp.sum(before * route_hits, axis=-1)
    slot_index = slot_index.reshape(toks, TOP)
    slot_count = experts_all * micro * capacity
    slot_ids = jnp.arange(slot_count, dtype=jnp.int32)
    hits = [(slot_index[:, choice, None] == slot_ids).astype(bf16) for choice in range(TOP)]
    slots = (experts_all, micro, capacity, D)
    sent_rows = lax.dot_general(sum(hits), normed_bf, first_dims, preferred_element_type=f32)
    dy_rows = cotangent.reshape(toks, D).astype(f32)
    scaled_dy = [
        (gate_share[:, choice, None] * dy_rows).astype(bf16) for choice in range(TOP)
    ]
    sent_grads = lax.dot_general(
        jnp.concatenate(hits, axis=0), jnp.concatenate(scaled_dy, axis=0), first_dims,
        preferred_element_type=f32,
    )
    sent_rows = sent_rows.astype(bf16)
    sent_grads = sent_grads.astype(bf16)
    got_rows, got_grads = plane_swap((sent_rows.reshape(slots), sent_grads.reshape(slots)), True, 2)
    got_rows, down_own = lax.optimization_barrier((line_settle(got_rows), down_own))
    for step in range(3, line - 1):
        line_round(step)
    flat_rows = got_rows.reshape(-1, D)
    flat_grads = got_grads.reshape(-1, D)

    blocks = []
    for k in range(line):
        mine = pair_late
        if k:
            mine = jnp.where(line_place + k < line, left[k], right[line - k])
        blocks += [mine, swap_bit(mine, 0)]
    w_down = gather_expert(down_own)
    kernels = pair_own.shape[1] % 128 == 0
    if kernels:
        units, value, slope = expert_front(flat_rows, blocks)
    else:

        def whole(part):
            pieces = []
            for mine, theirs in zip(blocks[::2], blocks[1::2]):
                pieces += [jnp.where(low, mine, theirs)[part], jnp.where(low, theirs, mine)[part]]
            return jnp.concatenate(pieces, axis=0)

        def turned(value, shift):
            twice = jnp.concatenate([value, value], axis=1)
            return lax.dynamic_slice_in_dim(twice, shift * (D // line), D, 1)

        w_gate, w_up = whole(0), whole(1)
        turned_rows = turned(flat_rows, line_place)
        gate_pre = jnp.dot(turned_rows, w_gate, preferred_element_type=f32)
        up_pre = jnp.dot(turned_rows, w_up, preferred_element_type=f32)
        value, slope = gelu_pair(gate_pre)
        units, slope = (value * up_pre).astype(bf16), slope * up_pre
    down_grad = lax.dot_general(units, flat_grads, first_dims, preferred_element_type=f32)
    down_sum = scatter_expert(core_sum(down_grad.astype(bf16)))
    grad_gate, grad_up = expert_middle(flat_grads, w_down, value, slope)
    up_grad = lax.dot_general(flat_rows, grad_up, first_dims, preferred_element_type=f32)
    up_sum = scatter_expert(core_sum(up_grad.astype(bf16)))
    gate_grad = lax.dot_general(flat_rows, grad_gate, first_dims, preferred_element_type=f32)
    gate_sum = scatter_expert(core_sum(gate_grad.astype(bf16)))
    out_rows = jnp.dot(units, w_down, preferred_element_type=f32).astype(bf16)
    if kernels:
        grad_rows = expert_rear(grad_gate, grad_up, blocks)
    else:
        grad_rows = lax.dot_general(grad_gate, w_gate, last_dims, preferred_element_type=f32)
        grad_rows = grad_rows + lax.dot_general(
            grad_up, w_up, last_dims, preferred_element_type=f32
        )
        grad_rows = turned(grad_rows.astype(bf16), line - line_place)
    back_out, back_grad = plane_swap((out_rows.reshape(slots), grad_rows.reshape(slots)), False, 3)
    back_out, back_grad = back_out.reshape(slot_count, D), back_grad.reshape(slot_count, D)

    returned = [jnp.dot(hit, back_out, preferred_element_type=f32) for hit in hits]
    mix_out = sum(gate_share[:, c, None] * returned[c] for c in range(TOP))
    output = (hidden_state + mix_out).astype(bf16)
    grad_gates = jnp.stack([jnp.sum(dy_rows * returned[c], axis=-1) for c in range(TOP)], axis=1)
    grad_chosen = grad_gates / chosen_sum - jnp.sum(grad_gates * chosen, axis=-1, keepdims=True) / (
        chosen_sum * chosen_sum
    )
    grad_probs = jnp.sum(grad_chosen[:, :, None] * picked, axis=1)
    grad_logits = router_probs * (
        grad_probs - jnp.sum(router_probs * grad_probs, axis=-1, keepdims=True)
    )
    router_grad = lax.dot_general(
        normed_bf.astype(f32), grad_logits, first_dims, precision=highest
    )
    grad_normed = jnp.dot(sum(hits), back_grad, preferred_element_type=f32) + lax.dot_general(
        grad_logits, router_wide, last_dims, precision=highest
    )
    grad_hidden, gain_mix_grad = norm_back(hidden_state, factor_mix, gain_mix, grad_normed)
    grad_hidden = grad_hidden + dy_rows
    grad_branch = grad_hidden.astype(bf16)
    grad_attended = lax.dot_general(grad_branch, w_out, last_dims, preferred_element_type=f32)
    grad_attended = grad_attended.astype(bf16).reshape(micro, tok_rows, group, width)
    grad_attended = grad_attended.transpose(0, 2, 1, 3).reshape(cycle, tok_rows, width)
    grad_attended = cycle_swap(grad_attended, 4).reshape(length, width)
    out_grad = lax.dot_general(attended_bf, grad_branch, first_dims, preferred_element_type=f32)
    out_grad = out_grad.astype(bf16).reshape(cycle, 2, 2, rows, D).transpose(2, 1, 0, 3, 4)
    out_grad = cube_sum(out_grad, 0)
    out_grad = cube_sum(out_grad, 1)

    dqkv, diag = attend_back(qkv, offset_bias, grad_attended, summed, total)
    partial_normed = jnp.einsum("cte,cde->td", dqkv, w_qkv, preferred_element_type=f32)
    partial_normed = partial_normed.astype(bf16).reshape(cycle, tok_rows, D)
    dqkv, partial_normed = lax.optimization_barrier((dqkv, partial_normed))
    pieces = lax.all_to_all(partial_normed, "ctx", 0, 0, tiled=True)
    qkv_grad = jnp.einsum("td,cte->cde", normed, dqkv, preferred_element_type=f32)
    qkv_grad = qkv_grad.astype(bf16).reshape(3, cycle, 2, 2, rows, width)
    qkv_grad = qkv_grad.transpose(3, 2, 1, 0, 4, 5)
    qkv_grad = cube_sum(qkv_grad, 0)
    qkv_grad = cube_sum(qkv_grad, 1)
    expert_results = [
        adamw_step(master, total[None].astype(f32), first_old, second_old)
        for master, total, first_old, second_old in zip(
            masters[6:], (gate_sum, up_sum, down_sum), firsts[6:], seconds[6:]
        )
    ]
    pieces, expert_results = lax.optimization_barrier((pieces, expert_results))
    grad_normed_attn = jnp.sum(pieces.reshape(micro, group, tok_rows, D).astype(f32), axis=1)
    grad_inputs, gain_attn_grad = norm_back(
        inputs, factor_attn, gain_attn, grad_normed_attn.reshape(toks, D)
    )
    grad_inputs = grad_inputs + grad_hidden

    blocks = length // BLOCK
    offset_grad = jnp.zeros((own_heads, 2 * length), f32)
    for d in range(blocks):
        first = (blocks - d - 1) * BLOCK
        offset_grad = offset_grad + jnp.pad(
            diag[:, d], ((0, 0), (first, 2 * length - first - 2 * BLOCK))
        )
    offset_grad = jnp.pad(offset_grad[:, 1:], ((0, 0), (0, 1)))
    own_grad = jnp.dot(offset_grad, bucket_hits.astype(f32), precision=highest)
    table_grad = lax.dynamic_update_slice_in_dim(
        jnp.zeros((HEADS, bucket_count), f32), own_grad, head_group * own_heads, 0
    )
    small_grads = jnp.concatenate(
        [
            router_grad.reshape(count, -1), gain_attn_grad.reshape(count, -1),
            gain_mix_grad.reshape(count, -1), table_grad.reshape(count, -1),
        ],
        axis=1,
    )
    small_grads = jnp.pad(small_grads, ((0, 0), (0, -small_grads.shape[1] % 128)))
    small_grads = small_grads.reshape(cycle, EXP_AXIS, 1, -1)
    qkv_grad, out_grad, small_parts = closing(qkv_grad, out_grad, small_grads)
    qkv_sum = jnp.sum(qkv_grad.reshape(micro, group, 3, rows, width).astype(f32), axis=0)
    qkv_sum = qkv_sum.transpose(1, 2, 0, 3).reshape(3, rows, D)
    out_sum = jnp.sum(out_grad.astype(f32), axis=0)
    small_sum = jnp.sum(small_parts, axis=(0, 1))
    small_sum = lax.dynamic_index_in_dim(small_sum, lax.axis_index("exp"), 0, keepdims=False)
    small_sum = small_sum[0, :small_size]
    gradients = (
        qkv_sum,
        out_sum,
        small_sum[: edges[1]].reshape(rows, experts_all),
        small_sum[edges[1] : edges[2]],
        small_sum[edges[2] : edges[3]],
        small_sum[edges[3] :],
    )
    results = [
        adamw_step(master, gradient, first_old, second_old)
        for master, gradient, first_old, second_old in zip(masters, gradients, firsts, seconds)
    ] + expert_results
    flat = [result[kind] for kind in range(4) for result in results]
    return (output.reshape(tokens.shape), grad_inputs.reshape(tokens.shape), *flat)


def solution(mesh):
    token_spec = P(None, "exp", "ctx", None)
    weight_specs = (
        P(None, both, None), P(both, None), P(both, None), P(both), P(both), P(both),
        P("exp", "ctx", None), P("exp", "ctx", None), P("exp", "ctx", None),
    )
    return jax.shard_map(
        layer,
        mesh=mesh,
        in_specs=(token_spec, token_spec, P(), token_spec) + weight_specs * 3,
        out_specs=(token_spec, token_spec) + weight_specs * 4,
        check_vma=False,
    )
```
